256 devices in a mesh: ctx: 128 (over x, y, z_lo, core), fsdp: 2 (over z_hi).
Axes of the slice: x: 4, y: 4, z: 8 (z_hi: 2, z_lo: 4; z = z_hi * 4 + z_lo), core: 2. Of those that a mesh axis runs over, the one named last changes fastest.
Arguments:
- layer_input: bfloat16 [16384, 4096], P('ctx'), may hold values from -8 to 8
- gain: float32 [4096], replicated, may hold values from 0.5 to 1.5
- codes: int32 [4096, 384], P('fsdp'), may hold values from -2147483648 to 2147483646
- column_scale_quantized: int32 [64, 3072], P('fsdp'), may hold values from 0 to 255
- block_second_scale: float32 [64], replicated, may hold values from 0.03 to 0.12
- query_down_map: bfloat16 [4096, 16], replicated, may hold values from -0.09375 to 0.09375
- query_up_map: bfloat16 [16, 2048], P(None, 'fsdp'), may hold values from -0.29882812 to 0.29882812
- token_document: int32 [16384], P('ctx'), may hold values from 0 to 3, as said below
- output_cotangent: bfloat16 [16384, 2048], P('ctx', 'fsdp'), may hold values from -0.059814453 to 0.059814453
Outputs:
- attn: bfloat16 [16384, 2048], P('ctx', 'fsdp')
- grad_a: float32 [4096, 16], replicated
- up_map_gradient: float32 [16, 2048], P(None, 'fsdp')
The draws below stay inside these ranges and needn't reach their ends.
Inputs may be any that keep to these rules, and one draw needn't show every extreme that they name: token_document never falls along the sequence; each document has 1 to 12288 tokens and one has exactly 12288.
All inputs are finite; a program needn't handle non-finite values.
Results may differ from the reference program's by a relative error of at most 0.028.
Values may be sent and summed in bfloat16 or wider, within the bound.
A program may use at most 192 MiB of HBM per device.

```python
import math
import jax
import jax.numpy as jnp
import numpy as np
from jax import lax

MODEL_WIDTH = 4096
QUERY_HEADS = 16
KEY_VALUE_HEADS = 4
HEAD_SIZE = 128
ADAPTER_RANK = 16
DOCS = 4
SEQUENCE_TOKENS = 16384
MOST = 12288
QUERY_FEATURES = 2048
COLS = 3072
N_FSDP = 2


NF4_LEVELS = [-1.0, -0.6961928009986877, -0.5250730514526367, -0.39491748809814453, -0.28444138169288635, -0.18477343022823334, -0.09105003625154495, 0.0, 0.07958029955625534, 0.16093020141124725, 0.24611230194568634, 0.33791524171829224, 0.44070982933044434, 0.5626170039176941, 0.7229568362236023, 1.0]


def weight_parts(key):
    code_key = jax.random.fold_in(key, 101)
    scale_key = jax.random.fold_in(key, 102)
    const_key = jax.random.fold_in(key, 103)
    packed = jax.random.randint(code_key, (MODEL_WIDTH, COLS // 8), -2147483648, 2147483647, dtype=jnp.int32)
    scales = jax.random.randint(scale_key, (MODEL_WIDTH // 64, COLS), 0, 256, dtype=jnp.int32)
    lower, upper = (0.03, 0.09)
    consts = jnp.exp(jax.random.uniform(const_key, (MODEL_WIDTH // 64,), jnp.float32, math.log(lower), math.log(upper)))
    return (packed, scales, consts)


def unpack_weights(packed, scales, consts):
    row_count = packed.shape[0]
    pieces = [jnp.bitwise_and(jnp.right_shift(packed, 4 * nibble), 15) for nibble in range(8)]
    unpacked = jnp.stack(pieces, axis=-1).reshape(row_count, packed.shape[1] * 8)
    table = jnp.asarray(NF4_LEVELS, jnp.float32)
    levels = table[unpacked]
    absmax = (scales.astype(jnp.float32) + 1.0) / 256.0 * consts[:, None]
    return (levels.reshape(row_count // 64, 64, -1) * absmax[:, None, :]).reshape(row_count, -1)


def doc_layout(key):
    layout_key = jax.random.fold_in(key, 401)
    long_slot = jax.random.randint(jax.random.fold_in(layout_key, 1), (), 1, DOCS, dtype=jnp.int32)
    remaining = jnp.int32(SEQUENCE_TOKENS - MOST)
    others = []
    for number in range(DOCS - 2):
        upper_len = remaining - (DOCS - 2 - number) + 1
        length_now = jax.random.randint(jax.random.fold_in(layout_key, 10 + number), (), 1, upper_len, dtype=jnp.int32)
        others.append(length_now)
        remaining = remaining - length_now
    others.append(remaining)
    lengths = []
    for number in range(DOCS):
        before = others[min(number, DOCS - 2)]
        after = others[max(number - 1, 0)]
        lengths.append(jnp.where(number < long_slot, before, jnp.where(number == long_slot, jnp.int32(MOST), after)))
    lengths = jnp.stack(lengths).astype(jnp.int32)
    ends = jnp.cumsum(lengths).astype(jnp.int32)
    positions = jnp.arange(SEQUENCE_TOKENS, dtype=jnp.int32)
    ids = jnp.sum((positions[:, None] >= ends[None, :DOCS - 1]).astype(jnp.int32), axis=1).astype(jnp.int32)
    starts = ends - lengths
    long_start = jnp.sum(jnp.where(jnp.arange(DOCS, dtype=jnp.int32) == long_slot, starts, 0)).astype(jnp.int32)
    return (ids, long_start)


def draw_token_document(key, part):
    return doc_layout(key)[0]


def draw_codes(key, part):
    return weight_parts(key)[0]


def draw_column_scale_quantized(key, part):
    return weight_parts(key)[1]


def draw_block_second_scale(key, part):
    return weight_parts(key)[2]


def far_pairs(key, fields, weight):
    long_start = doc_layout(key)[1]
    hq_local = QUERY_HEADS // N_FSDP
    key_value_local = KEY_VALUE_HEADS // N_FSDP
    group_columns = COLS // N_FSDP
    head_grouped = QUERY_HEADS // KEY_VALUE_HEADS
    half_size = HEAD_SIZE // 2
    edge_dims = max(HEAD_SIZE // 16, 1)
    aligned = list(range(half_size - edge_dims, half_size)) + list(range(HEAD_SIZE - edge_dims, HEAD_SIZE))
    root_width = math.sqrt(MODEL_WIDTH)
    for plant in range(8):
        query_head = 3 * plant % QUERY_HEADS
        group_id = query_head // hq_local
        key_head = query_head // head_grouped
        query_cols = np.array([group_id * group_columns + (query_head - group_id * hq_local) * HEAD_SIZE + dim for dim in aligned])
        key_cols = np.array([group_id * group_columns + hq_local * HEAD_SIZE + (key_head - group_id * key_value_local) * HEAD_SIZE + dim for dim in aligned])
        columns = jnp.concatenate([weight[:, query_cols], weight[:, key_cols]], axis=1)
        direction = jnp.sum(columns, axis=1)
        direction = direction / jnp.sqrt(jnp.sum(direction * direction))
        offset = jax.random.randint(jax.random.fold_in(key, 500 + plant), (), 0, SEQUENCE_TOKENS // 4, dtype=jnp.int32)
        position = long_start + offset
        vector = root_width * direction
        fields = fields.at[position].set(vector)
        fields = fields.at[position + SEQUENCE_TOKENS // 2].set(vector)
    return fields


def draw_layer_input(key, part):
    fields = jax.random.normal(jax.random.fold_in(key, 201), (SEQUENCE_TOKENS, MODEL_WIDTH), jnp.float32)
    packed, scales, consts = weight_parts(key)
    weight = unpack_weights(packed, scales, consts)
    fields = far_pairs(key, fields, weight)
    return jnp.clip(fields, -6.0, 6.0).astype(jnp.bfloat16)


def shard_levels(stream_key, shape, shards, low, top_value):
    level = 1.0
    for dim, shards_of in shards:
        steps = jax.random.uniform(jax.random.fold_in(jax.random.fold_in(stream_key, 6), dim), (shards_of,), jnp.float32, low / len(shards), top_value / len(shards))
        level = level * jnp.repeat(jnp.exp(steps), shape[dim] // shards_of).reshape((-1,) + (1,) * (len(shape) - 1 - dim))
    return level


def bell_draw(key, dims, width, most, cuts=(), held_as=jnp.bfloat16):
    result = jax.random.normal(key, dims, jnp.float32) * width
    if len(cuts) > 0:
        result = shard_levels(key, dims, cuts, -0.22, 0.18) * result
    return jnp.clip(result, min=-most, max=most).astype(held_as)


def setup_inputs(seed: int = 0) -> dict:
    splits = jax.random.split(jax.random.key(seed), 10)
    layer_input = draw_layer_input(jax.random.fold_in(splits[9], 71), 0)
    gain = jnp.clip(1.0 + 0.1 * jax.random.normal(splits[1], (MODEL_WIDTH,), jnp.float32), 0.5, 1.5)
    codes = draw_codes(jax.random.fold_in(splits[9], 71), 0)
    column_scale_quantized = draw_column_scale_quantized(jax.random.fold_in(splits[9], 71), 0)
    block_second_scale = draw_block_second_scale(jax.random.fold_in(splits[9], 71), 0)
    query_down_map = bell_draw(splits[5], (MODEL_WIDTH, ADAPTER_RANK), MODEL_WIDTH ** -0.5, 0.09375)
    query_up_map = bell_draw(splits[6], (ADAPTER_RANK, QUERY_FEATURES), 0.05, 0.29882812, ((1, 2),))
    token_document = draw_token_document(jax.random.fold_in(splits[9], 71), 0)
    output_cotangent = bell_draw(splits[8], (SEQUENCE_TOKENS, QUERY_FEATURES), 0.01, 0.059814453, ((0, 128), (1, 2)))
    return {"layer_input": layer_input, "gain": gain, "codes": codes, "column_scale_quantized": column_scale_quantized, "block_second_scale": block_second_scale, "query_down_map": query_down_map, "query_up_map": query_up_map, "token_document": token_document, "output_cotangent": output_cotangent}


NF4_LEVELS = [-1.0, -0.6961928009986877, -0.5250730514526367, -0.39491748809814453, -0.28444138169288635, -0.18477343022823334, -0.09105003625154495, 0.0, 0.07958029955625534, 0.16093020141124725, 0.24611230194568634, 0.33791524171829224, 0.44070982933044434, 0.5626170039176941, 0.7229568362236023, 1.0]
ADAPTER_SCALE = 2.0
ROPE_BASE = 500000.0

def dequantize(packed, column_scale_quantized, block_second_scale):
    row_count = packed.shape[0]
    pieces = [jnp.bitwise_and(jnp.right_shift(packed, 4 * nibble), 15) for nibble in range(8)]
    unpacked = jnp.stack(pieces, axis=-1).reshape(row_count, packed.shape[1] * 8)
    levels = jnp.zeros(unpacked.shape, jnp.float32)
    for slot_code, level_value in enumerate(NF4_LEVELS):
        levels = levels + jnp.where(unpacked == slot_code, jnp.float32(level_value), jnp.float32(0.0))
    absmax = (column_scale_quantized.astype(jnp.float32) + 1.0) / 256.0 * block_second_scale[:, None]
    scaled = levels.reshape(row_count // 64, 64, -1) * absmax[:, None, :]
    return scaled.reshape(row_count, -1).astype(jnp.bfloat16)

def rope_angles(positions):
    freqs = jnp.exp(jnp.arange(HEAD_SIZE // 2, dtype=jnp.float32) * (-2.0 * math.log(ROPE_BASE) / HEAD_SIZE))
    angle = positions.astype(jnp.float32)[:, None] * freqs[None, :]
    cosine = jnp.concatenate([jnp.cos(angle), jnp.cos(angle)], axis=-1)
    sine = jnp.concatenate([jnp.sin(angle), jnp.sin(angle)], axis=-1)
    return (cosine, sine)

def apply_rotation(field, rotary_phases):
    cosine, sine = rotary_phases
    half = HEAD_SIZE // 2
    turned = jnp.concatenate([-field[..., half:], field[..., :half]], axis=-1)
    return field * cosine[:, None, :] + turned * sine[:, None, :]

def rotate_back(grads, rotary_phases):
    cosine, sine = rotary_phases
    half = HEAD_SIZE // 2
    scaled = grads * sine[:, None, :]
    turned = jnp.concatenate([-scaled[..., half:], scaled[..., :half]], axis=-1)
    return grads * cosine[:, None, :] - turned

def rms_norm(layer_input, gain):
    wide = layer_input.astype(jnp.float32)
    inverse = lax.rsqrt(lax.optimization_barrier(jnp.mean(wide * wide, axis=-1, keepdims=True)) + 1e-05)
    return (wide * inverse * gain[None, :]).astype(jnp.bfloat16)

def reference(layer_input, gain, codes, column_scale_quantized, block_second_scale, query_down_map, query_up_map, token_document, output_cotangent):
    input_normalized = rms_norm(layer_input, gain)
    weight = dequantize(codes, column_scale_quantized, block_second_scale)
    projection_output = jnp.dot(input_normalized.astype(jnp.float32), weight.astype(jnp.float32), preferred_element_type=jnp.float32)
    group_columns = (QUERY_HEADS + 2 * KEY_VALUE_HEADS) * HEAD_SIZE // N_FSDP
    q_local = QUERY_HEADS // N_FSDP * HEAD_SIZE
    key_value_local = KEY_VALUE_HEADS // N_FSDP * HEAD_SIZE
    query_slices, key_slices, value_slices = ([], [], [])
    for member in range(N_FSDP):
        anchor = member * group_columns
        query_slices.append(projection_output[:, anchor:anchor + q_local])
        key_slices.append(projection_output[:, anchor + q_local:anchor + q_local + key_value_local])
        value_slices.append(projection_output[:, anchor + q_local + key_value_local:anchor + group_columns])
    rank_reduced = jnp.dot(input_normalized.astype(jnp.float32), query_down_map.astype(jnp.float32), preferred_element_type=jnp.float32).astype(jnp.bfloat16)
    query_complete = jnp.concatenate(query_slices, axis=1) + ADAPTER_SCALE * jnp.dot(rank_reduced.astype(jnp.float32), query_up_map.astype(jnp.float32), preferred_element_type=jnp.float32)
    positions = jnp.arange(SEQUENCE_TOKENS, dtype=jnp.int32)
    rotary_phases = rope_angles(positions)
    query_rows = apply_rotation(query_complete.reshape(SEQUENCE_TOKENS, QUERY_HEADS, HEAD_SIZE), rotary_phases).astype(jnp.bfloat16)
    key_rows = apply_rotation(jnp.concatenate(key_slices, axis=1).reshape(SEQUENCE_TOKENS, KEY_VALUE_HEADS, HEAD_SIZE), rotary_phases).astype(jnp.bfloat16)
    value_rows = jnp.concatenate(value_slices, axis=1).reshape(SEQUENCE_TOKENS, KEY_VALUE_HEADS, HEAD_SIZE).astype(jnp.bfloat16)
    head_grouped = QUERY_HEADS // KEY_VALUE_HEADS
    query_grouped = query_rows.reshape(SEQUENCE_TOKENS, KEY_VALUE_HEADS, head_grouped, HEAD_SIZE).astype(jnp.float32)
    grouped_gradient = output_cotangent.reshape(SEQUENCE_TOKENS, KEY_VALUE_HEADS, head_grouped, HEAD_SIZE).astype(jnp.float32)
    keys_wide = key_rows.astype(jnp.float32)
    values_wide = value_rows.astype(jnp.float32)
    soft_scale = 1.0 / math.sqrt(HEAD_SIZE)
    block = math.gcd(SEQUENCE_TOKENS, 256)

    def one_block(block_id):
        start = (block_id * block).astype(jnp.int32)
        query_blk = lax.dynamic_slice_in_dim(query_grouped, start, block, 0)
        grad_blk = lax.dynamic_slice_in_dim(grouped_gradient, start, block, 0)
        ids_blk = lax.dynamic_slice_in_dim(token_document, start, block, 0)
        pos_blk = start + jnp.arange(block, dtype=jnp.int32)
        allowed = (ids_blk[:, None] == token_document[None, :]) & (positions[None, :] <= pos_blk[:, None])
        scores = jnp.einsum('bhgd,shd->hgbs', query_blk, keys_wide) * soft_scale
        masked = jnp.where(allowed, scores, -1e+30)
        top = lax.optimization_barrier(jnp.max(masked, axis=-1, keepdims=True))
        expo = jnp.where(allowed, jnp.exp(masked - top), 0.0)
        probs = expo / lax.optimization_barrier(jnp.sum(expo, axis=-1, keepdims=True))
        rounded = probs.astype(jnp.bfloat16).astype(jnp.float32)
        output = jnp.einsum('hgbs,shd->bhgd', rounded, values_wide)
        grad_dots = jnp.einsum('bhgd,shd->hgbs', grad_blk, values_wide)
        mean_dot = lax.optimization_barrier(jnp.sum(probs * grad_dots, axis=-1, keepdims=True))
        grad_scores = (probs * (grad_dots - mean_dot)).astype(jnp.bfloat16).astype(jnp.float32)
        grad_query = jnp.einsum('hgbs,shd->bhgd', grad_scores, keys_wide) * soft_scale
        return (output, grad_query)
    outputs, grad_queries = lax.map(one_block, jnp.arange(SEQUENCE_TOKENS // block, dtype=jnp.int32))
    attn = outputs.reshape(SEQUENCE_TOKENS, QUERY_HEADS * HEAD_SIZE).astype(jnp.bfloat16)
    linear_gradient = rotate_back(grad_queries.reshape(SEQUENCE_TOKENS, QUERY_HEADS, HEAD_SIZE), rotary_phases).reshape(SEQUENCE_TOKENS, QUERY_HEADS * HEAD_SIZE).astype(jnp.bfloat16)
    up_map_gradient = ADAPTER_SCALE * jnp.dot(rank_reduced.T.astype(jnp.float32), linear_gradient.astype(jnp.float32), preferred_element_type=jnp.float32)
    middle_gradient = (ADAPTER_SCALE * jnp.dot(linear_gradient.astype(jnp.float32), query_up_map.T.astype(jnp.float32), preferred_element_type=jnp.float32)).astype(jnp.bfloat16)
    grad_a = jnp.dot(input_normalized.T.astype(jnp.float32), middle_gradient.astype(jnp.float32), preferred_element_type=jnp.float32)
    return (attn, grad_a, up_map_gradient)
```

```python
import functools
import math

import jax
import jax.numpy as jnp
from jax import lax
from jax.experimental import pallas as pl
from jax.experimental.pallas import tpu as pltpu
from jax.sharding import PartitionSpec as P

MESH = pl.DeviceIdType.MESH
HEAD = 128
NF4_LEVELS = [
    -1.0,
    -0.6961928009986877,
    -0.5250730514526367,
    -0.39491748809814453,
    -0.28444138169288635,
    -0.18477343022823334,
    -0.09105003625154495,
    0.0,
    0.07958029955625534,
    0.16093020141124725,
    0.24611230194568634,
    0.33791524171829224,
    0.44070982933044434,
    0.5626170039176941,
    0.7229568362236023,
    1.0,
]
ADAPTER_SCALE = 2.0
ROPE_BASE = 500000.0
SOFT_SCALE = 1.0 / math.sqrt(HEAD)
QUERY_SCALE = SOFT_SCALE * math.log2(math.e)
F32, BF16, I32 = jnp.float32, jnp.bfloat16, jnp.int32
VMEM_LIMIT = 60 * 1024 * 1024


def places():
    c = lax.axis_index("ctx")
    f = lax.axis_index("fsdp")
    return c // 32, (c // 8) % 4, (c // 2) % 4, c % 2, f


def ctx_of(x, y, z, j):
    return ((x * 4 + y) * 4 + z) * 2 + j


def lookup(table, index):
    return lax.gather(
        table,
        index[..., None],
        lax.GatherDimensionNumbers(
            offset_dims=(),
            collapsed_slice_dims=(1,),
            start_index_map=(1,),
            operand_batching_dims=(0,),
            start_indices_batching_dims=(0,),
        ),
        slice_sizes=(1, 1),
        mode=lax.GatherScatterMode.PROMISE_IN_BOUNDS,
    )


def remote(src, dst, send, recv, ctx, f):
    return pltpu.make_async_remote_copy(
        src_ref=src, dst_ref=dst, send_sem=send, recv_sem=recv, device_id=(ctx, f), device_id_type=MESH
    )


def project_kernel(
    x_ref, gain_ref, codes_ref, sq_ref, bs_ref, downt_ref, up_ref, cos_ref, sin_ref, table_ref,
    q_ref, kv_ref, normed_ref, lowt_ref,
    perm, scale, w_buf, acc, nat, send_main, send_half, recv_main, recv_half, total, send_sem, recv_sem,
):
    c = lax.axis_index("ctx")
    f = lax.axis_index("fsdp")
    other = 1 - f
    barrier = pltpu.get_barrier_semaphore()
    pl.semaphore_signal(barrier, inc=1, device_id=(c, other), device_id_type=MESH)

    wide = x_ref[...].astype(F32)
    inverse = lax.rsqrt(jnp.mean(wide * wide, axis=-1, keepdims=True) + 1e-05)
    normed_ref[...] = (wide * inverse * gain_ref[...]).astype(BF16)

    for part in range(8):
        m = lax.broadcasted_iota(I32, (128, 1024), 0)
        k = lax.broadcasted_iota(I32, (128, 1024), 1)
        perm[128 * part : 128 * part + 128, :] = jnp.where(k == 8 * m + part, 1.0, 0.0).astype(BF16)
    second = bs_ref[pl.ds(pl.multiple_of(32 * f, 32), 32), :] * (1.0 / 256.0)
    for t in range(3):
        quantized = (sq_ref[:, 1024 * t : 1024 * t + 1024].astype(F32) + 1.0).astype(BF16)
        packed = lax.dot_general(quantized, perm[...], (((1,), (1,)), ((), ())), preferred_element_type=F32)
        scale[t] = packed * second

    table = jnp.broadcast_to(table_ref[...], (64, 128))

    def tile(t):
        lane = pl.multiple_of(t * 128, 128)
        acc[...] = jnp.zeros_like(acc)

        def chunk(kc, carry):
            for b in range(4):
                row = pl.multiple_of(kc * 256 + b * 64, 64)
                words = codes_ref[pl.ds(row, 64), pl.ds(lane, 128)]
                scale_row = scale[t, pl.ds(kc * 4 + b, 1), :]
                for n in range(8):
                    index = jnp.bitwise_and(jnp.right_shift(words, 4 * n), 15)
                    levels = lookup(table, index)
                    w_buf[64 * b : 64 * b + 64, 128 * n : 128 * n + 128] = (
                        levels * scale_row[:, 128 * n : 128 * n + 128]
                    ).astype(BF16)
            col = pl.multiple_of(f * 2048 + kc * 256, 256)
            acc[...] += jnp.dot(normed_ref[:, pl.ds(col, 256)], w_buf[...], preferred_element_type=F32)
            return carry

        lax.fori_loop(0, 8, chunk, 0)
        full = acc[...]
        high = full.astype(BF16)
        low = (full - high.astype(F32)).astype(BF16)
        nat[...] = jnp.dot(high, perm[...], preferred_element_type=F32) + jnp.dot(
            low, perm[...], preferred_element_type=F32
        )

    own_main = pl.ds(pl.multiple_of(512 * f, 512), 1024)
    own_half = pl.ds(pl.multiple_of(1024 * (1 - f), 512), 512)

    tile(2 * (1 - f))
    send_main[...] = nat[...].astype(BF16)
    pl.semaphore_wait(barrier, 1)
    copy_main = remote(send_main, recv_main, send_sem.at[0], recv_sem.at[0], c, other)
    copy_main.start()
    tile(1)
    send_half[...] = nat[:, pl.ds(pl.multiple_of(512 * (1 - f), 512), 512)].astype(BF16)
    copy_half = remote(send_half, recv_half, send_sem.at[1], recv_sem.at[1], c, other)
    copy_half.start()
    total[:, own_half] = nat[:, pl.ds(pl.multiple_of(512 * f, 512), 512)]
    tile(2 * f)
    total[:, own_main] = nat[...]

    lowt = lax.dot_general(
        downt_ref[...], normed_ref[...], (((1,), (1,)), ((), ())), preferred_element_type=F32
    ).astype(BF16)
    lowt_ref[...] = lowt
    nat[...] = ADAPTER_SCALE * lax.dot_general(
        lowt, up_ref[...], (((0,), (0,)), ((), ())), preferred_element_type=F32
    )

    copy_main.wait()
    total[:, own_main] += recv_main[...].astype(F32)
    copy_half.wait()
    total[:, own_half] += recv_half[...].astype(F32)

    cosine, sine = cos_ref[...], sin_ref[...]

    def rotate(v):
        return v * cosine + pltpu.roll(v, 64, 1) * sine

    for h in range(8):
        s = slice(128 * h, 128 * h + 128)
        q_ref[:, s] = (rotate(total[:, s] + nat[:, s]) * QUERY_SCALE).astype(BF16)
    for h in range(2):
        kv_ref[h, :, 0:128] = rotate(total[:, 1024 + 128 * h : 1152 + 128 * h]).astype(BF16)
        kv_ref[h, :, 128:256] = total[:, 1280 + 128 * h : 1408 + 128 * h].astype(BF16)


def project(x, gain, codes, sq, bs, downt, up, cosine, sine, table):
    vmem = pl.BlockSpec(memory_space=pltpu.VMEM)
    return pl.pallas_call(
        project_kernel,
        name="project",
        out_shape=(
            jax.ShapeDtypeStruct((128, 1024), BF16),
            jax.ShapeDtypeStruct((2, 128, 256), BF16),
            jax.ShapeDtypeStruct((128, 4096), BF16),
            jax.ShapeDtypeStruct((16, 128), BF16),
        ),
        in_specs=[vmem] * 10,
        out_specs=(vmem,) * 4,
        scratch_shapes=[
            pltpu.VMEM((1024, 1024), BF16),
            pltpu.VMEM((3, 32, 1024), F32),
            pltpu.VMEM((256, 1024), BF16),
            pltpu.VMEM((128, 1024), F32),
            pltpu.VMEM((128, 1024), F32),
            pltpu.VMEM((128, 1024), BF16),
            pltpu.VMEM((128, 512), BF16),
            pltpu.VMEM((128, 1024), BF16),
            pltpu.VMEM((128, 512), BF16),
            pltpu.VMEM((128, 1536), F32),
            pltpu.SemaphoreType.DMA((2,)),
            pltpu.SemaphoreType.DMA((2,)),
        ],
        compiler_params=pltpu.CompilerParams(
            collective_id=0, has_side_effects=True, vmem_limit_bytes=VMEM_LIMIT
        ),
    )(x, gain, codes, sq, bs, downt, up, cosine, sine, table)


def gather_kernel(
    q_ref, kv_ref, do_ref, lowt_ref, ids_ref,
    qx, dox, kvg, idg, lowx,
    pair_send, pair_recv, own_sem, z_send, z_recv, zi_send, zi_recv, a_send, a_recv, ai_send, ai_recv,
    b_send, b_recv, bi_send, bi_recv,
):
    x, y, z, j, f = places()
    i = 1 - j
    u = x * i + y * j
    v = y * i + x * j

    def at(uu, vv, zz):
        return ctx_of(uu * i + vv * j, vv * i + uu * j, zz, j)

    def slot(uu, vv, zz):
        return (uu * 4 + vv) * 4 + zz

    sibling = ctx_of(x, y, z, i)
    vr, vl, vo = (v + 1) % 4, (v + 3) % 4, (v + 2) % 4
    ur, ul, uo = (u + 1) % 4, (u + 3) % 4, (u + 2) % 4
    right_v, left_v = at(u, vr, z), at(u, vl, z)
    right_u, left_u = at(ur, v, z), at(ul, v, z)

    barrier = pltpu.get_barrier_semaphore()
    peers = [sibling, right_v, left_v, right_u, left_u] + [at(u, v, (z + d) % 4) for d in (1, 2, 3)]
    for peer in peers:
        pl.semaphore_signal(barrier, inc=1, device_id=(peer, f), device_id_type=MESH)
    pl.semaphore_wait(barrier, len(peers))

    mine = slot(u, v, z)
    theirs = slot(v, u, z)
    near = pl.ds(pl.multiple_of(512 * j, 512), 512)
    far = pl.ds(pl.multiple_of(512 * i, 512), 512)
    pairs = [
        (kv_ref.at[i], kvg.at[theirs, j]),
        (ids_ref, idg.at[theirs, j]),
        (q_ref.at[:, far], qx.at[j]),
        (do_ref.at[:, far], dox.at[j]),
        (lowt_ref, lowx.at[j]),
    ]
    sent = []
    for n, (src, dst) in enumerate(pairs):
        copy = remote(src, dst, pair_send.at[n], pair_recv.at[n], sibling, f)
        copy.start()
        sent.append(copy)
    own = [
        (kv_ref.at[j], kvg.at[mine, j]),
        (ids_ref, idg.at[mine, j]),
        (q_ref.at[:, near], qx.at[j]),
        (do_ref.at[:, near], dox.at[j]),
        (lowt_ref, lowx.at[j]),
    ]
    local = []
    for n, (src, dst) in enumerate(own):
        copy = pltpu.make_async_copy(src, dst, own_sem.at[n])
        copy.start()
        local.append(copy)

    def arrived(ref, send, recv):
        remote(ref, ref, send, recv, sibling, f).wait_recv()

    arrived(kvg.at[mine, i], pair_send.at[0], pair_recv.at[0])
    arrived(idg.at[mine, i], pair_send.at[1], pair_recv.at[1])
    local[0].wait()
    local[1].wait()

    for d in (1, 2, 3):
        peer = at(u, v, (z + d) % 4)
        for ref, send, recv in ((kvg, z_send, z_recv), (idg, zi_send, zi_recv)):
            copy = remote(ref.at[mine], ref.at[mine], send.at[d - 1], recv.at[d - 1], peer, f)
            copy.start()
            sent.append(copy)
    for d in (1, 2, 3):
        source = slot(u, v, (z + 4 - d) % 4)
        arrived(kvg.at[source], z_send.at[d - 1], z_recv.at[d - 1])
        arrived(idg.at[source], zi_send.at[d - 1], zi_recv.at[d - 1])

    def half(vv, h):
        return pl.ds(slot(u, vv, 0) + 2 * h, 2)

    def whole(vv):
        return pl.ds(slot(u, vv, 0), 4)

    def piece(uu, vv):
        return pl.ds(slot(uu, vv, 0), 4)

    def push(part, n, send, recv, peer, ref=kvg):
        copy = remote(ref.at[part], ref.at[part], send.at[n], recv.at[n], peer, f)
        copy.start()
        sent.append(copy)

    def got(part, n, send, recv, ref=kvg):
        arrived(ref.at[part], send.at[n], recv.at[n])

    push(half(v, 0), 0, a_send, a_recv, right_v)
    push(half(v, 1), 3, a_send, a_recv, left_v)
    push(half(v, 1), 1, a_send, a_recv, right_v)
    push(half(v, 0), 4, a_send, a_recv, left_v)
    push(whole(v), 0, ai_send, ai_recv, right_v, idg)
    push(whole(v), 1, ai_send, ai_recv, left_v, idg)
    push(piece(u, v), 0, b_send, b_recv, right_u)
    push(piece(u, v), 4, b_send, b_recv, left_u)
    got(half(vl, 0), 0, a_send, a_recv)
    push(half(vl, 0), 2, a_send, a_recv, right_v)
    got(half(vr, 1), 3, a_send, a_recv)
    push(half(vr, 1), 5, a_send, a_recv, left_v)
    got(half(vl, 1), 1, a_send, a_recv)
    got(whole(vl), 0, ai_send, ai_recv, idg)
    push(whole(vl), 2, ai_send, ai_recv, right_v, idg)
    push(piece(u, vl), 1, b_send, b_recv, right_u)
    push(piece(u, vl), 5, b_send, b_recv, left_u)
    got(half(vr, 0), 4, a_send, a_recv)
    got(whole(vr), 1, ai_send, ai_recv, idg)
    push(piece(u, vr), 2, b_send, b_recv, right_u)
    push(piece(u, vr), 6, b_send, b_recv, left_u)
    got(half(vo, 0), 2, a_send, a_recv)
    got(half(vo, 1), 5, a_send, a_recv)
    got(whole(vo), 2, ai_send, ai_recv, idg)
    push(piece(u, vo), 3, b_send, b_recv, right_u)
    push(piece(u, vo), 7, b_send, b_recv, left_u)

    def all_of(uu):
        return pl.ds(slot(uu, 0, 0), 16)

    push(all_of(u), 0, bi_send, bi_recv, right_u, idg)
    push(all_of(u), 1, bi_send, bi_recv, left_u, idg)

    got(piece(ul, v), 0, b_send, b_recv)
    push(piece(ul, v), 8, b_send, b_recv, right_u)
    got(piece(ul, vl), 1, b_send, b_recv)
    push(piece(ul, vl), 9, b_send, b_recv, right_u)
    got(piece(ur, vr), 6, b_send, b_recv)
    push(piece(ur, vr), 10, b_send, b_recv, left_u)
    got(piece(ur, vo), 7, b_send, b_recv)
    push(piece(ur, vo), 11, b_send, b_recv, left_u)
    got(all_of(ul), 0, bi_send, bi_recv, idg)
    push(all_of(ul), 2, bi_send, bi_recv, right_u, idg)
    got(all_of(ur), 1, bi_send, bi_recv, idg)
    got(piece(ul, vr), 2, b_send, b_recv)
    got(piece(ul, vo), 3, b_send, b_recv)
    got(piece(ur, v), 4, b_send, b_recv)
    got(piece(ur, vl), 5, b_send, b_recv)
    got(piece(uo, v), 8, b_send, b_recv)
    got(piece(uo, vl), 9, b_send, b_recv)
    got(piece(uo, vr), 10, b_send, b_recv)
    got(piece(uo, vo), 11, b_send, b_recv)
    got(all_of(uo), 2, bi_send, bi_recv, idg)

    arrived(qx.at[i], pair_send.at[2], pair_recv.at[2])
    arrived(dox.at[i], pair_send.at[3], pair_recv.at[3])
    arrived(lowx.at[i], pair_send.at[4], pair_recv.at[4])
    for copy in local[2:]:
        copy.wait()
    for copy in sent:
        copy.wait_send()


def gather(q, kv, do, lowt, ids):
    vmem = pl.BlockSpec(memory_space=pltpu.VMEM)
    hbm = pl.BlockSpec(memory_space=pl.ANY)
    dma = pltpu.SemaphoreType.DMA
    counts = (5, 5, 5, 3, 3, 3, 3, 6, 6, 3, 3, 12, 12, 3, 3)
    return pl.pallas_call(
        gather_kernel,
        name="gather",
        out_shape=(
            jax.ShapeDtypeStruct((2, 128, 512), BF16),
            jax.ShapeDtypeStruct((2, 128, 512), BF16),
            jax.ShapeDtypeStruct((64, 2, 128, 256), BF16),
            jax.ShapeDtypeStruct((64, 2, 8, 128), I32),
            jax.ShapeDtypeStruct((2, 16, 128), BF16),
        ),
        in_specs=[vmem] * 5,
        out_specs=(hbm,) * 5,
        scratch_shapes=[dma((n,)) for n in counts],
        compiler_params=pltpu.CompilerParams(
            collective_id=1, has_side_effects=True, vmem_limit_bytes=VMEM_LIMIT
        ),
    )(q, kv, do, lowt, ids)


def attend_kernel(
    qx_ref, dox_ref, kvg_ref, idg_ref, cos_ref, sin_ref, ox_ref, glx_ref, qt, dot_, run_max, run_sum, acc, acc2
):
    x, y, z, j, _ = places()
    chip = (x * 4 + y) * 4 + z

    def slot(number):
        a, b, d = number // 16, (number // 4) % 4, number % 4
        return jnp.where(j == 0, (a * 4 + b) * 4 + d, (b * 4 + a) * 4 + d)

    here = slot(chip)
    ids = jnp.concatenate([idg_ref[here, 0, 0:1, :], idg_ref[here, 1, 0:1, :]], axis=1)
    every = idg_ref[...].reshape(128, 8, 128)
    start = jnp.zeros((1, 256), I32)
    for d in (1, 2, 3):
        below = jnp.sum(jnp.sum(jnp.where(every < d, 1, 0), axis=0), axis=1, keepdims=True)[0:1, :]
        start = jnp.where(ids == d, below, start)
    first = jnp.min(start) // 256
    position = chip * 256 + lax.broadcasted_iota(I32, (1, 256), 1)

    for g in range(4):
        lanes = slice(128 * g, 128 * g + 128)
        for b in range(2):
            cols = slice(256 * g + 128 * b, 256 * g + 128 * b + 128)
            qt[:, cols] = qx_ref[b, :, lanes].T
            dot_[:, cols] = dox_ref[b, :, lanes].T
    run_max[...] = jnp.full_like(run_max, -1e29)
    run_sum[...] = jnp.zeros_like(run_sum)
    acc[...] = jnp.zeros_like(acc)
    acc2[...] = jnp.zeros_like(acc2)

    def chunk(number, carry):
        at = slot(number)
        kv = jnp.concatenate([kvg_ref[at, 0], kvg_ref[at, 1]], axis=0)
        kvt = kv.T
        keys, values = kv[:, :128], kv[:, 128:]
        key_pos = number * 256 + lax.broadcasted_iota(I32, (256, 256), 0)
        allowed = (key_pos >= start) & (key_pos <= position)
        for g in range(4):
            cols = slice(256 * g, 256 * g + 256)
            scores = jnp.dot(keys, qt[:, cols], preferred_element_type=F32)
            scores = jnp.where(allowed, scores, -1e30)
            old = run_max[g, 0:1, :]
            new = jnp.maximum(old, jnp.max(scores, axis=0, keepdims=True))
            expo = jnp.exp2(scores - new)
            decay = jnp.exp2(old - new)
            run_max[g, 0:1, :] = new
            run_sum[g, 0:1, :] = run_sum[g, 0:1, :] * decay + jnp.sum(expo, axis=0, keepdims=True)
            grad_dots = jnp.dot(values, dot_[:, cols], preferred_element_type=F32)
            weighted = (expo * grad_dots).astype(BF16)
            acc[:, cols] = acc[:, cols] * decay + jnp.dot(kvt, expo.astype(BF16), preferred_element_type=F32)
            acc2[:, cols] = acc2[:, cols] * decay + jnp.dot(kvt[:128], weighted, preferred_element_type=F32)
        return carry

    lax.fori_loop(first, chip + 1, chunk, 0)

    cosine, sine = cos_ref[...], sin_ref[...]
    for g in range(4):
        cols = slice(256 * g, 256 * g + 256)
        lanes = slice(128 * g, 128 * g + 128)
        inverse = 1.0 / run_sum[g, 0:1, :]
        out = acc[128:256, cols] * inverse
        mean_dot = jnp.sum(dot_[:, cols].astype(F32) * out, axis=0, keepdims=True)
        grad = (acc2[:, cols] - mean_dot * acc[0:128, cols]) * (inverse * SOFT_SCALE)
        ga, gb = grad[:64], grad[64:]
        back = jnp.concatenate([ga * cosine + gb * sine, gb * cosine - ga * sine], axis=0)
        for b in range(2):
            ox_ref[b, :, lanes] = out[:, 128 * b : 128 * b + 128].T.astype(BF16)
            glx_ref[b, :, lanes] = back[:, 128 * b : 128 * b + 128].T.astype(BF16)


def attend(qx, dox, kvg, idg, cosine, sine):
    vmem = pl.BlockSpec(memory_space=pltpu.VMEM)
    return pl.pallas_call(
        attend_kernel,
        name="attend",
        out_shape=(jax.ShapeDtypeStruct((2, 128, 512), BF16), jax.ShapeDtypeStruct((2, 128, 512), BF16)),
        in_specs=[vmem] * 6,
        out_specs=(vmem, vmem),
        scratch_shapes=[
            pltpu.VMEM((128, 1024), BF16),
            pltpu.VMEM((128, 1024), BF16),
            pltpu.VMEM((4, 8, 256), F32),
            pltpu.VMEM((4, 8, 256), F32),
            pltpu.VMEM((256, 1024), F32),
            pltpu.VMEM((128, 1024), F32),
        ],
        compiler_params=pltpu.CompilerParams(vmem_limit_bytes=VMEM_LIMIT),
    )(qx, dox, kvg, idg, cosine, sine)


def reduce_kernel(
    ox_ref, glx_ref, lowx_ref, normed_ref, up_ref,
    attn_ref, grad_at_ref, up_out_ref,
    mid_send, mid_recv, buf, rcore, b1, rx, b2, ry, b3, rz, final,
    p_send, p_recv, x_send, x_recv, y_send, y_recv, z_send, z_recv,
    gy_send, gy_recv, gx_send, gx_recv,
):
    x, y, z, j, f = places()
    i = 1 - j
    sibling = ctx_of(x, y, z, i)
    xs = [(x + d) % 4 for d in (1, 2, 3)]
    ys = [(y + d) % 4 for d in (1, 2, 3)]
    whole_z = f * 4 + z
    zs = [(whole_z + d) % 8 for d in range(1, 8)]

    barrier = pltpu.get_barrier_semaphore()
    peers = [(sibling, f)]
    peers += [(ctx_of(p, y, z, j), f) for p in xs]
    peers += [(ctx_of(x, p, z, j), f) for p in ys]
    peers += [(ctx_of(x, y, p % 4, j), p // 4) for p in zs]
    for peer in peers:
        pl.semaphore_signal(barrier, inc=1, device_id=peer, device_id_type=MESH)

    glx = jnp.concatenate([glx_ref[0], glx_ref[1]], axis=0)
    up = up_ref[:, pl.ds(pl.multiple_of(512 * j, 512), 512)]
    midt = ADAPTER_SCALE * lax.dot_general(
        up, glx, (((1,), (1,)), ((), ())), preferred_element_type=F32
    )
    mid_send[0] = midt[:, 0:128]
    mid_send[1] = midt[:, 128:256]
    pl.semaphore_wait(barrier, len(peers))

    sent = []
    mid_copy = remote(mid_send.at[i], mid_recv, p_send.at[0], p_recv.at[0], sibling, f)
    mid_copy.start()
    near = pl.ds(pl.multiple_of(512 * j, 512), 512)
    out_copy = remote(ox_ref.at[i], attn_ref.at[:, near], p_send.at[1], p_recv.at[1], sibling, f)
    out_copy.start()
    attn_ref[:, near] = ox_ref[j]

    lowt = jnp.concatenate([lowx_ref[0], lowx_ref[1]], axis=1)
    upg = ADAPTER_SCALE * jnp.dot(lowt, glx, preferred_element_type=F32)
    buf[64:96] = jnp.zeros((32, 8, 128), F32)
    for s in range(2):
        for t in range(4):
            buf[64 + 16 * s + 8 * f + 4 * j + t] = upg[8 * s : 8 * s + 8, 128 * t : 128 * t + 128]
    mid_copy.wait()
    mid = (mid_send[j] + mid_recv[...]).astype(BF16)
    for t in range(4):
        part = jnp.dot(mid, normed_ref[:, 1024 * t : 1024 * t + 1024], preferred_element_type=F32)
        for s in range(2):
            for w in range(8):
                buf[32 * s + 8 * t + w] = part[8 * s : 8 * s + 8, 128 * w : 128 * w + 128]

    core_copy = remote(buf.at[pl.ds(48 * i, 48)], rcore, p_send.at[2], p_recv.at[2], sibling, f)
    core_copy.start()
    core_copy.wait()
    b1[...] = buf[pl.ds(48 * j, 48)] + rcore[...]
    copies = []
    for n, p in enumerate(xs):
        copy = remote(b1.at[pl.ds(12 * p, 12)], rx.at[n], x_send.at[n], x_recv.at[n], ctx_of(p, y, z, j), f)
        copy.start()
        copies.append(copy)
    for copy in copies:
        copy.wait()
    b2[...] = b1[pl.ds(12 * x, 12)] + rx[0] + rx[1] + rx[2]
    copies = []
    for n, p in enumerate(ys):
        copy = remote(b2.at[pl.ds(3 * p, 3)], ry.at[n], y_send.at[n], y_recv.at[n], ctx_of(x, p, z, j), f)
        copy.start()
        copies.append(copy)
    for copy in copies:
        copy.wait()
    b3[...] = b2[pl.ds(3 * y, 3)] + ry[0] + ry[1] + ry[2]
    copies = []
    for n, p in enumerate(zs):
        copy = remote(b3, rz.at[whole_z], z_send.at[n], z_recv.at[n], ctx_of(x, y, p % 4, j), p // 4)
        copy.start()
        copies.append(copy)
    rz[whole_z] = b3[...]
    for n, copy in enumerate(copies):
        source = (whole_z + 7 - n) % 8
        remote(rz.at[source], rz.at[source], z_send.at[n], z_recv.at[n], sibling, f).wait_recv()
    added = rz[0]
    for n in range(1, 8):
        added = added + rz[n]
    row = 48 * j + 12 * x + 3 * y
    final[pl.ds(row, 3)] = added
    sent += copies

    for n, p in enumerate(ys):
        part = final.at[pl.ds(row, 3)]
        copy = remote(part, part, gy_send.at[n], gy_recv.at[n], ctx_of(x, p, z, j), f)
        copy.start()
        sent.append(copy)
    for n in range(3):
        part = final.at[pl.ds(48 * j + 12 * x + 3 * ((y + 3 - n) % 4), 3)]
        remote(part, part, gy_send.at[n], gy_recv.at[n], sibling, f).wait_recv()
    for n, p in enumerate(xs):
        part = final.at[pl.ds(48 * j + 12 * x, 12)]
        copy = remote(part, part, gx_send.at[n], gx_recv.at[n], ctx_of(p, y, z, j), f)
        copy.start()
        sent.append(copy)
    for n in range(3):
        part = final.at[pl.ds(48 * j + 12 * ((x + 3 - n) % 4), 12)]
        remote(part, part, gx_send.at[n], gx_recv.at[n], sibling, f).wait_recv()
    part = final.at[pl.ds(48 * j, 48)]
    copy = remote(part, part, p_send.at[3], p_recv.at[3], sibling, f)
    copy.start()
    sent.append(copy)
    part = final.at[pl.ds(48 * i, 48)]
    remote(part, part, p_send.at[3], p_recv.at[3], sibling, f).wait_recv()

    for s in range(2):
        for t in range(32):
            grad_at_ref[8 * s : 8 * s + 8, 128 * t : 128 * t + 128] = final[32 * s + t]
        for t in range(8):
            up_out_ref[8 * s : 8 * s + 8, 128 * t : 128 * t + 128] = final[64 + 16 * s + 8 * f + t]

    other_half = attn_ref.at[:, pl.ds(pl.multiple_of(512 * i, 512), 512)]
    remote(ox_ref.at[i], other_half, p_send.at[1], p_recv.at[1], sibling, f).wait_recv()
    out_copy.wait_send()
    for copy in sent:
        copy.wait_send()


def reduce_all(ox, glx, lowx, normed, up):
    vmem = pl.BlockSpec(memory_space=pltpu.VMEM)
    hbm = pl.BlockSpec(memory_space=pl.ANY)
    dma = pltpu.SemaphoreType.DMA
    tiles = lambda *lead: pltpu.VMEM((*lead, 8, 128), F32)
    return pl.pallas_call(
        reduce_kernel,
        name="reduce_all",
        out_shape=(
            jax.ShapeDtypeStruct((128, 1024), BF16),
            jax.ShapeDtypeStruct((16, 4096), F32),
            jax.ShapeDtypeStruct((16, 1024), F32),
        ),
        in_specs=[vmem] * 5,
        out_specs=(vmem, vmem, vmem),
        scratch_shapes=[
            pltpu.VMEM((2, 16, 128), F32),
            pltpu.VMEM((16, 128), F32),
            tiles(96), tiles(48), tiles(48), tiles(3, 12), tiles(12), tiles(3, 3), tiles(3), tiles(8, 3),
            tiles(96),
        ]
        + [dma((n,)) for n in (4, 4, 3, 3, 3, 3, 7, 7, 3, 3, 3, 3)],
        compiler_params=pltpu.CompilerParams(
            collective_id=2, has_side_effects=True, vmem_limit_bytes=VMEM_LIMIT
        ),
    )(ox, glx, lowx, normed, up)


def on_device(
    layer_input,
    gain,
    codes,
    column_scale_quantized,
    block_second_scale,
    query_down_map,
    query_up_map,
    token_document,
    output_cotangent,
):
    place = lax.axis_index("ctx")
    chip = place // 2
    freqs = jnp.exp(jnp.arange(HEAD // 2, dtype=F32) * (-2.0 * math.log(ROPE_BASE) / HEAD))
    chip_positions = (chip * 256 + jnp.arange(256, dtype=I32)).astype(F32)
    angle_t = freqs[:, None] * chip_positions[None, :]
    cos_t, sin_t = jnp.cos(angle_t), jnp.sin(angle_t)
    cosine = lax.dynamic_slice_in_dim(cos_t, (place % 2) * 128, 128, 1).T
    sine = lax.dynamic_slice_in_dim(sin_t, (place % 2) * 128, 128, 1).T
    cosine = jnp.concatenate([cosine, cosine], axis=1)
    sine = jnp.concatenate([-sine, sine], axis=1)
    table = jnp.asarray(NF4_LEVELS * 8, F32)[None, :]
    ids = jnp.broadcast_to(token_document[None, :], (8, 128))

    q, kv, normed, lowt = project(
        layer_input,
        gain[None, :],
        codes,
        column_scale_quantized,
        block_second_scale[:, None],
        query_down_map.T,
        query_up_map,
        cosine,
        sine,
        table,
    )
    qx, dox, kvg, idg, lowx = gather(q, kv, output_cotangent, lowt, ids)
    ox, glx = attend(qx, dox, kvg, idg, cos_t, sin_t)
    attn, grad_at, up_map_gradient = reduce_all(ox, glx, lowx, normed, query_up_map)
    return (attn, grad_at.T, up_map_gradient)


def solution(mesh):
    return jax.shard_map(
        on_device,
        mesh=mesh,
        in_specs=(
            P("ctx", None),
            P(),
            P("fsdp", None),
            P("fsdp", None),
            P(),
            P(),
            P(None, "fsdp"),
            P("ctx"),
            P("ctx", "fsdp"),
        ),
        out_specs=(P("ctx", "fsdp"), P(), P(None, "fsdp")),
        check_vma=False,
    )
```

```python
import functools
import math

import jax
import jax.numpy as jnp
from jax import lax
from jax.experimental import pallas as pl
from jax.experimental.pallas import tpu as pltpu
from jax.sharding import PartitionSpec as P

MESH = pl.DeviceIdType.MESH
HEAD = 128
NF4_LEVELS = [
    -1.0,
    -0.6961928009986877,
    -0.5250730514526367,
    -0.39491748809814453,
    -0.28444138169288635,
    -0.18477343022823334,
    -0.09105003625154495,
    0.0,
    0.07958029955625534,
    0.16093020141124725,
    0.24611230194568634,
    0.33791524171829224,
    0.44070982933044434,
    0.5626170039176941,
    0.7229568362236023,
    1.0,
]
ADAPTER_SCALE = 2.0
ROPE_BASE = 500000.0
SOFT_SCALE = 1.0 / math.sqrt(HEAD)
QUERY_SCALE = SOFT_SCALE * math.log2(math.e)
F32, BF16, I32 = jnp.float32, jnp.bfloat16, jnp.int32
VMEM_LIMIT = 60 * 1024 * 1024


def places():
    c = lax.axis_index("ctx")
    f = lax.axis_index("fsdp")
    return c // 32, (c // 8) % 4, (c // 2) % 4, c % 2, f


def ctx_of(x, y, z, j):
    return ((x * 4 + y) * 4 + z) * 2 + j


def pair_of(x, y, z, j):
    return ctx_of(3 - x, 3 - y, (z + 2) % 4, j)


def lookup(table, index):
    return lax.gather(
        table,
        index[..., None],
        lax.GatherDimensionNumbers(
            offset_dims=(),
            collapsed_slice_dims=(1,),
            start_index_map=(1,),
            operand_batching_dims=(0,),
            start_indices_batching_dims=(0,),
        ),
        slice_sizes=(1, 1),
        mode=lax.GatherScatterMode.PROMISE_IN_BOUNDS,
    )


def remote(src, dst, send, recv, ctx, f):
    return pltpu.make_async_remote_copy(
        src_ref=src, dst_ref=dst, send_sem=send, recv_sem=recv, device_id=(ctx, f), device_id_type=MESH
    )


def project_kernel(
    x_ref, gain_ref, codes_ref, sq_ref, bs_ref, downt_ref, up_ref, cos_ref, sin_ref, table_ref, doc_ref, do_ref,
    q_ref, kv_ref, normed_ref, lowt_ref, ids_ref, dox,
    perm, scale, w_buf, acc, nat, send_main, send_half, recv_main, recv_half, total, send_sem, recv_sem,
):
    x, y, z, j, f = places()
    c = lax.axis_index("ctx")
    other = 1 - f
    pair = pair_of(x, y, z, j)
    k = z // 2
    barrier = pltpu.get_barrier_semaphore()
    pl.semaphore_signal(barrier, inc=1, device_id=(c, other), device_id_type=MESH)
    pl.semaphore_signal(barrier, inc=1, device_id=(pair, f), device_id_type=MESH)

    wide = x_ref[...].astype(F32)
    inverse = lax.rsqrt(jnp.mean(wide * wide, axis=-1, keepdims=True) + 1e-05)
    normed_ref[...] = (wide * inverse * gain_ref[...]).astype(BF16)
    ids_ref[...] = jnp.broadcast_to(doc_ref[...], (8, 128))
    dox[0] = do_ref[:, pl.ds(pl.multiple_of(512 * k, 512), 512)]

    pl.semaphore_wait(barrier, 2)
    far = pl.ds(pl.multiple_of(512 * (1 - k), 512), 512)
    copy_do = remote(do_ref.at[:, far], dox.at[1], send_sem.at[2], recv_sem.at[2], pair, f)
    copy_do.start()

    for part in range(8):
        m = lax.broadcasted_iota(I32, (128, 1024), 0)
        k = lax.broadcasted_iota(I32, (128, 1024), 1)
        perm[128 * part : 128 * part + 128, :] = jnp.where(k == 8 * m + part, 1.0, 0.0).astype(BF16)
    pick = lax.broadcasted_iota(I32, (32, 64), 1) == lax.broadcasted_iota(I32, (32, 64), 0) + 32 * f
    second = jnp.sum(jnp.where(pick, bs_ref[...], 0.0), axis=1, keepdims=True) * (1.0 / 256.0)
    for t in range(3):
        quantized = (sq_ref[:, 1024 * t : 1024 * t + 1024].astype(F32) + 1.0).astype(BF16)
        packed = lax.dot_general(quantized, perm[...], (((1,), (1,)), ((), ())), preferred_element_type=F32)
        scale[t] = packed * second

    table = jnp.broadcast_to(table_ref[...], (64, 128))

    def tile(t):
        lane = pl.multiple_of(t * 128, 128)
        acc[...] = jnp.zeros_like(acc)

        def chunk(kc, carry):
            for b in range(4):
                row = pl.multiple_of(kc * 256 + b * 64, 64)
                words = codes_ref[pl.ds(row, 64), pl.ds(lane, 128)]
                scale_row = scale[t, pl.ds(kc * 4 + b, 1), :]
                for n in range(8):
                    index = jnp.bitwise_and(jnp.right_shift(words, 4 * n), 15)
                    levels = lookup(table, index)
                    w_buf[64 * b : 64 * b + 64, 128 * n : 128 * n + 128] = (
                        levels * scale_row[:, 128 * n : 128 * n + 128]
                    ).astype(BF16)
            col = pl.multiple_of(f * 2048 + kc * 256, 256)
            acc[...] += jnp.dot(normed_ref[:, pl.ds(col, 256)], w_buf[...], preferred_element_type=F32)
            return carry

        lax.fori_loop(0, 8, chunk, 0)
        full = acc[...]
        high = full.astype(BF16)
        low = (full - high.astype(F32)).astype(BF16)
        nat[...] = jnp.dot(high, perm[...], preferred_element_type=F32) + jnp.dot(
            low, perm[...], preferred_element_type=F32
        )

    own_main = pl.ds(pl.multiple_of(512 * f, 512), 1024)
    own_half = pl.ds(pl.multiple_of(1024 * (1 - f), 512), 512)

    tile(2 * (1 - f))
    send_main[...] = nat[...].astype(BF16)
    copy_main = remote(send_main, recv_main, send_sem.at[0], recv_sem.at[0], c, other)
    copy_main.start()
    tile(1)
    send_half[...] = nat[:, pl.ds(pl.multiple_of(512 * (1 - f), 512), 512)].astype(BF16)
    copy_half = remote(send_half, recv_half, send_sem.at[1], recv_sem.at[1], c, other)
    copy_half.start()
    total[:, own_half] = nat[:, pl.ds(pl.multiple_of(512 * f, 512), 512)]
    tile(2 * f)
    total[:, own_main] = nat[...]

    lowt = lax.dot_general(
        downt_ref[...], normed_ref[...], (((1,), (1,)), ((), ())), preferred_element_type=F32
    ).astype(BF16)
    lowt_ref[...] = lowt
    nat[...] = ADAPTER_SCALE * lax.dot_general(
        lowt, up_ref[...], (((0,), (0,)), ((), ())), preferred_element_type=F32
    )

    copy_main.wait()
    total[:, own_main] += recv_main[...].astype(F32)
    copy_half.wait()
    total[:, own_half] += recv_half[...].astype(F32)

    cosine, sine = cos_ref[0].T, sin_ref[0].T
    cosine = jnp.concatenate([cosine, cosine], axis=1)
    sine = jnp.concatenate([-sine, sine], axis=1)

    def rotate(v):
        return v * cosine + pltpu.roll(v, 64, 1) * sine

    for h in range(8):
        s = slice(128 * h, 128 * h + 128)
        q_ref[:, s] = (rotate(total[:, s] + nat[:, s]) * QUERY_SCALE).astype(BF16)
    for h in range(2):
        kv_ref[h, :, 0:128] = rotate(total[:, 1024 + 128 * h : 1152 + 128 * h]).astype(BF16)
        kv_ref[h, :, 128:256] = total[:, 1280 + 128 * h : 1408 + 128 * h].astype(BF16)
    copy_do.wait()


def project(x, gain, codes, sq, bs, downt, up, cosine, sine, table, doc, do):
    vmem = pl.BlockSpec(memory_space=pltpu.VMEM)
    return pl.pallas_call(
        project_kernel,
        name="project",
        out_shape=(
            jax.ShapeDtypeStruct((128, 1024), BF16),
            jax.ShapeDtypeStruct((2, 128, 256), BF16),
            jax.ShapeDtypeStruct((128, 4096), BF16),
            jax.ShapeDtypeStruct((16, 128), BF16),
            jax.ShapeDtypeStruct((8, 128), I32),
            jax.ShapeDtypeStruct((2, 128, 512), BF16),
        ),
        in_specs=[vmem] * 12,
        out_specs=(vmem,) * 6,
        scratch_shapes=[
            pltpu.VMEM((1024, 1024), BF16),
            pltpu.VMEM((3, 32, 1024), F32),
            pltpu.VMEM((256, 1024), BF16),
            pltpu.VMEM((128, 1024), F32),
            pltpu.VMEM((128, 1024), F32),
            pltpu.VMEM((128, 1024), BF16),
            pltpu.VMEM((128, 512), BF16),
            pltpu.VMEM((128, 1024), BF16),
            pltpu.VMEM((128, 512), BF16),
            pltpu.VMEM((128, 1536), F32),
            pltpu.SemaphoreType.DMA((3,)),
            pltpu.SemaphoreType.DMA((3,)),
        ],
        compiler_params=pltpu.CompilerParams(
            collective_id=0, has_side_effects=True, vmem_limit_bytes=VMEM_LIMIT
        ),
    )(x, gain, codes, sq, bs, downt, up, cosine, sine, table, doc, do)


def gather_kernel(
    q_ref, kv_ref, lowt_ref, ids_ref,
    qx, kvg, idg, lowx,
    e_send, e_recv, own_sem, z_send, z_recv, zi_send, zi_recv, a_send, a_recv, ai_send, ai_recv,
    b_send, b_recv, bi_send, bi_recv, s_send, s_recv,
):
    x, y, z, j, f = places()
    i = 1 - j
    k = z // 2
    u = x * i + y * j
    v = y * i + x * j

    def at(uu, vv, zz):
        return ctx_of(uu * i + vv * j, vv * i + uu * j, zz, j)

    def slot(uu, vv, zz):
        return (uu * 4 + vv) * 4 + zz

    sibling = ctx_of(x, y, z, i)
    pair = pair_of(x, y, z, j)
    zo = (z + 2) % 4
    zn = z + 1 - 2 * (z % 2)
    zf = (zn + 2) % 4
    across, next_z, far_z = at(u, v, zo), at(u, v, zn), at(u, v, zf)
    vr, vl, vo = (v + 1) % 4, (v + 3) % 4, (v + 2) % 4
    ur, ul, uo = (u + 1) % 4, (u + 3) % 4, (u + 2) % 4
    right_v, left_v = at(u, vr, z), at(u, vl, z)
    right_u, left_u = at(ur, v, z), at(ul, v, z)

    barrier = pltpu.get_barrier_semaphore()
    peers = [sibling, pair, across, next_z, far_z, right_v, left_v, right_u, left_u]
    for peer in peers:
        pl.semaphore_signal(barrier, inc=1, device_id=(peer, f), device_id_type=MESH)
    pl.semaphore_wait(barrier, len(peers))

    sent = []

    def push(src, dst, n, send, recv, peer):
        copy = remote(src, dst, send.at[n], recv.at[n], peer, f)
        copy.start()
        sent.append(copy)

    def got(ref, n, send, recv):
        remote(ref, ref, send.at[n], recv.at[n], sibling, f).wait_recv()

    mine = slot(u, v, z)
    near = pl.ds(pl.multiple_of(512 * k, 512), 512)
    far = pl.ds(pl.multiple_of(512 * (1 - k), 512), 512)
    push(kv_ref.at[1 - k], kvg.at[j, mine], 0, e_send, e_recv, across)
    push(kv_ref.at[k], kvg.at[j, mine], 0, z_send, z_recv, next_z)
    for n, peer in enumerate((next_z, across, far_z)):
        push(ids_ref, idg.at[j, mine], n, zi_send, zi_recv, peer)
    push(q_ref.at[:, far], qx.at[1], 1, e_send, e_recv, pair)
    push(lowt_ref, lowx.at[1], 2, e_send, e_recv, pair)
    local = []
    for n, (src, dst) in enumerate(
        (
            (kv_ref.at[k], kvg.at[j, mine]),
            (ids_ref, idg.at[j, mine]),
            (q_ref.at[:, near], qx.at[0]),
            (lowt_ref, lowx.at[0]),
        )
    ):
        copy = pltpu.make_async_copy(src, dst, own_sem.at[n])
        copy.start()
        local.append(copy)

    second = kvg.at[j, slot(u, v, zo)]
    got(second, 0, e_send, e_recv)
    push(second, second, 1, z_send, z_recv, next_z)
    got(kvg.at[j, slot(u, v, zn)], 0, z_send, z_recv)
    for n, zz in enumerate((zn, zo, zf)):
        got(idg.at[j, slot(u, v, zz)], n, zi_send, zi_recv)
    local[0].wait()
    local[1].wait()
    got(kvg.at[j, slot(u, v, zf)], 1, z_send, z_recv)

    def half(vv, h):
        return kvg.at[j, pl.ds(slot(u, vv, 0) + 2 * h, 2)]

    def piece(uu, vv):
        return kvg.at[j, pl.ds(slot(uu, vv, 0), 4)]

    def marks(vv):
        return idg.at[j, pl.ds(slot(u, vv, 0), 4)]

    def all_marks(uu):
        return idg.at[j, pl.ds(slot(uu, 0, 0), 16)]

    def same(part, n, send, recv, peer):
        push(part, part, n, send, recv, peer)

    shared = []

    def share(du, dv):
        part = piece((u + du) % 4, (v + dv) % 4)
        same(part, len(shared), s_send, s_recv, sibling)
        shared.append((du, dv))

    same(half(v, 0), 0, a_send, a_recv, right_v)
    same(half(v, 1), 3, a_send, a_recv, left_v)
    same(half(v, 1), 1, a_send, a_recv, right_v)
    same(half(v, 0), 4, a_send, a_recv, left_v)
    same(marks(v), 0, ai_send, ai_recv, right_v)
    same(marks(v), 1, ai_send, ai_recv, left_v)
    same(piece(u, v), 0, b_send, b_recv, right_u)
    same(piece(u, v), 4, b_send, b_recv, left_u)
    share(0, 0)
    got(half(vl, 0), 0, a_send, a_recv)
    same(half(vl, 0), 2, a_send, a_recv, right_v)
    got(half(vr, 1), 3, a_send, a_recv)
    same(half(vr, 1), 5, a_send, a_recv, left_v)
    got(half(vl, 1), 1, a_send, a_recv)
    got(marks(vl), 0, ai_send, ai_recv)
    same(marks(vl), 2, ai_send, ai_recv, right_v)
    same(piece(u, vl), 1, b_send, b_recv, right_u)
    same(piece(u, vl), 5, b_send, b_recv, left_u)
    share(0, 3)
    got(half(vr, 0), 4, a_send, a_recv)
    got(marks(vr), 1, ai_send, ai_recv)
    same(piece(u, vr), 2, b_send, b_recv, right_u)
    same(piece(u, vr), 6, b_send, b_recv, left_u)
    share(0, 1)
    got(half(vo, 0), 2, a_send, a_recv)
    got(half(vo, 1), 5, a_send, a_recv)
    got(marks(vo), 2, ai_send, ai_recv)
    same(piece(u, vo), 3, b_send, b_recv, right_u)
    same(piece(u, vo), 7, b_send, b_recv, left_u)
    share(0, 2)
    same(all_marks(u), 0, bi_send, bi_recv, right_u)
    same(all_marks(u), 1, bi_send, bi_recv, left_u)

    got(piece(ul, v), 0, b_send, b_recv)
    same(piece(ul, v), 8, b_send, b_recv, right_u)
    share(3, 0)
    got(piece(ul, vl), 1, b_send, b_recv)
    same(piece(ul, vl), 9, b_send, b_recv, right_u)
    share(3, 3)
    got(piece(ur, vr), 6, b_send, b_recv)
    same(piece(ur, vr), 10, b_send, b_recv, left_u)
    share(1, 1)
    got(piece(ur, vo), 7, b_send, b_recv)
    same(piece(ur, vo), 11, b_send, b_recv, left_u)
    share(1, 2)
    got(all_marks(ul), 0, bi_send, bi_recv)
    same(all_marks(ul), 2, bi_send, bi_recv, right_u)
    got(all_marks(ur), 1, bi_send, bi_recv)
    got(piece(ul, vr), 2, b_send, b_recv)
    share(3, 1)
    got(piece(ul, vo), 3, b_send, b_recv)
    share(3, 2)
    got(piece(ur, v), 4, b_send, b_recv)
    share(1, 0)
    got(piece(ur, vl), 5, b_send, b_recv)
    share(1, 3)
    got(all_marks(uo), 2, bi_send, bi_recv)
    same(idg.at[j], 16, s_send, s_recv, sibling)
    got(piece(uo, v), 8, b_send, b_recv)
    share(2, 0)
    got(piece(uo, vr), 10, b_send, b_recv)
    share(2, 1)
    got(piece(uo, vl), 9, b_send, b_recv)
    share(2, 3)
    got(piece(uo, vo), 11, b_send, b_recv)
    share(2, 2)

    got(qx.at[1], 1, e_send, e_recv)
    got(lowx.at[1], 2, e_send, e_recv)
    for n, (du, dv) in enumerate(shared):
        got(kvg.at[i, pl.ds(slot((v + du) % 4, (u + dv) % 4, 0), 4)], n, s_send, s_recv)
    got(idg.at[i], 16, s_send, s_recv)
    for copy in local[2:]:
        copy.wait()
    for copy in sent:
        copy.wait_send()


def gather(q, kv, lowt, ids):
    vmem = pl.BlockSpec(memory_space=pltpu.VMEM)
    hbm = pl.BlockSpec(memory_space=pl.ANY)
    dma = pltpu.SemaphoreType.DMA
    counts = (3, 3, 4, 2, 2, 3, 3, 6, 6, 3, 3, 12, 12, 3, 3, 17, 17)
    return pl.pallas_call(
        gather_kernel,
        name="gather",
        out_shape=(
            jax.ShapeDtypeStruct((2, 128, 512), BF16),
            jax.ShapeDtypeStruct((2, 64, 128, 256), BF16),
            jax.ShapeDtypeStruct((2, 64, 8, 128), I32),
            jax.ShapeDtypeStruct((2, 16, 128), BF16),
        ),
        in_specs=[vmem] * 4,
        out_specs=(hbm,) * 4,
        scratch_shapes=[dma((n,)) for n in counts],
        compiler_params=pltpu.CompilerParams(
            collective_id=1, has_side_effects=True, vmem_limit_bytes=VMEM_LIMIT
        ),
    )(q, kv, lowt, ids)


STEP = 512


def attend_kernel(
    qx_ref, dox_ref, kvg_ref, idg_ref, cos_ref, sin_ref, ox_ref, glx_ref,
    qt, dot_, limits, ahead0, ahead1, max0, max1, run_max, run_sum, acc, acc2,
):
    x, y, z, j, _ = places()
    here = ctx_of(x, y, z, j)
    there = pair_of(x, y, z, j)

    def slot(number, core):
        a, b, d = number // 16, (number // 4) % 4, number % 4
        first, second = (a * 4 + b) * 4 + d, (b * 4 + a) * 4 + d
        if isinstance(core, int):
            return second if core else first
        return jnp.where(core == 0, first, second)

    def block(number):
        return jnp.concatenate([kvg_ref[0, slot(number, 0)], kvg_ref[1, slot(number, 1)]], axis=0)

    every = idg_ref[...].reshape(128, 8, 128)
    below = [
        jnp.sum(jnp.sum(jnp.where(every < d, 1, 0), axis=0), axis=1, keepdims=True)[0:1, :] for d in (1, 2, 3)
    ]
    lane = lax.broadcasted_iota(I32, (1, 128), 1)
    for t, place in enumerate((here, there)):
        ids = idg_ref[j, slot(place // 2, j), 0:1, :]
        start = jnp.zeros((1, 128), I32)
        for d in (1, 2, 3):
            start = jnp.where(ids == d, below[d - 1], start)
        limits[t, 0:1, :] = jnp.concatenate([start, start], axis=1)
        position = place * 128 + lane
        limits[t, 1:2, :] = jnp.concatenate([position, position], axis=1)
        for g in range(4):
            lanes = slice(128 * g, 128 * g + 128)
            qt[t, :, lanes] = qx_ref[t, :, lanes].T
            dot_[t, :, lanes] = dox_ref[t, :, lanes].T
    run_max[...] = jnp.full_like(run_max, -1e29)
    run_sum[...] = jnp.zeros_like(run_sum)
    acc[...] = jnp.zeros_like(acc)
    acc2[...] = jnp.zeros_like(acc2)

    def rows(t, carry):
        place = jnp.where(t == 0, here, there)
        first = jnp.min(limits[t, 0:1, :]) // STEP
        latest = jnp.max(limits[t, 0:1, :])
        stop = (place * 128 + 127) // STEP + 1

        def scores_of(number, masked, ahead, ahead_max):
            key = jnp.minimum(number, 31) * 2
            base = number * STEP
            for h in range(2):
                keys = block(key + h)[:, :128]
                for p in range(2):
                    cols = slice(256 * p, 256 * p + 256)
                    scores = jnp.dot(keys, qt[t, :, cols], preferred_element_type=F32)
                    if masked:
                        pos = base + 256 * h + lax.broadcasted_iota(I32, (256, 256), 0)
                        allowed = (pos >= limits[t, 0:1, :]) & (pos <= limits[t, 1:2, :])
                        scores = jnp.where(allowed, scores, -1e30)
                    ahead[256 * h : 256 * h + 256, cols] = scores
                    top = jnp.max(scores, axis=0, keepdims=True)
                    ahead_max[h : h + 1, cols] = top

        def is_edge(number):
            return (number * STEP < latest) | (number * STEP + STEP - 1 > place * 128)

        def step(number, masked, ahead, ahead_max, later, later_max):
            scores_of(number + 1, masked, later, later_max)
            kv = jnp.concatenate([block(2 * number), block(2 * number + 1)], axis=0)
            kvt = kv.T
            values = kv[:, 128:]
            for p in range(2):
                cols = slice(256 * p, 256 * p + 256)
                tops = jnp.maximum(ahead_max[0:1, cols], ahead_max[1:2, cols])
                old = run_max[t, 0:1, cols]
                new = jnp.maximum(old, tops)
                decay = jnp.exp2(old - new)
                run_max[t, 0:1, cols] = new
                grad_dots = jnp.dot(values, dot_[t, :, cols], preferred_element_type=F32)
                expo = jnp.exp2(ahead[:, cols] - new)
                run_sum[t, 0:1, cols] = run_sum[t, 0:1, cols] * decay + jnp.sum(expo, axis=0, keepdims=True)
                weighted = (expo * grad_dots).astype(BF16)
                acc[t, :, cols] = acc[t, :, cols] * decay + jnp.dot(
                    kvt, expo.astype(BF16), preferred_element_type=F32
                )
                acc2[t, :, cols] = acc2[t, :, cols] * decay + jnp.dot(
                    kvt[:128], weighted, preferred_element_type=F32
                )

        scores_of(first, True, ahead0, max0)

        def one(number, *buffers):
            edge = is_edge(number + 1)

            @pl.when(edge)
            def _():
                step(number, True, *buffers)

            @pl.when(jnp.logical_not(edge))
            def _():
                step(number, False, *buffers)

        def body(twice, c):
            number = first + 2 * twice
            one(number, ahead0, max0, ahead1, max1)

            @pl.when(number + 1 < stop)
            def _():
                one(number + 1, ahead1, max1, ahead0, max0)

            return c

        lax.fori_loop(0, (stop - first + 1) // 2, body, 0)
        return carry

    lax.fori_loop(0, 2, rows, 0)

    for t in range(2):
        cosine, sine = cos_ref[t], sin_ref[t]
        for g in range(4):
            lanes = slice(128 * g, 128 * g + 128)
            inverse = 1.0 / run_sum[t, 0:1, lanes]
            out = acc[t, 128:256, lanes] * inverse
            mean_dot = jnp.sum(dot_[t, :, lanes].astype(F32) * out, axis=0, keepdims=True)
            grad = (acc2[t, :, lanes] - mean_dot * acc[t, 0:128, lanes]) * (inverse * SOFT_SCALE)
            ga, gb = grad[:64], grad[64:]
            back = jnp.concatenate([ga * cosine + gb * sine, gb * cosine - ga * sine], axis=0)
            ox_ref[t, :, lanes] = out.T.astype(BF16)
            glx_ref[t, :, lanes] = back.T.astype(BF16)


def attend(qx, dox, kvg, idg, cosine, sine):
    vmem = pl.BlockSpec(memory_space=pltpu.VMEM)
    return pl.pallas_call(
        attend_kernel,
        name="attend",
        out_shape=(jax.ShapeDtypeStruct((2, 128, 512), BF16), jax.ShapeDtypeStruct((2, 128, 512), BF16)),
        in_specs=[vmem] * 6,
        out_specs=(vmem, vmem),
        scratch_shapes=[
            pltpu.VMEM((2, 128, 512), BF16),
            pltpu.VMEM((2, 128, 512), BF16),
            pltpu.VMEM((2, 8, 256), I32),
            pltpu.VMEM((512, 512), F32),
            pltpu.VMEM((512, 512), F32),
            pltpu.VMEM((8, 512), F32),
            pltpu.VMEM((8, 512), F32),
            pltpu.VMEM((2, 8, 512), F32),
            pltpu.VMEM((2, 8, 512), F32),
            pltpu.VMEM((2, 256, 512), F32),
            pltpu.VMEM((2, 128, 512), F32),
        ],
        compiler_params=pltpu.CompilerParams(vmem_limit_bytes=VMEM_LIMIT),
    )(qx, dox, kvg, idg, cosine, sine)


def reduce_kernel(
    ox_ref, glx_ref, lowx_ref, normed_ref, up_ref,
    attn_ref, grad_at_ref, up_out_ref,
    mid_send, mid_recv, buf, rcore, b1, rx, b2, ry, b3, rz, final,
    p_send, p_recv, x_send, x_recv, y_send, y_recv, z_send, z_recv,
    gy_send, gy_recv, gx_send, gx_recv,
):
    x, y, z, j, f = places()
    i = 1 - j
    sibling = ctx_of(x, y, z, i)
    xs = [(x + d) % 4 for d in (1, 2, 3)]
    ys = [(y + d) % 4 for d in (1, 2, 3)]
    whole_z = f * 4 + z
    zs = [(whole_z + d) % 8 for d in range(1, 8)]

    pair = pair_of(x, y, z, j)
    k = z // 2
    barrier = pltpu.get_barrier_semaphore()
    peers = [(sibling, f), (pair, f)]
    peers += [(ctx_of(p, y, z, j), f) for p in xs]
    peers += [(ctx_of(x, p, z, j), f) for p in ys]
    peers += [(ctx_of(x, y, p % 4, j), p // 4) for p in zs]
    for peer in peers:
        pl.semaphore_signal(barrier, inc=1, device_id=peer, device_id_type=MESH)

    glx = jnp.concatenate([glx_ref[0], glx_ref[1]], axis=0)
    up = up_ref[:, pl.ds(pl.multiple_of(512 * k, 512), 512)]
    midt = ADAPTER_SCALE * lax.dot_general(
        up, glx, (((1,), (1,)), ((), ())), preferred_element_type=F32
    )
    mid_send[0] = midt[:, 0:128]
    mid_send[1] = midt[:, 128:256]
    pl.semaphore_wait(barrier, len(peers))

    sent = []
    mid_copy = remote(mid_send.at[1], mid_recv, p_send.at[0], p_recv.at[0], pair, f)
    mid_copy.start()
    near = pl.ds(pl.multiple_of(512 * k, 512), 512)
    out_copy = remote(ox_ref.at[1], attn_ref.at[:, near], p_send.at[1], p_recv.at[1], pair, f)
    out_copy.start()
    attn_ref[:, near] = ox_ref[0]

    lowt = jnp.concatenate([lowx_ref[0], lowx_ref[1]], axis=1)
    upg = ADAPTER_SCALE * jnp.dot(lowt, glx, preferred_element_type=F32)
    buf[64:96] = jnp.zeros((32, 8, 128), F32)
    for s in range(2):
        for t in range(4):
            buf[64 + 16 * s + 8 * f + 4 * k + t] = upg[8 * s : 8 * s + 8, 128 * t : 128 * t + 128]
    mid_copy.wait()
    mid = (mid_send[0] + mid_recv[...]).astype(BF16)
    for t in range(4):
        part = jnp.dot(mid, normed_ref[:, 1024 * t : 1024 * t + 1024], preferred_element_type=F32)
        for s in range(2):
            for w in range(8):
                buf[32 * s + 8 * t + w] = part[8 * s : 8 * s + 8, 128 * w : 128 * w + 128]

    core_copy = remote(buf.at[pl.ds(48 * i, 48)], rcore, p_send.at[2], p_recv.at[2], sibling, f)
    core_copy.start()
    core_copy.wait()
    b1[...] = buf[pl.ds(48 * j, 48)] + rcore[...]
    copies = []
    for n, p in enumerate(xs):
        copy = remote(b1.at[pl.ds(12 * p, 12)], rx.at[n], x_send.at[n], x_recv.at[n], ctx_of(p, y, z, j), f)
        copy.start()
        copies.append(copy)
    for copy in copies:
        copy.wait()
    b2[...] = b1[pl.ds(12 * x, 12)] + rx[0] + rx[1] + rx[2]
    copies = []
    for n, p in enumerate(ys):
        copy = remote(b2.at[pl.ds(3 * p, 3)], ry.at[n], y_send.at[n], y_recv.at[n], ctx_of(x, p, z, j), f)
        copy.start()
        copies.append(copy)
    for copy in copies:
        copy.wait()
    b3[...] = b2[pl.ds(3 * y, 3)] + ry[0] + ry[1] + ry[2]
    copies = []
    for n, p in enumerate(zs):
        copy = remote(b3, rz.at[whole_z], z_send.at[n], z_recv.at[n], ctx_of(x, y, p % 4, j), p // 4)
        copy.start()
        copies.append(copy)
    rz[whole_z] = b3[...]
    for n, copy in enumerate(copies):
        source = (whole_z + 7 - n) % 8
        remote(rz.at[source], rz.at[source], z_send.at[n], z_recv.at[n], sibling, f).wait_recv()
    added = rz[0]
    for n in range(1, 8):
        added = added + rz[n]
    row = 48 * j + 12 * x + 3 * y
    final[pl.ds(row, 3)] = added
    sent += copies

    for n, p in enumerate(ys):
        part = final.at[pl.ds(row, 3)]
        copy = remote(part, part, gy_send.at[n], gy_recv.at[n], ctx_of(x, p, z, j), f)
        copy.start()
        sent.append(copy)
    for n in range(3):
        part = final.at[pl.ds(48 * j + 12 * x + 3 * ((y + 3 - n) % 4), 3)]
        remote(part, part, gy_send.at[n], gy_recv.at[n], sibling, f).wait_recv()
    for n, p in enumerate(xs):
        part = final.at[pl.ds(48 * j + 12 * x, 12)]
        copy = remote(part, part, gx_send.at[n], gx_recv.at[n], ctx_of(p, y, z, j), f)
        copy.start()
        sent.append(copy)
    for n in range(3):
        part = final.at[pl.ds(48 * j + 12 * ((x + 3 - n) % 4), 12)]
        remote(part, part, gx_send.at[n], gx_recv.at[n], sibling, f).wait_recv()
    part = final.at[pl.ds(48 * j, 48)]
    copy = remote(part, part, p_send.at[3], p_recv.at[3], sibling, f)
    copy.start()
    sent.append(copy)
    part = final.at[pl.ds(48 * i, 48)]
    remote(part, part, p_send.at[3], p_recv.at[3], sibling, f).wait_recv()

    for s in range(2):
        for t in range(32):
            grad_at_ref[8 * s : 8 * s + 8, 128 * t : 128 * t + 128] = final[32 * s + t]
        for t in range(8):
            up_out_ref[8 * s : 8 * s + 8, 128 * t : 128 * t + 128] = final[64 + 16 * s + 8 * f + t]

    other_half = attn_ref.at[:, pl.ds(pl.multiple_of(512 * (1 - k), 512), 512)]
    remote(ox_ref.at[1], other_half, p_send.at[1], p_recv.at[1], sibling, f).wait_recv()
    out_copy.wait_send()
    for copy in sent:
        copy.wait_send()


def reduce_all(ox, glx, lowx, normed, up):
    vmem = pl.BlockSpec(memory_space=pltpu.VMEM)
    hbm = pl.BlockSpec(memory_space=pl.ANY)
    dma = pltpu.SemaphoreType.DMA
    tiles = lambda *lead: pltpu.VMEM((*lead, 8, 128), F32)
    return pl.pallas_call(
        reduce_kernel,
        name="reduce_all",
        out_shape=(
            jax.ShapeDtypeStruct((128, 1024), BF16),
            jax.ShapeDtypeStruct((16, 4096), F32),
            jax.ShapeDtypeStruct((16, 1024), F32),
        ),
        in_specs=[vmem] * 5,
        out_specs=(vmem, vmem, vmem),
        scratch_shapes=[
            pltpu.VMEM((2, 16, 128), F32),
            pltpu.VMEM((16, 128), F32),
            tiles(96), tiles(48), tiles(48), tiles(3, 12), tiles(12), tiles(3, 3), tiles(3), tiles(8, 3),
            tiles(96),
        ]
        + [dma((n,)) for n in (4, 4, 3, 3, 3, 3, 7, 7, 3, 3, 3, 3)],
        compiler_params=pltpu.CompilerParams(
            collective_id=2, has_side_effects=True, vmem_limit_bytes=VMEM_LIMIT
        ),
    )(ox, glx, lowx, normed, up)


def on_device(
    layer_input,
    gain,
    codes,
    column_scale_quantized,
    block_second_scale,
    query_down_map,
    query_up_map,
    token_document,
    output_cotangent,
):
    x, y, z, j, _ = places()
    places_two = jnp.stack([ctx_of(x, y, z, j), pair_of(x, y, z, j)])
    freqs = jnp.exp(jnp.arange(HEAD // 2, dtype=F32) * (-2.0 * math.log(ROPE_BASE) / HEAD))
    positions = (places_two[:, None] * 128 + jnp.arange(128, dtype=I32)[None, :]).astype(F32)
    angle = positions[:, None, :] * freqs[None, :, None]
    cosine, sine = jnp.cos(angle), jnp.sin(angle)
    table = jnp.asarray(NF4_LEVELS * 8, F32)[None, :]

    q, kv, normed, lowt, ids, dox = project(
        layer_input,
        gain[None, :],
        codes,
        column_scale_quantized,
        block_second_scale[None, :],
        query_down_map.T,
        query_up_map,
        cosine,
        sine,
        table,
        token_document[None, :],
        output_cotangent,
    )
    qx, kvg, idg, lowx = gather(q, kv, lowt, ids)
    ox, glx = attend(qx, dox, kvg, idg, cosine, sine)
    attn, grad_at, up_map_gradient = reduce_all(ox, glx, lowx, normed, query_up_map)
    return (attn, grad_at.T, up_map_gradient)


def solution(mesh):
    return jax.shard_map(
        on_device,
        mesh=mesh,
        in_specs=(
            P("ctx", None),
            P(),
            P("fsdp", None),
            P("fsdp", None),
            P(),
            P(),
            P(None, "fsdp"),
            P("ctx"),
            P("ctx", "fsdp"),
        ),
        out_specs=(P("ctx", "fsdp"), P(), P(None, "fsdp")),
        check_vma=False,
    )
```

```python
import functools
import math

import jax
import jax.numpy as jnp
from jax import lax
from jax.experimental import pallas as pl
from jax.experimental.pallas import tpu as pltpu
from jax.sharding import PartitionSpec as P

MESH = pl.DeviceIdType.MESH
HEAD = 128
NF4_LEVELS = [
    -1.0,
    -0.6961928009986877,
    -0.5250730514526367,
    -0.39491748809814453,
    -0.28444138169288635,
    -0.18477343022823334,
    -0.09105003625154495,
    0.0,
    0.07958029955625534,
    0.16093020141124725,
    0.24611230194568634,
    0.33791524171829224,
    0.44070982933044434,
    0.5626170039176941,
    0.7229568362236023,
    1.0,
]
ADAPTER_SCALE = 2.0
ROPE_BASE = 500000.0
SOFT_SCALE = 1.0 / math.sqrt(HEAD)
QUERY_SCALE = SOFT_SCALE * math.log2(math.e)
F32, BF16, I32 = jnp.float32, jnp.bfloat16, jnp.int32
VMEM_LIMIT = 60 * 1024 * 1024


def places():
    c = lax.axis_index("ctx")
    f = lax.axis_index("fsdp")
    return c // 32, (c // 8) % 4, (c // 2) % 4, c % 2, f


def ctx_of(x, y, z, j):
    return ((x * 4 + y) * 4 + z) * 2 + j


def pair_of(x, y, z, j):
    return ctx_of(3 - x, 3 - y, (z + 2) % 4, j)


def lookup(table, index):
    return lax.gather(
        table,
        index[..., None],
        lax.GatherDimensionNumbers(
            offset_dims=(),
            collapsed_slice_dims=(1,),
            start_index_map=(1,),
            operand_batching_dims=(0,),
            start_indices_batching_dims=(0,),
        ),
        slice_sizes=(1, 1),
        mode=lax.GatherScatterMode.PROMISE_IN_BOUNDS,
    )


def remote(src, dst, send, recv, ctx, f):
    return pltpu.make_async_remote_copy(
        src_ref=src, dst_ref=dst, send_sem=send, recv_sem=recv, device_id=(ctx, f), device_id_type=MESH
    )


def project_kernel(
    x_ref, gain_ref, codes_ref, sq_ref, bs_ref, downt_ref, up_ref, cos_ref, sin_ref, table_ref, doc_ref, do_ref,
    normed_ref, dox, qx, kvg, idg, lowx,
    perm, scale, w_buf, acc, parts, send_kv, recv_kv, send_q, recv_q, extra, kv_buf, q_buf, low_buf, ids_buf,
    p_send, p_recv, e_send, e_recv, own_sem, z_send, z_recv, zi_send, zi_recv, a_send, a_recv, ai_send, ai_recv,
    b_send, b_recv, bi_send, bi_recv, s_send, s_recv,
):
    x, y, z, j, f = places()
    here = lax.axis_index("ctx")
    other = 1 - f
    i = 1 - j
    k = z // 2
    u = x * i + y * j
    v = y * i + x * j

    def at(uu, vv, zz):
        return ctx_of(uu * i + vv * j, vv * i + uu * j, zz, j)

    def slot(uu, vv, zz):
        return (uu * 4 + vv) * 4 + zz

    sibling = ctx_of(x, y, z, i)
    pair = pair_of(x, y, z, j)
    zo = (z + 2) % 4
    zn = z + 1 - 2 * (z % 2)
    zf = (zn + 2) % 4
    across, next_z, far_z = at(u, v, zo), at(u, v, zn), at(u, v, zf)
    vr, vl, vo = (v + 1) % 4, (v + 3) % 4, (v + 2) % 4
    ur, ul, uo = (u + 1) % 4, (u + 3) % 4, (u + 2) % 4
    right_v, left_v = at(u, vr, z), at(u, vl, z)
    right_u, left_u = at(ur, v, z), at(ul, v, z)

    barrier = pltpu.get_barrier_semaphore()
    pl.semaphore_signal(barrier, inc=1, device_id=(here, other), device_id_type=MESH)
    peers = [sibling, pair, across, next_z, far_z, right_v, left_v, right_u, left_u]
    for peer in peers:
        pl.semaphore_signal(barrier, inc=1, device_id=(peer, f), device_id_type=MESH)

    wide = x_ref[...].astype(F32)
    inverse = lax.rsqrt(jnp.mean(wide * wide, axis=-1, keepdims=True) + 1e-05)
    normed_ref[...] = (wide * inverse * gain_ref[...]).astype(BF16)
    ids_buf[...] = jnp.broadcast_to(doc_ref[...], (8, 128))
    near = pl.ds(pl.multiple_of(512 * k, 512), 512)
    far = pl.ds(pl.multiple_of(512 * (1 - k), 512), 512)
    dox[0] = do_ref[:, near]

    sent = []

    def push(src, dst, n, send, recv, peer, group=f):
        copy = remote(src, dst, send.at[n], recv.at[n], peer, group)
        copy.start()
        sent.append(copy)

    def got(ref, n, send, recv):
        remote(ref, ref, send.at[n], recv.at[n], sibling, f).wait_recv()

    mine = slot(u, v, z)
    pl.semaphore_wait(barrier, len(peers) + 1)
    push(do_ref.at[:, far], dox.at[1], 3, e_send, e_recv, pair)
    for n, peer in enumerate((next_z, across, far_z)):
        push(ids_buf, idg.at[j, mine], n, zi_send, zi_recv, peer)

    for part in range(8):
        m = lax.broadcasted_iota(I32, (128, 1024), 0)
        column = lax.broadcasted_iota(I32, (128, 1024), 1)
        perm[128 * part : 128 * part + 128, :] = jnp.where(column == 8 * m + part, 1.0, 0.0).astype(BF16)
    pick = lax.broadcasted_iota(I32, (32, 64), 1) == lax.broadcasted_iota(I32, (32, 64), 0) + 32 * f
    second = jnp.sum(jnp.where(pick, bs_ref[...], 0.0), axis=1, keepdims=True) * (1.0 / 256.0)
    for t in range(3):
        quantized = (sq_ref[:, 1024 * t : 1024 * t + 1024].astype(F32) + 1.0).astype(BF16)
        packed = lax.dot_general(quantized, perm[...], (((1,), (1,)), ((), ())), preferred_element_type=F32)
        scale[t] = packed * second

    table = jnp.broadcast_to(table_ref[...], (64, 128))

    def tile(t):
        lane = pl.multiple_of(t * 128, 128)
        acc[...] = jnp.zeros_like(acc)

        def chunk(kc, carry):
            for b in range(4):
                row = pl.multiple_of(kc * 256 + b * 64, 64)
                words = codes_ref[pl.ds(row, 64), pl.ds(lane, 128)]
                scale_row = scale[t, pl.ds(kc * 4 + b, 1), :]
                for n in range(8):
                    index = jnp.bitwise_and(jnp.right_shift(words, 4 * n), 15)
                    levels = lookup(table, index)
                    w_buf[64 * b : 64 * b + 64, 128 * n : 128 * n + 128] = (
                        levels * scale_row[:, 128 * n : 128 * n + 128]
                    ).astype(BF16)
            col = pl.multiple_of(f * 2048 + kc * 256, 256)
            acc[...] += jnp.dot(normed_ref[:, pl.ds(col, 256)], w_buf[...], preferred_element_type=F32)
            return carry

        lax.fori_loop(0, 8, chunk, 0)
        full = acc[...]
        high = full.astype(BF16)
        low = (full - high.astype(F32)).astype(BF16)
        parts[t] = jnp.dot(high, perm[...], preferred_element_type=F32) + jnp.dot(
            low, perm[...], preferred_element_type=F32
        )

    def columns(t, offset):
        return parts[t, :, pl.ds(pl.multiple_of(offset, 512), 512)]

    tile(2 - f)
    send_kv[...] = columns(2 - f, 512 * other).astype(BF16)
    push(send_kv, recv_kv, 0, p_send, p_recv, here, other)
    tile(1 + f)
    tile(0)
    send_q[:, 0:512] = columns(other, 512 * other).astype(BF16)
    send_q[:, 512:1024] = columns(2 * other, 512 * f).astype(BF16)

    cosine, sine = cos_ref[0].T, sin_ref[0].T
    cosine = jnp.concatenate([cosine, cosine], axis=1)
    sine = jnp.concatenate([-sine, sine], axis=1)

    def rotate(vector):
        return vector * cosine + pltpu.roll(vector, 64, 1) * sine

    got(recv_kv, 0, p_send, p_recv)
    both = columns(1 + f, 512 * f) + recv_kv[...].astype(F32)
    for h in range(2):
        kv_buf[h, :, 0:128] = rotate(both[:, 128 * h : 128 * h + 128]).astype(BF16)
        kv_buf[h, :, 128:256] = both[:, 256 + 128 * h : 384 + 128 * h].astype(BF16)

    push(kv_buf.at[1 - k], kvg.at[j, mine], 0, e_send, e_recv, across)
    push(kv_buf.at[k], kvg.at[j, mine], 0, z_send, z_recv, next_z)
    local = []

    def keep(src, dst, n):
        copy = pltpu.make_async_copy(src, dst, own_sem.at[n])
        copy.start()
        local.append(copy)

    keep(kv_buf.at[k], kvg.at[j, mine], 0)
    keep(ids_buf, idg.at[j, mine], 1)

    lowt = lax.dot_general(
        downt_ref[...], normed_ref[...], (((1,), (1,)), ((), ())), preferred_element_type=F32
    ).astype(BF16)
    low_buf[...] = lowt
    extra[...] = ADAPTER_SCALE * lax.dot_general(
        lowt, up_ref[...], (((0,), (0,)), ((), ())), preferred_element_type=F32
    )

    block = kvg.at[j, slot(u, v, zo)]
    got(block, 0, e_send, e_recv)
    push(block, block, 1, z_send, z_recv, next_z)
    push(send_q, recv_q, 1, p_send, p_recv, here, other)
    push(low_buf, lowx.at[1], 2, e_send, e_recv, pair)
    keep(low_buf, lowx.at[0], 2)
    got(kvg.at[j, slot(u, v, zn)], 0, z_send, z_recv)
    for n, zz in enumerate((zn, zo, zf)):
        got(idg.at[j, slot(u, v, zz)], n, zi_send, zi_recv)
    local[0].wait()
    local[1].wait()
    got(kvg.at[j, slot(u, v, zf)], 1, z_send, z_recv)

    def half(vv, h):
        return kvg.at[j, pl.ds(slot(u, vv, 0) + 2 * h, 2)]

    def piece(uu, vv):
        return kvg.at[j, pl.ds(slot(uu, vv, 0), 4)]

    def marks(vv):
        return idg.at[j, pl.ds(slot(u, vv, 0), 4)]

    def all_marks(uu):
        return idg.at[j, pl.ds(slot(uu, 0, 0), 16)]

    def same(part, n, send, recv, peer):
        push(part, part, n, send, recv, peer)

    shared = []

    def share(du, dv):
        part = piece((u + du) % 4, (v + dv) % 4)
        same(part, len(shared), s_send, s_recv, sibling)
        shared.append((du, dv))

    same(half(v, 0), 0, a_send, a_recv, right_v)
    same(half(v, 1), 3, a_send, a_recv, left_v)
    same(half(v, 1), 1, a_send, a_recv, right_v)
    same(half(v, 0), 4, a_send, a_recv, left_v)
    same(marks(v), 0, ai_send, ai_recv, right_v)
    same(marks(v), 1, ai_send, ai_recv, left_v)
    same(piece(u, v), 0, b_send, b_recv, right_u)
    same(piece(u, v), 4, b_send, b_recv, left_u)
    share(0, 0)
    got(half(vl, 0), 0, a_send, a_recv)
    same(half(vl, 0), 2, a_send, a_recv, right_v)
    got(half(vr, 1), 3, a_send, a_recv)
    same(half(vr, 1), 5, a_send, a_recv, left_v)
    got(half(vl, 1), 1, a_send, a_recv)
    got(marks(vl), 0, ai_send, ai_recv)
    same(marks(vl), 2, ai_send, ai_recv, right_v)
    same(piece(u, vl), 1, b_send, b_recv, right_u)
    same(piece(u, vl), 5, b_send, b_recv, left_u)
    share(0, 3)
    got(half(vr, 0), 4, a_send, a_recv)
    got(marks(vr), 1, ai_send, ai_recv)
    same(piece(u, vr), 2, b_send, b_recv, right_u)
    same(piece(u, vr), 6, b_send, b_recv, left_u)
    share(0, 1)
    got(half(vo, 0), 2, a_send, a_recv)
    got(half(vo, 1), 5, a_send, a_recv)
    got(marks(vo), 2, ai_send, ai_recv)
    same(piece(u, vo), 3, b_send, b_recv, right_u)
    same(piece(u, vo), 7, b_send, b_recv, left_u)
    share(0, 2)
    same(all_marks(u), 0, bi_send, bi_recv, right_u)
    same(all_marks(u), 1, bi_send, bi_recv, left_u)

    got(piece(ul, v), 0, b_send, b_recv)
    same(piece(ul, v), 8, b_send, b_recv, right_u)
    share(3, 0)
    got(piece(ul, vl), 1, b_send, b_recv)
    same(piece(ul, vl), 9, b_send, b_recv, right_u)
    share(3, 3)

    got(recv_q, 1, p_send, p_recv)
    for h in range(8):
        s = slice(128 * h, 128 * h + 128)
        if h < 4:
            own = parts[f, :, pl.ds(pl.multiple_of(512 * f + 128 * h, 128), 128)]
        else:
            own = parts[2 * f, :, pl.ds(pl.multiple_of(512 * other + 128 * (h - 4), 128), 128)]
        whole = own + recv_q[:, s].astype(F32) + extra[:, s]
        q_buf[:, s] = (rotate(whole) * QUERY_SCALE).astype(BF16)
    push(q_buf.at[:, far], qx.at[1], 1, e_send, e_recv, pair)
    keep(q_buf.at[:, near], qx.at[0], 3)

    got(piece(ur, vr), 6, b_send, b_recv)
    same(piece(ur, vr), 10, b_send, b_recv, left_u)
    share(1, 1)
    got(piece(ur, vo), 7, b_send, b_recv)
    same(piece(ur, vo), 11, b_send, b_recv, left_u)
    share(1, 2)
    got(all_marks(ul), 0, bi_send, bi_recv)
    same(all_marks(ul), 2, bi_send, bi_recv, right_u)
    got(all_marks(ur), 1, bi_send, bi_recv)
    got(piece(ul, vr), 2, b_send, b_recv)
    share(3, 1)
    got(piece(ul, vo), 3, b_send, b_recv)
    share(3, 2)
    got(piece(ur, v), 4, b_send, b_recv)
    share(1, 0)
    got(piece(ur, vl), 5, b_send, b_recv)
    share(1, 3)
    got(all_marks(uo), 2, bi_send, bi_recv)
    same(idg.at[j], 16, s_send, s_recv, sibling)
    got(piece(uo, v), 8, b_send, b_recv)
    share(2, 0)
    got(piece(uo, vr), 10, b_send, b_recv)
    share(2, 1)
    got(piece(uo, vl), 9, b_send, b_recv)
    share(2, 3)
    got(piece(uo, vo), 11, b_send, b_recv)
    share(2, 2)

    got(dox.at[1], 3, e_send, e_recv)
    got(lowx.at[1], 2, e_send, e_recv)
    got(qx.at[1], 1, e_send, e_recv)
    for n, (du, dv) in enumerate(shared):
        got(kvg.at[i, pl.ds(slot((v + du) % 4, (u + dv) % 4, 0), 4)], n, s_send, s_recv)
    got(idg.at[i], 16, s_send, s_recv)
    for copy in local[2:]:
        copy.wait()
    for copy in sent:
        copy.wait_send()


def project(x, gain, codes, sq, bs, downt, up, cosine, sine, table, doc, do):
    vmem = pl.BlockSpec(memory_space=pltpu.VMEM)
    hbm = pl.BlockSpec(memory_space=pl.ANY)
    dma = pltpu.SemaphoreType.DMA
    counts = (2, 2, 4, 4, 4, 2, 2, 3, 3, 6, 6, 3, 3, 12, 12, 3, 3, 17, 17)
    return pl.pallas_call(
        project_kernel,
        name="project",
        out_shape=(
            jax.ShapeDtypeStruct((128, 4096), BF16),
            jax.ShapeDtypeStruct((2, 128, 512), BF16),
            jax.ShapeDtypeStruct((2, 128, 512), BF16),
            jax.ShapeDtypeStruct((2, 64, 128, 256), BF16),
            jax.ShapeDtypeStruct((2, 64, 8, 128), I32),
            jax.ShapeDtypeStruct((2, 16, 128), BF16),
        ),
        in_specs=[vmem] * 12,
        out_specs=(vmem, vmem, hbm, hbm, hbm, hbm),
        scratch_shapes=[
            pltpu.VMEM((1024, 1024), BF16),
            pltpu.VMEM((3, 32, 1024), F32),
            pltpu.VMEM((256, 1024), BF16),
            pltpu.VMEM((128, 1024), F32),
            pltpu.VMEM((3, 128, 1024), F32),
            pltpu.VMEM((128, 512), BF16),
            pltpu.VMEM((128, 512), BF16),
            pltpu.VMEM((128, 1024), BF16),
            pltpu.VMEM((128, 1024), BF16),
            pltpu.VMEM((128, 1024), F32),
            pltpu.VMEM((2, 128, 256), BF16),
            pltpu.VMEM((128, 1024), BF16),
            pltpu.VMEM((16, 128), BF16),
            pltpu.VMEM((8, 128), I32),
        ]
        + [dma((n,)) for n in counts],
        compiler_params=pltpu.CompilerParams(
            collective_id=0, has_side_effects=True, vmem_limit_bytes=VMEM_LIMIT
        ),
    )(x, gain, codes, sq, bs, downt, up, cosine, sine, table, doc, do)


STEP = 512


def attend_kernel(
    qx_ref, dox_ref, kvg_ref, idg_ref, cos_ref, sin_ref, ox_ref, glx_ref,
    qt, dot_, limits, ahead0, ahead1, max0, max1, run_max, run_sum, acc, acc2,
):
    x, y, z, j, _ = places()
    here = ctx_of(x, y, z, j)
    there = pair_of(x, y, z, j)

    def slot(number, core):
        a, b, d = number // 16, (number // 4) % 4, number % 4
        first, second = (a * 4 + b) * 4 + d, (b * 4 + a) * 4 + d
        if isinstance(core, int):
            return second if core else first
        return jnp.where(core == 0, first, second)

    def block(number):
        return jnp.concatenate([kvg_ref[0, slot(number, 0)], kvg_ref[1, slot(number, 1)]], axis=0)

    every = idg_ref[...].reshape(128, 8, 128)
    below = [
        jnp.sum(jnp.sum(jnp.where(every < d, 1, 0), axis=0), axis=1, keepdims=True)[0:1, :] for d in (1, 2, 3)
    ]
    lane = lax.broadcasted_iota(I32, (1, 128), 1)
    for t, place in enumerate((here, there)):
        ids = idg_ref[j, slot(place // 2, j), 0:1, :]
        start = jnp.zeros((1, 128), I32)
        for d in (1, 2, 3):
            start = jnp.where(ids == d, below[d - 1], start)
        limits[t, 0:1, :] = jnp.concatenate([start, start], axis=1)
        position = place * 128 + lane
        limits[t, 1:2, :] = jnp.concatenate([position, position], axis=1)
        for g in range(4):
            lanes = slice(128 * g, 128 * g + 128)
            qt[t, :, lanes] = qx_ref[t, :, lanes].T
            dot_[t, :, lanes] = dox_ref[t, :, lanes].T
    run_max[...] = jnp.full_like(run_max, -1e29)
    run_sum[...] = jnp.zeros_like(run_sum)
    acc[...] = jnp.zeros_like(acc)
    acc2[...] = jnp.zeros_like(acc2)

    def rows(t, carry):
        place = jnp.where(t == 0, here, there)
        first = jnp.min(limits[t, 0:1, :]) // STEP
        latest = jnp.max(limits[t, 0:1, :])
        stop = (place * 128 + 127) // STEP + 1

        def scores_of(number, masked, ahead, ahead_max):
            key = jnp.minimum(number, 31) * 2
            base = number * STEP
            for h in range(2):
                keys = block(key + h)[:, :128]
                for p in range(2):
                    cols = slice(256 * p, 256 * p + 256)
                    scores = jnp.dot(keys, qt[t, :, cols], preferred_element_type=F32)
                    if masked:
                        pos = base + 256 * h + lax.broadcasted_iota(I32, (256, 256), 0)
                        allowed = (pos >= limits[t, 0:1, :]) & (pos <= limits[t, 1:2, :])
                        scores = jnp.where(allowed, scores, -1e30)
                    ahead[256 * h : 256 * h + 256, cols] = scores
                    top = jnp.max(scores, axis=0, keepdims=True)
                    ahead_max[h : h + 1, cols] = top

        def is_edge(number):
            return (number * STEP < latest) | (number * STEP + STEP - 1 > place * 128)

        def step(number, masked, ahead, ahead_max, later, later_max):
            scores_of(number + 1, masked, later, later_max)
            kv = jnp.concatenate([block(2 * number), block(2 * number + 1)], axis=0)
            kvt = kv.T
            values = kv[:, 128:]
            for p in range(2):
                cols = slice(256 * p, 256 * p + 256)
                tops = jnp.maximum(ahead_max[0:1, cols], ahead_max[1:2, cols])
                old = run_max[t, 0:1, cols]
                new = jnp.maximum(old, tops)
                decay = jnp.exp2(old - new)
                run_max[t, 0:1, cols] = new
                grad_dots = jnp.dot(values, dot_[t, :, cols], preferred_element_type=F32)
                expo = jnp.exp2(ahead[:, cols] - new)
                run_sum[t, 0:1, cols] = run_sum[t, 0:1, cols] * decay + jnp.sum(expo, axis=0, keepdims=True)
                weighted = (expo * grad_dots).astype(BF16)
                acc[t, :, cols] = acc[t, :, cols] * decay + jnp.dot(
                    kvt, expo.astype(BF16), preferred_element_type=F32
                )
                acc2[t, :, cols] = acc2[t, :, cols] * decay + jnp.dot(
                    kvt[:128], weighted, preferred_element_type=F32
                )

        scores_of(first, True, ahead0, max0)

        def one(number, *buffers):
            edge = is_edge(number + 1)

            @pl.when(edge)
            def _():
                step(number, True, *buffers)

            @pl.when(jnp.logical_not(edge))
            def _():
                step(number, False, *buffers)

        def body(twice, c):
            number = first + 2 * twice
            one(number, ahead0, max0, ahead1, max1)

            @pl.when(number + 1 < stop)
            def _():
                one(number + 1, ahead1, max1, ahead0, max0)

            return c

        lax.fori_loop(0, (stop - first + 1) // 2, body, 0)
        return carry

    lax.fori_loop(0, 2, rows, 0)

    for t in range(2):
        cosine, sine = cos_ref[t], sin_ref[t]
        for g in range(4):
            lanes = slice(128 * g, 128 * g + 128)
            inverse = 1.0 / run_sum[t, 0:1, lanes]
            out = acc[t, 128:256, lanes] * inverse
            mean_dot = jnp.sum(dot_[t, :, lanes].astype(F32) * out, axis=0, keepdims=True)
            grad = (acc2[t, :, lanes] - mean_dot * acc[t, 0:128, lanes]) * (inverse * SOFT_SCALE)
            ga, gb = grad[:64], grad[64:]
            back = jnp.concatenate([ga * cosine + gb * sine, gb * cosine - ga * sine], axis=0)
            ox_ref[t, :, lanes] = out.T.astype(BF16)
            glx_ref[t, :, lanes] = back.T.astype(BF16)


def attend(qx, dox, kvg, idg, cosine, sine):
    vmem = pl.BlockSpec(memory_space=pltpu.VMEM)
    return pl.pallas_call(
        attend_kernel,
        name="attend",
        out_shape=(jax.ShapeDtypeStruct((2, 128, 512), BF16), jax.ShapeDtypeStruct((2, 128, 512), BF16)),
        in_specs=[vmem] * 6,
        out_specs=(vmem, vmem),
        scratch_shapes=[
            pltpu.VMEM((2, 128, 512), BF16),
            pltpu.VMEM((2, 128, 512), BF16),
            pltpu.VMEM((2, 8, 256), I32),
            pltpu.VMEM((512, 512), F32),
            pltpu.VMEM((512, 512), F32),
            pltpu.VMEM((8, 512), F32),
            pltpu.VMEM((8, 512), F32),
            pltpu.VMEM((2, 8, 512), F32),
            pltpu.VMEM((2, 8, 512), F32),
            pltpu.VMEM((2, 256, 512), F32),
            pltpu.VMEM((2, 128, 512), F32),
        ],
        compiler_params=pltpu.CompilerParams(vmem_limit_bytes=VMEM_LIMIT),
    )(qx, dox, kvg, idg, cosine, sine)


def reduce_kernel(
    ox_ref, glx_ref, lowx_ref, normed_ref, up_ref,
    attn_ref, grad_at_ref, up_out_ref,
    mid_send, mid_recv, buf, rcore, b1, rp, b3, rz, final,
    p_send, p_recv, x_send, x_recv, z_send, z_recv, g_send, g_recv,
):
    x, y, z, j, f = places()
    i = 1 - j
    sibling = ctx_of(x, y, z, i)
    flat = x * 4 + y
    plane = [(flat + d) % 16 for d in range(1, 16)]
    whole_z = f * 4 + z
    zs = [(whole_z + d) % 8 for d in range(1, 8)]

    pair = pair_of(x, y, z, j)
    k = z // 2
    barrier = pltpu.get_barrier_semaphore()
    peers = [(sibling, f), (pair, f)]
    peers += [(ctx_of(p // 4, p % 4, z, j), f) for p in plane]
    peers += [(ctx_of(x, y, p % 4, j), p // 4) for p in zs]
    for peer in peers:
        pl.semaphore_signal(barrier, inc=1, device_id=peer, device_id_type=MESH)

    glx = jnp.concatenate([glx_ref[0], glx_ref[1]], axis=0)
    up = up_ref[:, pl.ds(pl.multiple_of(512 * k, 512), 512)]
    midt = ADAPTER_SCALE * lax.dot_general(
        up, glx, (((1,), (1,)), ((), ())), preferred_element_type=F32
    )
    mid_send[0] = midt[:, 0:128]
    mid_send[1] = midt[:, 128:256]
    pl.semaphore_wait(barrier, len(peers))

    sent = []
    mid_copy = remote(mid_send.at[1], mid_recv, p_send.at[0], p_recv.at[0], pair, f)
    mid_copy.start()
    near = pl.ds(pl.multiple_of(512 * k, 512), 512)
    out_copy = remote(ox_ref.at[1], attn_ref.at[:, near], p_send.at[1], p_recv.at[1], pair, f)
    attn_ref[:, near] = ox_ref[0]

    lowt = jnp.concatenate([lowx_ref[0], lowx_ref[1]], axis=1)
    upg = ADAPTER_SCALE * jnp.dot(lowt, glx, preferred_element_type=F32)
    buf[64:96] = jnp.zeros((32, 8, 128), F32)
    for s in range(2):
        for t in range(4):
            buf[64 + 16 * s + 8 * f + 4 * k + t] = upg[8 * s : 8 * s + 8, 128 * t : 128 * t + 128]
    mid_copy.wait()
    mid = (mid_send[0] + mid_recv[...]).astype(BF16)
    for t in range(4):
        part = jnp.dot(mid, normed_ref[:, 1024 * t : 1024 * t + 1024], preferred_element_type=F32)
        for s in range(2):
            for w in range(8):
                buf[32 * s + 8 * t + w] = part[8 * s : 8 * s + 8, 128 * w : 128 * w + 128]

    core_copy = remote(buf.at[pl.ds(48 * i, 48)], rcore, p_send.at[2], p_recv.at[2], sibling, f)
    core_copy.start()
    core_copy.wait()
    b1[...] = buf[pl.ds(48 * j, 48)] + rcore[...]
    copies = []
    for n, p in enumerate(plane):
        peer = ctx_of(p // 4, p % 4, z, j)
        copy = remote(b1.at[pl.ds(3 * p, 3)], rp.at[n], x_send.at[n], x_recv.at[n], peer, f)
        copy.start()
        copies.append(copy)
    out_copy.start()
    added = b1[pl.ds(3 * flat, 3)]
    for n, copy in enumerate(copies):
        copy.wait()
        added = added + rp[n]
    b3[...] = added
    copies = []
    for n, p in enumerate(zs):
        copy = remote(b3, rz.at[whole_z], z_send.at[n], z_recv.at[n], ctx_of(x, y, p % 4, j), p // 4)
        copy.start()
        copies.append(copy)
    rz[whole_z] = b3[...]
    for n, copy in enumerate(copies):
        source = (whole_z + 7 - n) % 8
        remote(rz.at[source], rz.at[source], z_send.at[n], z_recv.at[n], sibling, f).wait_recv()
    added = rz[0]
    for n in range(1, 8):
        added = added + rz[n]
    row = 48 * j + 3 * flat
    final[pl.ds(row, 3)] = added
    sent += copies

    for n, p in enumerate(plane):
        part = final.at[pl.ds(row, 3)]
        copy = remote(part, part, g_send.at[n], g_recv.at[n], ctx_of(p // 4, p % 4, z, j), f)
        copy.start()
        sent.append(copy)
    for n in range(15):
        part = final.at[pl.ds(48 * j + 3 * ((flat + 15 - n) % 16), 3)]
        remote(part, part, g_send.at[n], g_recv.at[n], sibling, f).wait_recv()
    part = final.at[pl.ds(48 * j, 48)]
    copy = remote(part, part, p_send.at[3], p_recv.at[3], sibling, f)
    copy.start()
    sent.append(copy)
    part = final.at[pl.ds(48 * i, 48)]
    remote(part, part, p_send.at[3], p_recv.at[3], sibling, f).wait_recv()

    for s in range(2):
        for t in range(32):
            grad_at_ref[8 * s : 8 * s + 8, 128 * t : 128 * t + 128] = final[32 * s + t]
        for t in range(8):
            up_out_ref[8 * s : 8 * s + 8, 128 * t : 128 * t + 128] = final[64 + 16 * s + 8 * f + t]

    other_half = attn_ref.at[:, pl.ds(pl.multiple_of(512 * (1 - k), 512), 512)]
    remote(ox_ref.at[1], other_half, p_send.at[1], p_recv.at[1], sibling, f).wait_recv()
    out_copy.wait_send()
    for copy in sent:
        copy.wait_send()


def reduce_all(ox, glx, lowx, normed, up):
    vmem = pl.BlockSpec(memory_space=pltpu.VMEM)
    hbm = pl.BlockSpec(memory_space=pl.ANY)
    dma = pltpu.SemaphoreType.DMA
    tiles = lambda *lead: pltpu.VMEM((*lead, 8, 128), F32)
    return pl.pallas_call(
        reduce_kernel,
        name="reduce_all",
        out_shape=(
            jax.ShapeDtypeStruct((128, 1024), BF16),
            jax.ShapeDtypeStruct((16, 4096), F32),
            jax.ShapeDtypeStruct((16, 1024), F32),
        ),
        in_specs=[vmem] * 5,
        out_specs=(vmem, vmem, vmem),
        scratch_shapes=[
            pltpu.VMEM((2, 16, 128), F32),
            pltpu.VMEM((16, 128), F32),
            tiles(96), tiles(48), tiles(48), tiles(15, 3), tiles(3), tiles(8, 3),
            tiles(96),
        ]
        + [dma((n,)) for n in (4, 4, 15, 15, 7, 7, 15, 15)],
        compiler_params=pltpu.CompilerParams(
            collective_id=1, has_side_effects=True, vmem_limit_bytes=VMEM_LIMIT
        ),
    )(ox, glx, lowx, normed, up)


def hand_over_kernel(a_ref, b_ref, c_ref, a_out, b_out, c_out):
    a_out[...] = a_ref[...]
    b_out[...] = b_ref[...]
    c_out[...] = c_ref[...]


def hand_over(*arrays):
    vmem = pl.BlockSpec(memory_space=pltpu.VMEM)
    return pl.pallas_call(
        hand_over_kernel,
        name="hand_over",
        out_shape=tuple(jax.ShapeDtypeStruct(a.shape, a.dtype) for a in arrays),
        in_specs=[vmem] * 3,
        out_specs=(vmem,) * 3,
        compiler_params=pltpu.CompilerParams(vmem_limit_bytes=VMEM_LIMIT),
    )(*arrays)


def on_device(
    layer_input,
    gain,
    codes,
    column_scale_quantized,
    block_second_scale,
    query_down_map,
    query_up_map,
    token_document,
    output_cotangent,
):
    x, y, z, j, _ = places()
    places_two = jnp.stack([ctx_of(x, y, z, j), pair_of(x, y, z, j)])
    freqs = jnp.exp(jnp.arange(HEAD // 2, dtype=F32) * (-2.0 * math.log(ROPE_BASE) / HEAD))
    positions = (places_two[:, None] * 128 + jnp.arange(128, dtype=I32)[None, :]).astype(F32)
    angle = positions[:, None, :] * freqs[None, :, None]
    cosine, sine = jnp.cos(angle), jnp.sin(angle)
    table = jnp.asarray(NF4_LEVELS * 8, F32)[None, :]

    normed, dox, qx, kvg, idg, lowx = project(
        layer_input,
        gain[None, :],
        codes,
        column_scale_quantized,
        block_second_scale[None, :],
        query_down_map.T,
        query_up_map,
        cosine,
        sine,
        table,
        token_document[None, :],
        output_cotangent,
    )
    ox, glx = attend(qx, dox, kvg, idg, cosine, sine)
    attn, grad_at, up_map_gradient = reduce_all(ox, glx, lowx, normed, query_up_map)
    attn, grad_at, up_map_gradient = hand_over(attn, grad_at, up_map_gradient)
    return (attn, grad_at.T, up_map_gradient)


def solution(mesh):
    return jax.shard_map(
        on_device,
        mesh=mesh,
        in_specs=(
            P("ctx", None),
            P(),
            P("fsdp", None),
            P("fsdp", None),
            P(),
            P(),
            P(None, "fsdp"),
            P("ctx"),
            P("ctx", "fsdp"),
        ),
        out_specs=(P("ctx", "fsdp"), P(), P(None, "fsdp")),
        check_vma=False,
    )
```

```python
import functools
import math

import jax
import jax.numpy as jnp
from jax import lax
from jax.experimental import pallas as pl
from jax.experimental.pallas import tpu as pltpu
from jax.sharding import PartitionSpec as P

MESH = pl.DeviceIdType.MESH
HEAD = 128
NF4_LEVELS = [
    -1.0,
    -0.6961928009986877,
    -0.5250730514526367,
    -0.39491748809814453,
    -0.28444138169288635,
    -0.18477343022823334,
    -0.09105003625154495,
    0.0,
    0.07958029955625534,
    0.16093020141124725,
    0.24611230194568634,
    0.33791524171829224,
    0.44070982933044434,
    0.5626170039176941,
    0.7229568362236023,
    1.0,
]
ADAPTER_SCALE = 2.0
ROPE_BASE = 500000.0
SOFT_SCALE = 1.0 / math.sqrt(HEAD)
QUERY_SCALE = SOFT_SCALE * math.log2(math.e)
F32, BF16, I32 = jnp.float32, jnp.bfloat16, jnp.int32
VMEM_LIMIT = 60 * 1024 * 1024


def places():
    c = lax.axis_index("ctx")
    f = lax.axis_index("fsdp")
    return c // 32, (c // 8) % 4, (c // 2) % 4, c % 2, f


def ctx_of(x, y, z, j):
    return ((x * 4 + y) * 4 + z) * 2 + j


def pair_of(x, y, z, j):
    return ctx_of(3 - x, 3 - y, (z + 2) % 4, j)


def lookup(table, index):
    return lax.gather(
        table,
        index[..., None],
        lax.GatherDimensionNumbers(
            offset_dims=(),
            collapsed_slice_dims=(0,),
            start_index_map=(0,),
            operand_batching_dims=(1,),
            start_indices_batching_dims=(1,),
        ),
        slice_sizes=(1, 1),
        mode=lax.GatherScatterMode.PROMISE_IN_BOUNDS,
    )


def remote(src, dst, send, recv, ctx, f):
    return pltpu.make_async_remote_copy(
        src_ref=src, dst_ref=dst, send_sem=send, recv_sem=recv, device_id=(ctx, f), device_id_type=MESH
    )


def project_kernel(
    x_ref, gain_ref, codes_ref, sq_ref, bs_ref, downt_ref, up_ref, cos_ref, sin_ref, table_ref, doc_ref, do_ref,
    normed_ref, dox, qx, kvg, idg, lowx,
    perm, scale, w_buf, acc, parts, send_kv, recv_kv, send_q, recv_q, extra, kv_buf, q_buf, low_buf, ids_buf,
    p_send, p_recv, e_send, e_recv, own_sem, z_send, z_recv, zi_send, zi_recv, a_send, a_recv, ai_send, ai_recv,
    b_send, b_recv, bi_send, bi_recv, s_send, s_recv,
):
    x, y, z, j, f = places()
    here = lax.axis_index("ctx")
    other = 1 - f
    i = 1 - j
    k = z // 2
    u = x * i + y * j
    v = y * i + x * j

    def at(uu, vv, zz):
        return ctx_of(uu * i + vv * j, vv * i + uu * j, zz, j)

    def slot(uu, vv, zz):
        return (uu * 4 + vv) * 4 + zz

    sibling = ctx_of(x, y, z, i)
    pair = pair_of(x, y, z, j)
    zo = (z + 2) % 4
    zn = z + 1 - 2 * (z % 2)
    zf = (zn + 2) % 4
    across, next_z, far_z = at(u, v, zo), at(u, v, zn), at(u, v, zf)
    vr, vl, vo = (v + 1) % 4, (v + 3) % 4, (v + 2) % 4
    ur, ul, uo = (u + 1) % 4, (u + 3) % 4, (u + 2) % 4
    right_v, left_v = at(u, vr, z), at(u, vl, z)
    right_u, left_u = at(ur, v, z), at(ul, v, z)

    barrier = pltpu.get_barrier_semaphore()
    pl.semaphore_signal(barrier, inc=1, device_id=(here, other), device_id_type=MESH)
    peers = [sibling, pair, across, next_z, far_z, right_v, left_v, right_u, left_u]
    for peer in peers:
        pl.semaphore_signal(barrier, inc=1, device_id=(peer, f), device_id_type=MESH)

    wide = x_ref[...].astype(F32)
    inverse = lax.rsqrt(jnp.mean(wide * wide, axis=-1, keepdims=True) + 1e-05)
    normed_ref[...] = (wide * inverse * gain_ref[...]).astype(BF16)
    ids_buf[...] = jnp.broadcast_to(doc_ref[...], (8, 128))
    near = pl.ds(pl.multiple_of(512 * k, 512), 512)
    far = pl.ds(pl.multiple_of(512 * (1 - k), 512), 512)
    dox[0] = do_ref[:, near]

    sent = []

    def push(src, dst, n, send, recv, peer, group=f):
        copy = remote(src, dst, send.at[n], recv.at[n], peer, group)
        copy.start()
        sent.append(copy)

    def got(ref, n, send, recv):
        remote(ref, ref, send.at[n], recv.at[n], sibling, f).wait_recv()

    mine = slot(u, v, z)
    pl.semaphore_wait(barrier, len(peers) + 1)
    push(do_ref.at[:, far], dox.at[1], 3, e_send, e_recv, pair)
    for n, peer in enumerate((next_z, across, far_z)):
        push(ids_buf, idg.at[j, mine], n, zi_send, zi_recv, peer)

    for part in range(8):
        m = lax.broadcasted_iota(I32, (128, 1024), 0)
        column = lax.broadcasted_iota(I32, (128, 1024), 1)
        perm[128 * part : 128 * part + 128, :] = jnp.where(column == 8 * m + part, 1.0, 0.0).astype(BF16)
    pick = lax.broadcasted_iota(I32, (32, 64), 1) == lax.broadcasted_iota(I32, (32, 64), 0) + 32 * f
    second = jnp.sum(jnp.where(pick, bs_ref[...], 0.0), axis=1, keepdims=True) * (1.0 / 256.0)
    for t in range(3):
        quantized = (sq_ref[:, 1024 * t : 1024 * t + 1024].astype(F32) + 1.0).astype(BF16)
        packed = lax.dot_general(quantized, perm[...], (((1,), (1,)), ((), ())), preferred_element_type=F32)
        scale[t] = packed * second

    lower, upper = table_ref[0:8, :], table_ref[8:16, :]

    def tile(t):
        lane = pl.multiple_of(t * 128, 128)
        acc[...] = jnp.zeros_like(acc)

        def chunk(kc, carry):
            for b in range(4):
                row = pl.multiple_of(kc * 256 + b * 64, 64)
                words = codes_ref[pl.ds(row, 64), pl.ds(lane, 128)]
                scale_row = scale[t, pl.ds(kc * 4 + b, 1), :]
                for n in range(8):
                    rows = []
                    for r in range(8):
                        word = words[8 * r : 8 * r + 8]
                        index = jnp.bitwise_and(jnp.right_shift(word, 4 * n), 7)
                        high = jnp.left_shift(word, 28 - 4 * n) < 0
                        rows.append(jnp.where(high, lookup(upper, index), lookup(lower, index)))
                    w_buf[64 * b : 64 * b + 64, 128 * n : 128 * n + 128] = (
                        jnp.concatenate(rows, axis=0) * scale_row[:, 128 * n : 128 * n + 128]
                    ).astype(BF16)
            col = pl.multiple_of(f * 2048 + kc * 256, 256)
            acc[...] += jnp.dot(normed_ref[:, pl.ds(col, 256)], w_buf[...], preferred_element_type=F32)
            return carry

        lax.fori_loop(0, 8, chunk, 0)
        full = acc[...]
        high = full.astype(BF16)
        low = (full - high.astype(F32)).astype(BF16)
        parts[t] = jnp.dot(high, perm[...], preferred_element_type=F32) + jnp.dot(
            low, perm[...], preferred_element_type=F32
        )

    def columns(t, offset):
        return parts[t, :, pl.ds(pl.multiple_of(offset, 512), 512)]

    tile(2 - f)
    send_kv[...] = columns(2 - f, 512 * other).astype(BF16)
    push(send_kv, recv_kv, 0, p_send, p_recv, here, other)
    tile(1 + f)
    tile(0)
    send_q[:, 0:512] = columns(other, 512 * other).astype(BF16)
    send_q[:, 512:1024] = columns(2 * other, 512 * f).astype(BF16)

    cosine, sine = cos_ref[0].T, sin_ref[0].T
    cosine = jnp.concatenate([cosine, cosine], axis=1)
    sine = jnp.concatenate([-sine, sine], axis=1)

    def rotate(vector):
        return vector * cosine + pltpu.roll(vector, 64, 1) * sine

    got(recv_kv, 0, p_send, p_recv)
    both = columns(1 + f, 512 * f) + recv_kv[...].astype(F32)
    for h in range(2):
        kv_buf[h, :, 0:128] = rotate(both[:, 128 * h : 128 * h + 128]).astype(BF16)
        kv_buf[h, :, 128:256] = both[:, 256 + 128 * h : 384 + 128 * h].astype(BF16)

    push(kv_buf.at[1 - k], kvg.at[j, mine], 0, e_send, e_recv, across)
    push(kv_buf.at[k], kvg.at[j, mine], 0, z_send, z_recv, next_z)
    local = []

    def keep(src, dst, n):
        copy = pltpu.make_async_copy(src, dst, own_sem.at[n])
        copy.start()
        local.append(copy)

    keep(kv_buf.at[k], kvg.at[j, mine], 0)
    keep(ids_buf, idg.at[j, mine], 1)

    lowt = lax.dot_general(
        downt_ref[...], normed_ref[...], (((1,), (1,)), ((), ())), preferred_element_type=F32
    ).astype(BF16)
    low_buf[...] = lowt
    extra[...] = ADAPTER_SCALE * lax.dot_general(
        lowt, up_ref[...], (((0,), (0,)), ((), ())), preferred_element_type=F32
    )

    block = kvg.at[j, slot(u, v, zo)]
    got(block, 0, e_send, e_recv)
    push(block, block, 1, z_send, z_recv, next_z)
    push(send_q, recv_q, 1, p_send, p_recv, here, other)
    push(low_buf, lowx.at[1], 2, e_send, e_recv, pair)
    keep(low_buf, lowx.at[0], 2)
    got(kvg.at[j, slot(u, v, zn)], 0, z_send, z_recv)
    for n, zz in enumerate((zn, zo, zf)):
        got(idg.at[j, slot(u, v, zz)], n, zi_send, zi_recv)
    local[0].wait()
    local[1].wait()
    got(kvg.at[j, slot(u, v, zf)], 1, z_send, z_recv)

    def half(vv, h):
        return kvg.at[j, pl.ds(slot(u, vv, 0) + 2 * h, 2)]

    def piece(uu, vv):
        return kvg.at[j, pl.ds(slot(uu, vv, 0), 4)]

    def marks(vv):
        return idg.at[j, pl.ds(slot(u, vv, 0), 4)]

    def all_marks(uu):
        return idg.at[j, pl.ds(slot(uu, 0, 0), 16)]

    def same(part, n, send, recv, peer):
        push(part, part, n, send, recv, peer)

    shared = []

    def share(du, dv):
        part = piece((u + du) % 4, (v + dv) % 4)
        same(part, len(shared), s_send, s_recv, sibling)
        shared.append((du, dv))

    same(half(v, 0), 0, a_send, a_recv, right_v)
    same(half(v, 1), 3, a_send, a_recv, left_v)
    same(half(v, 1), 1, a_send, a_recv, right_v)
    same(half(v, 0), 4, a_send, a_recv, left_v)
    same(marks(v), 0, ai_send, ai_recv, right_v)
    same(marks(v), 1, ai_send, ai_recv, left_v)
    same(piece(u, v), 0, b_send, b_recv, right_u)
    same(piece(u, v), 4, b_send, b_recv, left_u)
    share(0, 0)
    got(half(vl, 0), 0, a_send, a_recv)
    same(half(vl, 0), 2, a_send, a_recv, right_v)
    got(half(vr, 1), 3, a_send, a_recv)
    same(half(vr, 1), 5, a_send, a_recv, left_v)
    got(half(vl, 1), 1, a_send, a_recv)
    got(marks(vl), 0, ai_send, ai_recv)
    same(marks(vl), 2, ai_send, ai_recv, right_v)
    same(piece(u, vl), 1, b_send, b_recv, right_u)
    same(piece(u, vl), 5, b_send, b_recv, left_u)
    share(0, 3)
    got(half(vr, 0), 4, a_send, a_recv)
    got(marks(vr), 1, ai_send, ai_recv)
    same(piece(u, vr), 2, b_send, b_recv, right_u)
    same(piece(u, vr), 6, b_send, b_recv, left_u)
    share(0, 1)
    got(half(vo, 0), 2, a_send, a_recv)
    got(half(vo, 1), 5, a_send, a_recv)
    got(marks(vo), 2, ai_send, ai_recv)
    same(piece(u, vo), 3, b_send, b_recv, right_u)
    same(piece(u, vo), 7, b_send, b_recv, left_u)
    share(0, 2)
    same(all_marks(u), 0, bi_send, bi_recv, right_u)
    same(all_marks(u), 1, bi_send, bi_recv, left_u)

    got(piece(ul, v), 0, b_send, b_recv)
    same(piece(ul, v), 8, b_send, b_recv, right_u)
    share(3, 0)
    got(piece(ul, vl), 1, b_send, b_recv)
    same(piece(ul, vl), 9, b_send, b_recv, right_u)
    share(3, 3)

    got(recv_q, 1, p_send, p_recv)
    for h in range(8):
        s = slice(128 * h, 128 * h + 128)
        if h < 4:
            own = parts[f, :, pl.ds(pl.multiple_of(512 * f + 128 * h, 128), 128)]
        else:
            own = parts[2 * f, :, pl.ds(pl.multiple_of(512 * other + 128 * (h - 4), 128), 128)]
        whole = own + recv_q[:, s].astype(F32) + extra[:, s]
        q_buf[:, s] = (rotate(whole) * QUERY_SCALE).astype(BF16)
    push(q_buf.at[:, far], qx.at[1], 1, e_send, e_recv, pair)
    keep(q_buf.at[:, near], qx.at[0], 3)

    got(piece(ur, vr), 6, b_send, b_recv)
    same(piece(ur, vr), 10, b_send, b_recv, left_u)
    share(1, 1)
    got(piece(ur, vo), 7, b_send, b_recv)
    same(piece(ur, vo), 11, b_send, b_recv, left_u)
    share(1, 2)
    got(all_marks(ul), 0, bi_send, bi_recv)
    same(all_marks(ul), 2, bi_send, bi_recv, right_u)
    got(all_marks(ur), 1, bi_send, bi_recv)
    got(piece(ul, vr), 2, b_send, b_recv)
    share(3, 1)
    got(piece(ul, vo), 3, b_send, b_recv)
    share(3, 2)
    got(piece(ur, v), 4, b_send, b_recv)
    share(1, 0)
    got(piece(ur, vl), 5, b_send, b_recv)
    share(1, 3)
    got(all_marks(uo), 2, bi_send, bi_recv)
    same(idg.at[j], 16, s_send, s_recv, sibling)
    got(piece(uo, v), 8, b_send, b_recv)
    share(2, 0)
    got(piece(uo, vr), 10, b_send, b_recv)
    share(2, 1)
    got(piece(uo, vl), 9, b_send, b_recv)
    share(2, 3)
    got(piece(uo, vo), 11, b_send, b_recv)
    share(2, 2)

    got(dox.at[1], 3, e_send, e_recv)
    got(lowx.at[1], 2, e_send, e_recv)
    got(qx.at[1], 1, e_send, e_recv)
    for n, (du, dv) in enumerate(shared):
        got(kvg.at[i, pl.ds(slot((v + du) % 4, (u + dv) % 4, 0), 4)], n, s_send, s_recv)
    got(idg.at[i], 16, s_send, s_recv)
    for copy in local[2:]:
        copy.wait()
    for copy in sent:
        copy.wait_send()


def project(x, gain, codes, sq, bs, downt, up, cosine, sine, table, doc, do):
    vmem = pl.BlockSpec(memory_space=pltpu.VMEM)
    hbm = pl.BlockSpec(memory_space=pl.ANY)
    dma = pltpu.SemaphoreType.DMA
    counts = (2, 2, 4, 4, 4, 2, 2, 3, 3, 6, 6, 3, 3, 12, 12, 3, 3, 17, 17)
    return pl.pallas_call(
        project_kernel,
        name="project",
        out_shape=(
            jax.ShapeDtypeStruct((128, 4096), BF16),
            jax.ShapeDtypeStruct((2, 128, 512), BF16),
            jax.ShapeDtypeStruct((2, 128, 512), BF16),
            jax.ShapeDtypeStruct((2, 64, 128, 256), BF16),
            jax.ShapeDtypeStruct((2, 64, 8, 128), I32),
            jax.ShapeDtypeStruct((2, 16, 128), BF16),
        ),
        in_specs=[vmem] * 12,
        out_specs=(vmem, vmem, hbm, hbm, hbm, hbm),
        scratch_shapes=[
            pltpu.VMEM((1024, 1024), BF16),
            pltpu.VMEM((3, 32, 1024), F32),
            pltpu.VMEM((256, 1024), BF16),
            pltpu.VMEM((128, 1024), F32),
            pltpu.VMEM((3, 128, 1024), F32),
            pltpu.VMEM((128, 512), BF16),
            pltpu.VMEM((128, 512), BF16),
            pltpu.VMEM((128, 1024), BF16),
            pltpu.VMEM((128, 1024), BF16),
            pltpu.VMEM((128, 1024), F32),
            pltpu.VMEM((2, 128, 256), BF16),
            pltpu.VMEM((128, 1024), BF16),
            pltpu.VMEM((16, 128), BF16),
            pltpu.VMEM((8, 128), I32),
        ]
        + [dma((n,)) for n in counts],
        compiler_params=pltpu.CompilerParams(
            collective_id=0, has_side_effects=True, vmem_limit_bytes=VMEM_LIMIT
        ),
    )(x, gain, codes, sq, bs, downt, up, cosine, sine, table, doc, do)


STEP = 512


def attend_kernel(
    qx_ref, dox_ref, kvg_ref, idg_ref, cos_ref, sin_ref, ox_ref, glx_ref,
    qt, dot_, limits, ahead0, ahead1, max0, max1, run_max, run_sum, acc, acc2,
):
    x, y, z, j, _ = places()
    here = ctx_of(x, y, z, j)
    there = pair_of(x, y, z, j)

    def slot(number, core):
        a, b, d = number // 16, (number // 4) % 4, number % 4
        first, second = (a * 4 + b) * 4 + d, (b * 4 + a) * 4 + d
        if isinstance(core, int):
            return second if core else first
        return jnp.where(core == 0, first, second)

    def block(number):
        return jnp.concatenate([kvg_ref[0, slot(number, 0)], kvg_ref[1, slot(number, 1)]], axis=0)

    every = idg_ref[...].reshape(128, 8, 128)
    below = [
        jnp.sum(jnp.sum(jnp.where(every < d, 1, 0), axis=0), axis=1, keepdims=True)[0:1, :] for d in (1, 2, 3)
    ]
    lane = lax.broadcasted_iota(I32, (1, 128), 1)
    for t, place in enumerate((here, there)):
        ids = idg_ref[j, slot(place // 2, j), 0:1, :]
        start = jnp.zeros((1, 128), I32)
        for d in (1, 2, 3):
            start = jnp.where(ids == d, below[d - 1], start)
        limits[t, 0:1, :] = jnp.concatenate([start, start], axis=1)
        position = place * 128 + lane
        limits[t, 1:2, :] = jnp.concatenate([position, position], axis=1)
        for g in range(4):
            lanes = slice(128 * g, 128 * g + 128)
            qt[t, :, lanes] = qx_ref[t, :, lanes].T
            dot_[t, :, lanes] = dox_ref[t, :, lanes].T
    run_max[...] = jnp.full_like(run_max, -1e29)
    run_sum[...] = jnp.zeros_like(run_sum)
    acc[...] = jnp.zeros_like(acc)
    acc2[...] = jnp.zeros_like(acc2)

    def rows(t, carry):
        place = jnp.where(t == 0, here, there)
        first = jnp.min(limits[t, 0:1, :]) // STEP
        latest = jnp.max(limits[t, 0:1, :])
        stop = (place * 128 + 127) // STEP + 1

        def scores_of(number, masked, ahead, ahead_max):
            key = jnp.minimum(number, 31) * 2
            base = number * STEP
            for h in range(2):
                keys = block(key + h)[:, :128]
                for p in range(2):
                    cols = slice(256 * p, 256 * p + 256)
                    scores = jnp.dot(keys, qt[t, :, cols], preferred_element_type=F32)
                    if masked:
                        pos = base + 256 * h + lax.broadcasted_iota(I32, (256, 256), 0)
                        allowed = (pos >= limits[t, 0:1, :]) & (pos <= limits[t, 1:2, :])
                        scores = jnp.where(allowed, scores, -1e30)
                    ahead[256 * h : 256 * h + 256, cols] = scores
                    top = jnp.max(scores, axis=0, keepdims=True)
                    ahead_max[h : h + 1, cols] = top

        def is_edge(number):
            return (number * STEP < latest) | (number * STEP + STEP - 1 > place * 128)

        def step(number, masked, ahead, ahead_max, later, later_max):
            scores_of(number + 1, masked, later, later_max)
            kv = jnp.concatenate([block(2 * number), block(2 * number + 1)], axis=0)
            kvt = kv.T
            values = kv[:, 128:]
            for p in range(2):
                cols = slice(256 * p, 256 * p + 256)
                tops = jnp.maximum(ahead_max[0:1, cols], ahead_max[1:2, cols])
                old = run_max[t, 0:1, cols]
                new = jnp.maximum(old, tops)
                decay = jnp.exp2(old - new)
                run_max[t, 0:1, cols] = new
                grad_dots = jnp.dot(values, dot_[t, :, cols], preferred_element_type=F32)
                expo = jnp.exp2(ahead[:, cols] - new)
                run_sum[t, 0:1, cols] = run_sum[t, 0:1, cols] * decay + jnp.sum(expo, axis=0, keepdims=True)
                weighted = (expo * grad_dots).astype(BF16)
                acc[t, :, cols] = acc[t, :, cols] * decay + jnp.dot(
                    kvt, expo.astype(BF16), preferred_element_type=F32
                )
                acc2[t, :, cols] = acc2[t, :, cols] * decay + jnp.dot(
                    kvt[:128], weighted, preferred_element_type=F32
                )

        scores_of(first, True, ahead0, max0)

        def one(number, *buffers):
            edge = is_edge(number + 1)

            @pl.when(edge)
            def _():
                step(number, True, *buffers)

            @pl.when(jnp.logical_not(edge))
            def _():
                step(number, False, *buffers)

        def body(twice, c):
            number = first + 2 * twice
            one(number, ahead0, max0, ahead1, max1)

            @pl.when(number + 1 < stop)
            def _():
                one(number + 1, ahead1, max1, ahead0, max0)

            return c

        lax.fori_loop(0, (stop - first + 1) // 2, body, 0)
        return carry

    lax.fori_loop(0, 2, rows, 0)

    for t in range(2):
        cosine, sine = cos_ref[t], sin_ref[t]
        for g in range(4):
            lanes = slice(128 * g, 128 * g + 128)
            inverse = 1.0 / run_sum[t, 0:1, lanes]
            out = acc[t, 128:256, lanes] * inverse
            mean_dot = jnp.sum(dot_[t, :, lanes].astype(F32) * out, axis=0, keepdims=True)
            grad = (acc2[t, :, lanes] - mean_dot * acc[t, 0:128, lanes]) * (inverse * SOFT_SCALE)
            ga, gb = grad[:64], grad[64:]
            back = jnp.concatenate([ga * cosine + gb * sine, gb * cosine - ga * sine], axis=0)
            ox_ref[t, :, lanes] = out.T.astype(BF16)
            glx_ref[t, :, lanes] = back.T.astype(BF16)


def attend(qx, dox, kvg, idg, cosine, sine):
    vmem = pl.BlockSpec(memory_space=pltpu.VMEM)
    return pl.pallas_call(
        attend_kernel,
        name="attend",
        out_shape=(jax.ShapeDtypeStruct((2, 128, 512), BF16), jax.ShapeDtypeStruct((2, 128, 512), BF16)),
        in_specs=[vmem] * 6,
        out_specs=(vmem, vmem),
        scratch_shapes=[
            pltpu.VMEM((2, 128, 512), BF16),
            pltpu.VMEM((2, 128, 512), BF16),
            pltpu.VMEM((2, 8, 256), I32),
            pltpu.VMEM((512, 512), F32),
            pltpu.VMEM((512, 512), F32),
            pltpu.VMEM((8, 512), F32),
            pltpu.VMEM((8, 512), F32),
            pltpu.VMEM((2, 8, 512), F32),
            pltpu.VMEM((2, 8, 512), F32),
            pltpu.VMEM((2, 256, 512), F32),
            pltpu.VMEM((2, 128, 512), F32),
        ],
        compiler_params=pltpu.CompilerParams(vmem_limit_bytes=VMEM_LIMIT),
    )(qx, dox, kvg, idg, cosine, sine)


def reduce_kernel(
    ox_ref, glx_ref, lowx_ref, normed_ref, up_ref,
    attn_ref, grad_at_ref, up_out_ref,
    mid_send, mid_recv, buf, rcore, b1, rp, b3, rz, final,
    p_send, p_recv, x_send, x_recv, z_send, z_recv, g_send, g_recv,
):
    x, y, z, j, f = places()
    i = 1 - j
    sibling = ctx_of(x, y, z, i)
    flat = x * 4 + y
    plane = [(flat + d) % 16 for d in range(1, 16)]
    whole_z = f * 4 + z
    zs = [(whole_z + d) % 8 for d in range(1, 8)]

    pair = pair_of(x, y, z, j)
    k = z // 2
    barrier = pltpu.get_barrier_semaphore()
    peers = [(sibling, f), (pair, f)]
    peers += [(ctx_of(p // 4, p % 4, z, j), f) for p in plane]
    peers += [(ctx_of(x, y, p % 4, j), p // 4) for p in zs]
    for peer in peers:
        pl.semaphore_signal(barrier, inc=1, device_id=peer, device_id_type=MESH)

    glx = jnp.concatenate([glx_ref[0], glx_ref[1]], axis=0)
    up = up_ref[:, pl.ds(pl.multiple_of(512 * k, 512), 512)]
    midt = ADAPTER_SCALE * lax.dot_general(
        up, glx, (((1,), (1,)), ((), ())), preferred_element_type=F32
    )
    mid_send[0] = midt[:, 0:128]
    mid_send[1] = midt[:, 128:256]
    pl.semaphore_wait(barrier, len(peers))

    sent = []
    mid_copy = remote(mid_send.at[1], mid_recv, p_send.at[0], p_recv.at[0], pair, f)
    mid_copy.start()
    near = pl.ds(pl.multiple_of(512 * k, 512), 512)
    out_copy = remote(ox_ref.at[1], attn_ref.at[:, near], p_send.at[1], p_recv.at[1], pair, f)
    attn_ref[:, near] = ox_ref[0]

    lowt = jnp.concatenate([lowx_ref[0], lowx_ref[1]], axis=1)
    upg = ADAPTER_SCALE * jnp.dot(lowt, glx, preferred_element_type=F32)
    buf[64:96] = jnp.zeros((32, 8, 128), F32)
    for s in range(2):
        for t in range(4):
            buf[64 + 16 * s + 8 * f + 4 * k + t] = upg[8 * s : 8 * s + 8, 128 * t : 128 * t + 128]
    mid_copy.wait()
    mid = (mid_send[0] + mid_recv[...]).astype(BF16)
    for t in range(4):
        part = jnp.dot(mid, normed_ref[:, 1024 * t : 1024 * t + 1024], preferred_element_type=F32)
        for s in range(2):
            for w in range(8):
                buf[32 * s + 8 * t + w] = part[8 * s : 8 * s + 8, 128 * w : 128 * w + 128]

    core_copy = remote(buf.at[pl.ds(48 * i, 48)], rcore, p_send.at[2], p_recv.at[2], sibling, f)
    core_copy.start()
    core_copy.wait()
    b1[...] = buf[pl.ds(48 * j, 48)] + rcore[...]
    copies = []
    for n, p in enumerate(plane):
        peer = ctx_of(p // 4, p % 4, z, j)
        copy = remote(b1.at[pl.ds(3 * p, 3)], rp.at[n], x_send.at[n], x_recv.at[n], peer, f)
        copy.start()
        copies.append(copy)
    out_copy.start()
    added = b1[pl.ds(3 * flat, 3)]
    for n, copy in enumerate(copies):
        copy.wait()
        added = added + rp[n]
    b3[...] = added
    copies = []
    for n, p in enumerate(zs):
        copy = remote(b3, rz.at[whole_z], z_send.at[n], z_recv.at[n], ctx_of(x, y, p % 4, j), p // 4)
        copy.start()
        copies.append(copy)
    rz[whole_z] = b3[...]
    for n, copy in enumerate(copies):
        source = (whole_z + 7 - n) % 8
        remote(rz.at[source], rz.at[source], z_send.at[n], z_recv.at[n], sibling, f).wait_recv()
    added = rz[0]
    for n in range(1, 8):
        added = added + rz[n]
    row = 48 * j + 3 * flat
    final[pl.ds(row, 3)] = added
    sent += copies

    for n, p in enumerate(plane):
        part = final.at[pl.ds(row, 3)]
        copy = remote(part, part, g_send.at[n], g_recv.at[n], ctx_of(p // 4, p % 4, z, j), f)
        copy.start()
        sent.append(copy)
    for n in range(15):
        part = final.at[pl.ds(48 * j + 3 * ((flat + 15 - n) % 16), 3)]
        remote(part, part, g_send.at[n], g_recv.at[n], sibling, f).wait_recv()
    part = final.at[pl.ds(48 * j, 48)]
    copy = remote(part, part, p_send.at[3], p_recv.at[3], sibling, f)
    copy.start()
    sent.append(copy)
    part = final.at[pl.ds(48 * i, 48)]
    remote(part, part, p_send.at[3], p_recv.at[3], sibling, f).wait_recv()

    for s in range(2):
        for t in range(32):
            grad_at_ref[8 * s : 8 * s + 8, 128 * t : 128 * t + 128] = final[32 * s + t]
        for t in range(8):
            up_out_ref[8 * s : 8 * s + 8, 128 * t : 128 * t + 128] = final[64 + 16 * s + 8 * f + t]

    other_half = attn_ref.at[:, pl.ds(pl.multiple_of(512 * (1 - k), 512), 512)]
    remote(ox_ref.at[1], other_half, p_send.at[1], p_recv.at[1], sibling, f).wait_recv()
    out_copy.wait_send()
    for copy in sent:
        copy.wait_send()


def reduce_all(ox, glx, lowx, normed, up):
    vmem = pl.BlockSpec(memory_space=pltpu.VMEM)
    hbm = pl.BlockSpec(memory_space=pl.ANY)
    dma = pltpu.SemaphoreType.DMA
    tiles = lambda *lead: pltpu.VMEM((*lead, 8, 128), F32)
    return pl.pallas_call(
        reduce_kernel,
        name="reduce_all",
        out_shape=(
            jax.ShapeDtypeStruct((128, 1024), BF16),
            jax.ShapeDtypeStruct((16, 4096), F32),
            jax.ShapeDtypeStruct((16, 1024), F32),
        ),
        in_specs=[vmem] * 5,
        out_specs=(vmem, vmem, vmem),
        scratch_shapes=[
            pltpu.VMEM((2, 16, 128), F32),
            pltpu.VMEM((16, 128), F32),
            tiles(96), tiles(48), tiles(48), tiles(15, 3), tiles(3), tiles(8, 3),
            tiles(96),
        ]
        + [dma((n,)) for n in (4, 4, 15, 15, 7, 7, 15, 15)],
        compiler_params=pltpu.CompilerParams(
            collective_id=1, has_side_effects=True, vmem_limit_bytes=VMEM_LIMIT
        ),
    )(ox, glx, lowx, normed, up)


def hand_over_kernel(a_ref, b_ref, c_ref, a_out, b_out, c_out):
    a_out[...] = a_ref[...]
    b_out[...] = b_ref[...]
    c_out[...] = c_ref[...]


def hand_over(*arrays):
    vmem = pl.BlockSpec(memory_space=pltpu.VMEM)
    return pl.pallas_call(
        hand_over_kernel,
        name="hand_over",
        out_shape=tuple(jax.ShapeDtypeStruct(a.shape, a.dtype) for a in arrays),
        in_specs=[vmem] * 3,
        out_specs=(vmem,) * 3,
        compiler_params=pltpu.CompilerParams(vmem_limit_bytes=VMEM_LIMIT),
    )(*arrays)


def on_device(
    layer_input,
    gain,
    codes,
    column_scale_quantized,
    block_second_scale,
    query_down_map,
    query_up_map,
    token_document,
    output_cotangent,
):
    x, y, z, j, _ = places()
    places_two = jnp.stack([ctx_of(x, y, z, j), pair_of(x, y, z, j)])
    freqs = jnp.exp(jnp.arange(HEAD // 2, dtype=F32) * (-2.0 * math.log(ROPE_BASE) / HEAD))
    positions = (places_two[:, None] * 128 + jnp.arange(128, dtype=I32)[None, :]).astype(F32)
    angle = positions[:, None, :] * freqs[None, :, None]
    cosine, sine = jnp.cos(angle), jnp.sin(angle)
    table = jnp.broadcast_to(jnp.asarray(NF4_LEVELS, F32)[:, None], (16, 128))

    normed, dox, qx, kvg, idg, lowx = project(
        layer_input,
        gain[None, :],
        codes,
        column_scale_quantized,
        block_second_scale[None, :],
        query_down_map.T,
        query_up_map,
        cosine,
        sine,
        table,
        token_document[None, :],
        output_cotangent,
    )
    ox, glx = attend(qx, dox, kvg, idg, cosine, sine)
    attn, grad_at, up_map_gradient = reduce_all(ox, glx, lowx, normed, query_up_map)
    attn, grad_at, up_map_gradient = hand_over(attn, grad_at, up_map_gradient)
    return (attn, grad_at.T, up_map_gradient)


def solution(mesh):
    return jax.shard_map(
        on_device,
        mesh=mesh,
        in_specs=(
            P("ctx", None),
            P(),
            P("fsdp", None),
            P("fsdp", None),
            P(),
            P(),
            P(None, "fsdp"),
            P("ctx"),
            P("ctx", "fsdp"),
        ),
        out_specs=(P("ctx", "fsdp"), P(), P(None, "fsdp")),
        check_vma=False,
    )
```

```python
import functools
import math

import jax
import jax.numpy as jnp
import numpy as np
from jax import lax
from jax.experimental import pallas as pl
from jax.experimental.pallas import tpu as pltpu
from jax.sharding import PartitionSpec as P

MESH = pl.DeviceIdType.MESH
HEAD = 128
NF4_LEVELS = [
    -1.0,
    -0.6961928009986877,
    -0.5250730514526367,
    -0.39491748809814453,
    -0.28444138169288635,
    -0.18477343022823334,
    -0.09105003625154495,
    0.0,
    0.07958029955625534,
    0.16093020141124725,
    0.24611230194568634,
    0.33791524171829224,
    0.44070982933044434,
    0.5626170039176941,
    0.7229568362236023,
    1.0,
]
ADAPTER_SCALE = 2.0
ROPE_BASE = 500000.0
SOFT_SCALE = 1.0 / math.sqrt(HEAD)
QUERY_SCALE = SOFT_SCALE * math.log2(math.e)
F32, BF16, I32 = jnp.float32, jnp.bfloat16, jnp.int32
VMEM_LIMIT = 60 * 1024 * 1024


def places():
    c = lax.axis_index("ctx")
    f = lax.axis_index("fsdp")
    return c // 32, (c // 8) % 4, (c // 2) % 4, c % 2, f


def ctx_of(x, y, z, j):
    return ((x * 4 + y) * 4 + z) * 2 + j


def pair_of(x, y, z, j):
    return ctx_of(3 - x, 3 - y, (z + 2) % 4, j)


def lookup(table, index):
    return lax.gather(
        table,
        index[..., None],
        lax.GatherDimensionNumbers(
            offset_dims=(),
            collapsed_slice_dims=(0,),
            start_index_map=(0,),
            operand_batching_dims=(1,),
            start_indices_batching_dims=(1,),
        ),
        slice_sizes=(1, 1),
        mode=lax.GatherScatterMode.PROMISE_IN_BOUNDS,
    )


def remote(src, dst, send, recv, ctx, f):
    return pltpu.make_async_remote_copy(
        src_ref=src, dst_ref=dst, send_sem=send, recv_sem=recv, device_id=(ctx, f), device_id_type=MESH
    )


def project_kernel(
    x_ref, gain_ref, codes_ref, sq_ref, bs_ref, downt_ref, up_ref, cos_ref, sin_ref, table_ref, doc_ref, do_ref,
    normed_ref, dox, qx, kvg, idg, lowx,
    perm, scale, w_buf, acc, parts, send_kv, recv_kv, send_q, recv_q, extra, kv_buf, q_buf, low_buf, ids_buf,
    p_send, p_recv, e_send, e_recv, own_sem, z_send, z_recv, zi_send, zi_recv, a_send, a_recv, ai_send, ai_recv,
    b_send, b_recv, bi_send, bi_recv, s_send, s_recv,
):
    x, y, z, j, f = places()
    here = lax.axis_index("ctx")
    other = 1 - f
    i = 1 - j
    k = z // 2
    u = x * i + y * j
    v = y * i + x * j

    def at(uu, vv, zz):
        return ctx_of(uu * i + vv * j, vv * i + uu * j, zz, j)

    def slot(uu, vv, zz):
        return (uu * 4 + vv) * 4 + zz

    sibling = ctx_of(x, y, z, i)
    pair = pair_of(x, y, z, j)
    zo = (z + 2) % 4
    zn = z + 1 - 2 * (z % 2)
    zf = (zn + 2) % 4
    across, next_z, far_z = at(u, v, zo), at(u, v, zn), at(u, v, zf)
    vr, vl, vo = (v + 1) % 4, (v + 3) % 4, (v + 2) % 4
    ur, ul, uo = (u + 1) % 4, (u + 3) % 4, (u + 2) % 4
    right_v, left_v = at(u, vr, z), at(u, vl, z)
    right_u, left_u = at(ur, v, z), at(ul, v, z)

    barrier = pltpu.get_barrier_semaphore()
    pl.semaphore_signal(barrier, inc=1, device_id=(here, other), device_id_type=MESH)
    peers = [sibling, pair, across, next_z, far_z, right_v, left_v, right_u, left_u]
    for peer in peers:
        pl.semaphore_signal(barrier, inc=1, device_id=(peer, f), device_id_type=MESH)

    for r in range(8):
        wide = x_ref[16 * r : 16 * r + 16, :].astype(F32)
        inverse = lax.rsqrt(jnp.mean(wide * wide, axis=-1, keepdims=True) + 1e-05)
        normed_ref[16 * r : 16 * r + 16, :] = (wide * inverse * gain_ref[...]).astype(BF16)
    ids_buf[...] = jnp.broadcast_to(doc_ref[...], (8, 128))
    near = pl.ds(pl.multiple_of(512 * k, 512), 512)
    far = pl.ds(pl.multiple_of(512 * (1 - k), 512), 512)
    dox[0] = do_ref[:, near]

    sent = []

    def push(src, dst, n, send, recv, peer, group=f):
        copy = remote(src, dst, send.at[n], recv.at[n], peer, group)
        copy.start()
        sent.append(copy)

    def got(ref, n, send, recv):
        remote(ref, ref, send.at[n], recv.at[n], sibling, f).wait_recv()

    mine = slot(u, v, z)
    pl.semaphore_wait(barrier, len(peers) + 1)
    push(do_ref.at[:, far], dox.at[1], 3, e_send, e_recv, pair)
    for n, peer in enumerate((next_z, across, far_z)):
        push(ids_buf, idg.at[j, mine], n, zi_send, zi_recv, peer)

    for part in range(8):
        m = lax.broadcasted_iota(I32, (128, 1024), 0)
        column = lax.broadcasted_iota(I32, (128, 1024), 1)
        perm[128 * part : 128 * part + 128, :] = jnp.where(column == 8 * m + part, 1.0, 0.0).astype(BF16)
    pick = lax.broadcasted_iota(I32, (32, 64), 1) == lax.broadcasted_iota(I32, (32, 64), 0) + 32 * f
    second = jnp.sum(jnp.where(pick, bs_ref[...], 0.0), axis=1, keepdims=True) * (1.0 / 256.0)
    quantized = jnp.concatenate([sq_ref[:, 1024 * t : 1024 * t + 1024] for t in range(3)], axis=0)
    packed = lax.dot_general(
        (quantized.astype(F32) + 1.0).astype(BF16),
        perm[...],
        (((1,), (1,)), ((), ())),
        preferred_element_type=F32,
    )
    for t in range(3):
        scale[t] = packed[32 * t : 32 * t + 32] * second

    lower, upper = table_ref[0:8, :], table_ref[8:16, :]

    def tile(t):
        lane = pl.multiple_of(t * 128, 128)
        acc[...] = jnp.zeros_like(acc)

        def chunk(kc, carry):
            for b in range(4):
                row = pl.multiple_of(kc * 256 + b * 64, 64)
                words = codes_ref[pl.ds(row, 64), pl.ds(lane, 128)]
                scale_row = scale[t, pl.ds(kc * 4 + b, 1), :]
                for n in range(8):
                    rows = []
                    for r in range(8):
                        word = words[8 * r : 8 * r + 8]
                        index = jnp.bitwise_and(jnp.right_shift(word, 4 * n), 7)
                        high = jnp.left_shift(word, 28 - 4 * n) < 0
                        rows.append(jnp.where(high, lookup(upper, index), lookup(lower, index)))
                    w_buf[64 * b : 64 * b + 64, 128 * n : 128 * n + 128] = (
                        jnp.concatenate(rows, axis=0) * scale_row[:, 128 * n : 128 * n + 128]
                    ).astype(BF16)
            col = pl.multiple_of(f * 2048 + kc * 256, 256)
            acc[...] += jnp.dot(normed_ref[:, pl.ds(col, 256)], w_buf[...], preferred_element_type=F32)
            return carry

        lax.fori_loop(0, 8, chunk, 0)
        full = acc[...]
        high = full.astype(BF16)
        low = (full - high.astype(F32)).astype(BF16)
        natural = jnp.dot(jnp.concatenate([high, low], axis=0), perm[...], preferred_element_type=F32)
        parts[t] = natural[0:128] + natural[128:256]

    def columns(t, offset):
        return parts[t, :, pl.ds(pl.multiple_of(offset, 512), 512)]

    tile(2 - f)
    send_kv[...] = columns(2 - f, 512 * other).astype(BF16)
    push(send_kv, recv_kv, 0, p_send, p_recv, here, other)
    tile(other)
    send_q[:, 0:512] = columns(other, 512 * other).astype(BF16)
    send_q[:, 512:1024] = columns(2 * other, 512 * f).astype(BF16)
    tile(2 * f)

    cosine, sine = cos_ref[0].T, sin_ref[0].T
    cosine = jnp.concatenate([cosine, cosine], axis=1)
    sine = jnp.concatenate([-sine, sine], axis=1)

    def rotate(vector):
        return vector * cosine + pltpu.roll(vector, 64, 1) * sine

    got(recv_kv, 0, p_send, p_recv)
    both = columns(1 + f, 512 * f) + recv_kv[...].astype(F32)
    for h in range(2):
        kv_buf[h, :, 0:128] = rotate(both[:, 128 * h : 128 * h + 128]).astype(BF16)
        kv_buf[h, :, 128:256] = both[:, 256 + 128 * h : 384 + 128 * h].astype(BF16)

    push(kv_buf.at[1 - k], kvg.at[j, mine], 0, e_send, e_recv, across)
    push(kv_buf.at[k], kvg.at[j, mine], 0, z_send, z_recv, next_z)
    local = []

    def keep(src, dst, n):
        copy = pltpu.make_async_copy(src, dst, own_sem.at[n])
        copy.start()
        local.append(copy)

    keep(kv_buf.at[k], kvg.at[j, mine], 0)
    keep(ids_buf, idg.at[j, mine], 1)

    lowt = lax.dot_general(
        downt_ref[...], normed_ref[...], (((1,), (1,)), ((), ())), preferred_element_type=F32
    ).astype(BF16)
    low_buf[...] = lowt
    extra[...] = ADAPTER_SCALE * lax.dot_general(
        lowt, up_ref[...], (((0,), (0,)), ((), ())), preferred_element_type=F32
    )

    block = kvg.at[j, slot(u, v, zo)]
    got(block, 0, e_send, e_recv)
    push(block, block, 1, z_send, z_recv, next_z)
    push(send_q, recv_q, 1, p_send, p_recv, here, other)
    push(low_buf, lowx.at[1], 2, e_send, e_recv, pair)
    keep(low_buf, lowx.at[0], 2)

    got(kvg.at[j, slot(u, v, zn)], 0, z_send, z_recv)
    for n, zz in enumerate((zn, zo, zf)):
        got(idg.at[j, slot(u, v, zz)], n, zi_send, zi_recv)
    local[0].wait()
    local[1].wait()
    got(kvg.at[j, slot(u, v, zf)], 1, z_send, z_recv)

    def half(vv, h):
        return kvg.at[j, pl.ds(slot(u, vv, 0) + 2 * h, 2)]

    def piece(uu, vv):
        return kvg.at[j, pl.ds(slot(uu, vv, 0), 4)]

    def marks(vv):
        return idg.at[j, pl.ds(slot(u, vv, 0), 4)]

    def all_marks(uu):
        return idg.at[j, pl.ds(slot(uu, 0, 0), 16)]

    def same(part, n, send, recv, peer):
        push(part, part, n, send, recv, peer)

    shared = []

    def share(du, dv):
        part = piece((u + du) % 4, (v + dv) % 4)
        same(part, len(shared), s_send, s_recv, sibling)
        shared.append((du, dv))

    same(half(v, 0), 0, a_send, a_recv, right_v)
    same(half(v, 1), 3, a_send, a_recv, left_v)
    same(half(v, 1), 1, a_send, a_recv, right_v)
    same(half(v, 0), 4, a_send, a_recv, left_v)
    same(marks(v), 0, ai_send, ai_recv, right_v)
    same(marks(v), 1, ai_send, ai_recv, left_v)
    same(piece(u, v), 0, b_send, b_recv, right_u)
    same(piece(u, v), 4, b_send, b_recv, left_u)
    share(0, 0)
    got(half(vl, 0), 0, a_send, a_recv)
    same(half(vl, 0), 2, a_send, a_recv, right_v)
    got(half(vr, 1), 3, a_send, a_recv)
    same(half(vr, 1), 5, a_send, a_recv, left_v)
    got(half(vl, 1), 1, a_send, a_recv)
    got(marks(vl), 0, ai_send, ai_recv)
    same(marks(vl), 2, ai_send, ai_recv, right_v)
    same(piece(u, vl), 1, b_send, b_recv, right_u)
    same(piece(u, vl), 5, b_send, b_recv, left_u)
    share(0, 3)
    got(half(vr, 0), 4, a_send, a_recv)
    got(marks(vr), 1, ai_send, ai_recv)
    same(piece(u, vr), 2, b_send, b_recv, right_u)
    same(piece(u, vr), 6, b_send, b_recv, left_u)
    share(0, 1)
    got(half(vo, 0), 2, a_send, a_recv)
    got(half(vo, 1), 5, a_send, a_recv)
    got(marks(vo), 2, ai_send, ai_recv)
    same(piece(u, vo), 3, b_send, b_recv, right_u)
    same(piece(u, vo), 7, b_send, b_recv, left_u)
    share(0, 2)
    same(all_marks(u), 0, bi_send, bi_recv, right_u)
    same(all_marks(u), 1, bi_send, bi_recv, left_u)

    got(piece(ul, v), 0, b_send, b_recv)
    same(piece(ul, v), 8, b_send, b_recv, right_u)
    share(3, 0)
    got(piece(ul, vl), 1, b_send, b_recv)
    same(piece(ul, vl), 9, b_send, b_recv, right_u)
    share(3, 3)

    got(recv_q, 1, p_send, p_recv)
    for h in range(8):
        s = slice(128 * h, 128 * h + 128)
        if h < 4:
            own = parts[f, :, pl.ds(pl.multiple_of(512 * f + 128 * h, 128), 128)]
        else:
            own = parts[2 * f, :, pl.ds(pl.multiple_of(512 * other + 128 * (h - 4), 128), 128)]
        whole = own + recv_q[:, s].astype(F32) + extra[:, s]
        q_buf[:, s] = (rotate(whole) * QUERY_SCALE).astype(BF16)
    push(q_buf.at[:, far], qx.at[1], 1, e_send, e_recv, pair)
    keep(q_buf.at[:, near], qx.at[0], 3)

    got(piece(ur, vr), 6, b_send, b_recv)
    same(piece(ur, vr), 10, b_send, b_recv, left_u)
    share(1, 1)
    got(piece(ur, vo), 7, b_send, b_recv)
    same(piece(ur, vo), 11, b_send, b_recv, left_u)
    share(1, 2)
    got(all_marks(ul), 0, bi_send, bi_recv)
    same(all_marks(ul), 2, bi_send, bi_recv, right_u)
    got(all_marks(ur), 1, bi_send, bi_recv)
    got(piece(ul, vr), 2, b_send, b_recv)
    share(3, 1)
    got(piece(ul, vo), 3, b_send, b_recv)
    share(3, 2)
    got(piece(ur, v), 4, b_send, b_recv)
    share(1, 0)
    got(piece(ur, vl), 5, b_send, b_recv)
    share(1, 3)
    got(all_marks(uo), 2, bi_send, bi_recv)
    same(idg.at[j], 16, s_send, s_recv, sibling)
    got(piece(uo, v), 8, b_send, b_recv)
    share(2, 0)
    got(piece(uo, vr), 10, b_send, b_recv)
    share(2, 1)
    got(piece(uo, vl), 9, b_send, b_recv)
    share(2, 3)
    got(piece(uo, vo), 11, b_send, b_recv)
    share(2, 2)

    got(dox.at[1], 3, e_send, e_recv)
    got(lowx.at[1], 2, e_send, e_recv)
    got(qx.at[1], 1, e_send, e_recv)
    for n, (du, dv) in enumerate(shared):
        got(kvg.at[i, pl.ds(slot((v + du) % 4, (u + dv) % 4, 0), 4)], n, s_send, s_recv)
    got(idg.at[i], 16, s_send, s_recv)
    for copy in local[2:]:
        copy.wait()
    for copy in sent:
        copy.wait_send()


def project(x, gain, codes, sq, bs, downt, up, cosine, sine, table, doc, do):
    vmem = pl.BlockSpec(memory_space=pltpu.VMEM)
    hbm = pl.BlockSpec(memory_space=pl.ANY)
    dma = pltpu.SemaphoreType.DMA
    counts = (2, 2, 4, 4, 4, 2, 2, 3, 3, 6, 6, 3, 3, 12, 12, 3, 3, 17, 17)
    return pl.pallas_call(
        project_kernel,
        name="project",
        out_shape=(
            jax.ShapeDtypeStruct((128, 4096), BF16),
            jax.ShapeDtypeStruct((2, 128, 512), BF16),
            jax.ShapeDtypeStruct((2, 128, 512), BF16),
            jax.ShapeDtypeStruct((2, 64, 128, 256), BF16),
            jax.ShapeDtypeStruct((2, 64, 8, 128), I32),
            jax.ShapeDtypeStruct((2, 16, 128), BF16),
        ),
        in_specs=[vmem] * 12,
        out_specs=(vmem, vmem, hbm, hbm, hbm, hbm),
        scratch_shapes=[
            pltpu.VMEM((1024, 1024), BF16),
            pltpu.VMEM((3, 32, 1024), F32),
            pltpu.VMEM((256, 1024), BF16),
            pltpu.VMEM((128, 1024), F32),
            pltpu.VMEM((3, 128, 1024), F32),
            pltpu.VMEM((128, 512), BF16),
            pltpu.VMEM((128, 512), BF16),
            pltpu.VMEM((128, 1024), BF16),
            pltpu.VMEM((128, 1024), BF16),
            pltpu.VMEM((128, 1024), F32),
            pltpu.VMEM((2, 128, 256), BF16),
            pltpu.VMEM((128, 1024), BF16),
            pltpu.VMEM((16, 128), BF16),
            pltpu.VMEM((8, 128), I32),
        ]
        + [dma((n,)) for n in counts],
        compiler_params=pltpu.CompilerParams(
            collective_id=0, has_side_effects=True, vmem_limit_bytes=VMEM_LIMIT
        ),
    )(x, gain, codes, sq, bs, downt, up, cosine, sine, table, doc, do)


STEP = 512


def attend_kernel(
    qx_ref, dox_ref, kvg_ref, idg_ref, cos_ref, sin_ref, ox_ref, glx_ref,
    qt, dot_, limits, ahead0, ahead1, max0, max1, run_max, run_sum, acc, acc2,
):
    x, y, z, j, _ = places()
    here = ctx_of(x, y, z, j)
    there = pair_of(x, y, z, j)

    def slot(number, core):
        a, b, d = number // 16, (number // 4) % 4, number % 4
        first, second = (a * 4 + b) * 4 + d, (b * 4 + a) * 4 + d
        if isinstance(core, int):
            return second if core else first
        return jnp.where(core == 0, first, second)

    def block(number):
        return jnp.concatenate([kvg_ref[0, slot(number, 0)], kvg_ref[1, slot(number, 1)]], axis=0)

    every = idg_ref[...].reshape(128, 8, 128)
    below = [
        jnp.sum(jnp.sum(jnp.where(every < d, 1, 0), axis=0), axis=1, keepdims=True)[0:1, :] for d in (1, 2, 3)
    ]
    lane = lax.broadcasted_iota(I32, (1, 128), 1)
    for t, place in enumerate((here, there)):
        ids = idg_ref[j, slot(place // 2, j), 0:1, :]
        start = jnp.zeros((1, 128), I32)
        for d in (1, 2, 3):
            start = jnp.where(ids == d, below[d - 1], start)
        limits[t, 0:1, :] = jnp.concatenate([start, start], axis=1)
        position = place * 128 + lane
        limits[t, 1:2, :] = jnp.concatenate([position, position], axis=1)
        for g in range(4):
            lanes = slice(128 * g, 128 * g + 128)
            qt[t, :, lanes] = qx_ref[t, :, lanes].T
            dot_[t, :, lanes] = dox_ref[t, :, lanes].T
    run_max[...] = jnp.full_like(run_max, -1e29)
    run_sum[...] = jnp.zeros_like(run_sum)
    acc[...] = jnp.zeros_like(acc)
    acc2[...] = jnp.zeros_like(acc2)

    def rows(t, carry):
        place = jnp.where(t == 0, here, there)
        first = jnp.min(limits[t, 0:1, :]) // STEP
        latest = jnp.max(limits[t, 0:1, :])
        stop = (place * 128 + 127) // STEP + 1

        def scores_of(number, masked, ahead, ahead_max):
            key = jnp.minimum(number, 31) * 2
            base = number * STEP
            for h in range(2):
                keys = block(key + h)[:, :128]
                for p in range(2):
                    cols = slice(256 * p, 256 * p + 256)
                    scores = jnp.dot(keys, qt[t, :, cols], preferred_element_type=F32)
                    if masked:
                        pos = base + 256 * h + lax.broadcasted_iota(I32, (256, 256), 0)
                        allowed = (pos >= limits[t, 0:1, :]) & (pos <= limits[t, 1:2, :])
                        scores = jnp.where(allowed, scores, -1e30)
                    ahead[256 * h : 256 * h + 256, cols] = scores
                    top = jnp.max(scores, axis=0, keepdims=True)
                    ahead_max[h : h + 1, cols] = top

        def is_edge(number):
            return (number * STEP < latest) | (number * STEP + STEP - 1 > place * 128)

        def step(number, masked, ahead, ahead_max, later, later_max):
            scores_of(number + 1, masked, later, later_max)
            kv = jnp.concatenate([block(2 * number), block(2 * number + 1)], axis=0)
            kvt = kv.T
            values = kv[:, 128:]
            for p in range(2):
                cols = slice(256 * p, 256 * p + 256)
                tops = jnp.maximum(ahead_max[0:1, cols], ahead_max[1:2, cols])
                old = run_max[t, 0:1, cols]
                new = jnp.maximum(old, tops)
                decay = jnp.exp2(old - new)
                run_max[t, 0:1, cols] = new
                grad_dots = jnp.dot(values, dot_[t, :, cols], preferred_element_type=F32)
                expo = jnp.exp2(ahead[:, cols] - new)
                run_sum[t, 0:1, cols] = run_sum[t, 0:1, cols] * decay + jnp.sum(expo, axis=0, keepdims=True)
                weighted = (expo * grad_dots).astype(BF16)
                acc[t, :, cols] = acc[t, :, cols] * decay + jnp.dot(
                    kvt, expo.astype(BF16), preferred_element_type=F32
                )
                acc2[t, :, cols] = acc2[t, :, cols] * decay + jnp.dot(
                    kvt[:128], weighted, preferred_element_type=F32
                )

        scores_of(first, True, ahead0, max0)

        def one(number, *buffers):
            edge = is_edge(number + 1)

            @pl.when(edge)
            def _():
                step(number, True, *buffers)

            @pl.when(jnp.logical_not(edge))
            def _():
                step(number, False, *buffers)

        def body(twice, c):
            number = first + 2 * twice
            one(number, ahead0, max0, ahead1, max1)

            @pl.when(number + 1 < stop)
            def _():
                one(number + 1, ahead1, max1, ahead0, max0)

            return c

        lax.fori_loop(0, (stop - first + 1) // 2, body, 0)
        return carry

    lax.fori_loop(0, 2, rows, 0)

    for t in range(2):
        cosine, sine = cos_ref[t], sin_ref[t]
        for g in range(4):
            lanes = slice(128 * g, 128 * g + 128)
            inverse = 1.0 / run_sum[t, 0:1, lanes]
            out = acc[t, 128:256, lanes] * inverse
            mean_dot = jnp.sum(dot_[t, :, lanes].astype(F32) * out, axis=0, keepdims=True)
            grad = (acc2[t, :, lanes] - mean_dot * acc[t, 0:128, lanes]) * (inverse * SOFT_SCALE)
            ga, gb = grad[:64], grad[64:]
            back = jnp.concatenate([ga * cosine + gb * sine, gb * cosine - ga * sine], axis=0)
            ox_ref[t, :, lanes] = out.T.astype(BF16)
            glx_ref[t, :, lanes] = back.T.astype(BF16)


def attend(qx, dox, kvg, idg, cosine, sine):
    vmem = pl.BlockSpec(memory_space=pltpu.VMEM)
    return pl.pallas_call(
        attend_kernel,
        name="attend",
        out_shape=(jax.ShapeDtypeStruct((2, 128, 512), BF16), jax.ShapeDtypeStruct((2, 128, 512), BF16)),
        in_specs=[vmem] * 6,
        out_specs=(vmem, vmem),
        scratch_shapes=[
            pltpu.VMEM((2, 128, 512), BF16),
            pltpu.VMEM((2, 128, 512), BF16),
            pltpu.VMEM((2, 8, 256), I32),
            pltpu.VMEM((512, 512), F32),
            pltpu.VMEM((512, 512), F32),
            pltpu.VMEM((8, 512), F32),
            pltpu.VMEM((8, 512), F32),
            pltpu.VMEM((2, 8, 512), F32),
            pltpu.VMEM((2, 8, 512), F32),
            pltpu.VMEM((2, 256, 512), F32),
            pltpu.VMEM((2, 128, 512), F32),
        ],
        compiler_params=pltpu.CompilerParams(vmem_limit_bytes=VMEM_LIMIT),
    )(qx, dox, kvg, idg, cosine, sine)


def reduce_kernel(
    ox_ref, glx_ref, lowx_ref, normed_ref, up_ref,
    attn_ref, grad_at_ref, up_out_ref,
    mid_send, mid_recv, buf, rcore, b1, rp, b3, rz, final,
    p_send, p_recv, x_send, x_recv, z_send, z_recv, g_send, g_recv,
):
    x, y, z, j, f = places()
    i = 1 - j
    sibling = ctx_of(x, y, z, i)
    flat = x * 4 + y
    plane = [(flat + d) % 16 for d in range(1, 16)]
    whole_z = f * 4 + z
    zs = [(whole_z + d) % 8 for d in range(1, 8)]

    pair = pair_of(x, y, z, j)
    k = z // 2
    barrier = pltpu.get_barrier_semaphore()
    peers = [(sibling, f), (pair, f)]
    peers += [(ctx_of(p // 4, p % 4, z, j), f) for p in plane]
    peers += [(ctx_of(x, y, p % 4, j), p // 4) for p in zs]
    for peer in peers:
        pl.semaphore_signal(barrier, inc=1, device_id=peer, device_id_type=MESH)

    glx = jnp.concatenate([glx_ref[0], glx_ref[1]], axis=0)
    up = up_ref[:, pl.ds(pl.multiple_of(512 * k, 512), 512)]
    midt = ADAPTER_SCALE * lax.dot_general(
        up, glx, (((1,), (1,)), ((), ())), preferred_element_type=F32
    )
    mid_send[0] = midt[:, 0:128]
    mid_send[1] = midt[:, 128:256]
    pl.semaphore_wait(barrier, len(peers))

    sent = []
    mid_copy = remote(mid_send.at[1], mid_recv, p_send.at[0], p_recv.at[0], pair, f)
    mid_copy.start()
    near = pl.ds(pl.multiple_of(512 * k, 512), 512)
    out_copy = remote(ox_ref.at[1], attn_ref.at[:, near], p_send.at[1], p_recv.at[1], pair, f)
    attn_ref[:, near] = ox_ref[0]

    lowt = jnp.concatenate([lowx_ref[0], lowx_ref[1]], axis=1)
    upg = ADAPTER_SCALE * jnp.dot(lowt, glx, preferred_element_type=F32)
    buf[64:96] = jnp.zeros((32, 8, 128), F32)
    for s in range(2):
        for t in range(4):
            buf[64 + 16 * s + 8 * f + 4 * k + t] = upg[8 * s : 8 * s + 8, 128 * t : 128 * t + 128]
    mid_copy.wait()
    mid = (mid_send[0] + mid_recv[...]).astype(BF16)
    for t in range(4):
        part = jnp.dot(mid, normed_ref[:, 1024 * t : 1024 * t + 1024], preferred_element_type=F32)
        for s in range(2):
            for w in range(8):
                buf[32 * s + 8 * t + w] = part[8 * s : 8 * s + 8, 128 * w : 128 * w + 128]

    core_copy = remote(buf.at[pl.ds(48 * i, 48)], rcore, p_send.at[2], p_recv.at[2], sibling, f)
    core_copy.start()
    core_copy.wait()
    b1[...] = buf[pl.ds(48 * j, 48)] + rcore[...]
    copies = []
    for n, p in enumerate(plane):
        peer = ctx_of(p // 4, p % 4, z, j)
        copy = remote(b1.at[pl.ds(3 * p, 3)], rp.at[n], x_send.at[n], x_recv.at[n], peer, f)
        copy.start()
        copies.append(copy)
    out_copy.start()
    added = b1[pl.ds(3 * flat, 3)]
    for n, copy in enumerate(copies):
        copy.wait()
        added = added + rp[n]
    b3[...] = added
    copies = []
    for n, p in enumerate(zs):
        copy = remote(b3, rz.at[whole_z], z_send.at[n], z_recv.at[n], ctx_of(x, y, p % 4, j), p // 4)
        copy.start()
        copies.append(copy)
    rz[whole_z] = b3[...]
    for n, copy in enumerate(copies):
        source = (whole_z + 7 - n) % 8
        remote(rz.at[source], rz.at[source], z_send.at[n], z_recv.at[n], sibling, f).wait_recv()
    added = rz[0]
    for n in range(1, 8):
        added = added + rz[n]
    row = 48 * j + 3 * flat
    final[pl.ds(row, 3)] = added
    sent += copies

    for n, p in enumerate(plane):
        part = final.at[pl.ds(row, 3)]
        copy = remote(part, part, g_send.at[n], g_recv.at[n], ctx_of(p // 4, p % 4, z, j), f)
        copy.start()
        sent.append(copy)
    for n in range(15):
        part = final.at[pl.ds(48 * j + 3 * ((flat + 15 - n) % 16), 3)]
        remote(part, part, g_send.at[n], g_recv.at[n], sibling, f).wait_recv()
    part = final.at[pl.ds(48 * j, 48)]
    copy = remote(part, part, p_send.at[3], p_recv.at[3], sibling, f)
    copy.start()
    sent.append(copy)
    part = final.at[pl.ds(48 * i, 48)]
    remote(part, part, p_send.at[3], p_recv.at[3], sibling, f).wait_recv()

    for s in range(2):
        for t in range(32):
            grad_at_ref[8 * s : 8 * s + 8, 128 * t : 128 * t + 128] = final[32 * s + t]
        for t in range(8):
            up_out_ref[8 * s : 8 * s + 8, 128 * t : 128 * t + 128] = final[64 + 16 * s + 8 * f + t]

    other_half = attn_ref.at[:, pl.ds(pl.multiple_of(512 * (1 - k), 512), 512)]
    remote(ox_ref.at[1], other_half, p_send.at[1], p_recv.at[1], sibling, f).wait_recv()
    out_copy.wait_send()
    for copy in sent:
        copy.wait_send()


def reduce_all(ox, glx, lowx, normed, up):
    vmem = pl.BlockSpec(memory_space=pltpu.VMEM)
    hbm = pl.BlockSpec(memory_space=pl.ANY)
    dma = pltpu.SemaphoreType.DMA
    tiles = lambda *lead: pltpu.VMEM((*lead, 8, 128), F32)
    return pl.pallas_call(
        reduce_kernel,
        name="reduce_all",
        out_shape=(
            jax.ShapeDtypeStruct((128, 1024), BF16),
            jax.ShapeDtypeStruct((16, 4096), F32),
            jax.ShapeDtypeStruct((16, 1024), F32),
        ),
        in_specs=[vmem] * 5,
        out_specs=(vmem, vmem, vmem),
        scratch_shapes=[
            pltpu.VMEM((2, 16, 128), F32),
            pltpu.VMEM((16, 128), F32),
            tiles(96), tiles(48), tiles(48), tiles(15, 3), tiles(3), tiles(8, 3),
            tiles(96),
        ]
        + [dma((n,)) for n in (4, 4, 15, 15, 7, 7, 15, 15)],
        compiler_params=pltpu.CompilerParams(
            collective_id=1, has_side_effects=True, vmem_limit_bytes=VMEM_LIMIT
        ),
    )(ox, glx, lowx, normed, up)


def hand_over_kernel(a_ref, b_ref, c_ref, a_out, b_out, c_out):
    a_out[...] = a_ref[...]
    b_out[...] = b_ref[...]
    c_out[...] = c_ref[...]


def hand_over(*arrays):
    vmem = pl.BlockSpec(memory_space=pltpu.VMEM)
    return pl.pallas_call(
        hand_over_kernel,
        name="hand_over",
        out_shape=tuple(jax.ShapeDtypeStruct(a.shape, a.dtype) for a in arrays),
        in_specs=[vmem] * 3,
        out_specs=(vmem,) * 3,
        compiler_params=pltpu.CompilerParams(vmem_limit_bytes=VMEM_LIMIT),
    )(*arrays)


def on_device(
    layer_input,
    gain,
    codes,
    column_scale_quantized,
    block_second_scale,
    query_down_map,
    query_up_map,
    token_document,
    output_cotangent,
):
    x, y, z, j, _ = places()
    places_two = jnp.stack([ctx_of(x, y, z, j), pair_of(x, y, z, j)])
    freqs = jnp.exp(jnp.arange(HEAD // 2, dtype=F32) * (-2.0 * math.log(ROPE_BASE) / HEAD))
    positions = (places_two[:, None] * 128 + jnp.arange(128, dtype=I32)[None, :]).astype(F32)
    angle = positions[:, None, :] * freqs[None, :, None]
    cosine, sine = jnp.cos(angle), jnp.sin(angle)
    table = jnp.asarray(np.tile(np.asarray(NF4_LEVELS, np.float32)[:, None], (1, 128)))

    normed, dox, qx, kvg, idg, lowx = project(
        layer_input,
        gain[None, :],
        codes,
        column_scale_quantized,
        block_second_scale[None, :],
        query_down_map.T,
        query_up_map,
        cosine,
        sine,
        table,
        token_document[None, :],
        output_cotangent,
    )
    ox, glx = attend(qx, dox, kvg, idg, cosine, sine)
    attn, grad_at, up_map_gradient = reduce_all(ox, glx, lowx, normed, query_up_map)
    attn, grad_at, up_map_gradient = hand_over(attn, grad_at, up_map_gradient)
    return (attn, grad_at.T, up_map_gradient)


def solution(mesh):
    return jax.shard_map(
        on_device,
        mesh=mesh,
        in_specs=(
            P("ctx", None),
            P(),
            P("fsdp", None),
            P("fsdp", None),
            P(),
            P(),
            P(None, "fsdp"),
            P("ctx"),
            P("ctx", "fsdp"),
        ),
        out_specs=(P("ctx", "fsdp"), P(), P(None, "fsdp")),
        check_vma=False,
    )
```

```python
import functools
import math

import jax
import jax.numpy as jnp
import numpy as np
from jax import lax
from jax.experimental import pallas as pl
from jax.experimental.pallas import tpu as pltpu
from jax.sharding import PartitionSpec as P

MESH = pl.DeviceIdType.MESH
HEAD = 128
NF4_LEVELS = [
    -1.0,
    -0.6961928009986877,
    -0.5250730514526367,
    -0.39491748809814453,
    -0.28444138169288635,
    -0.18477343022823334,
    -0.09105003625154495,
    0.0,
    0.07958029955625534,
    0.16093020141124725,
    0.24611230194568634,
    0.33791524171829224,
    0.44070982933044434,
    0.5626170039176941,
    0.7229568362236023,
    1.0,
]
ADAPTER_SCALE = 2.0
ROPE_BASE = 500000.0
SOFT_SCALE = 1.0 / math.sqrt(HEAD)
QUERY_SCALE = SOFT_SCALE * math.log2(math.e)
F32, BF16, I32 = jnp.float32, jnp.bfloat16, jnp.int32
VMEM_LIMIT = 60 * 1024 * 1024


def places():
    c = lax.axis_index("ctx")
    f = lax.axis_index("fsdp")
    return c // 32, (c // 8) % 4, (c // 2) % 4, c % 2, f


def ctx_of(x, y, z, j):
    return ((x * 4 + y) * 4 + z) * 2 + j


def pair_of(x, y, z, j):
    return ctx_of(3 - x, 3 - y, (z + 2) % 4, j)


def lookup(table, index):
    return lax.gather(
        table,
        index[..., None],
        lax.GatherDimensionNumbers(
            offset_dims=(),
            collapsed_slice_dims=(0,),
            start_index_map=(0,),
            operand_batching_dims=(1,),
            start_indices_batching_dims=(1,),
        ),
        slice_sizes=(1, 1),
        mode=lax.GatherScatterMode.PROMISE_IN_BOUNDS,
    )


def remote(src, dst, send, recv, ctx, f):
    return pltpu.make_async_remote_copy(
        src_ref=src, dst_ref=dst, send_sem=send, recv_sem=recv, device_id=(ctx, f), device_id_type=MESH
    )


def project_kernel(
    x_ref, gain_ref, codes_ref, sq_ref, bs_ref, downt_ref, up_ref, cos_ref, sin_ref, table_ref, doc_ref, do_ref,
    normed_ref, dox, qx, kvg, idg, lowx,
    perm, scale, w_buf, acc, parts, send_kv, recv_kv, send_q, recv_q, extra, kv_buf, q_buf, low_buf, ids_buf,
    p_send, p_recv, e_send, e_recv, own_sem, z_send, z_recv, zi_send, zi_recv, a_send, a_recv, ai_send, ai_recv,
    b_send, b_recv, bi_send, bi_recv, s_send, s_recv,
):
    x, y, z, j, f = places()
    here = lax.axis_index("ctx")
    other = 1 - f
    i = 1 - j
    k = z // 2
    u = x * i + y * j
    v = y * i + x * j

    def at(uu, vv, zz):
        return ctx_of(uu * i + vv * j, vv * i + uu * j, zz, j)

    def slot(uu, vv, zz):
        return (uu * 4 + vv) * 4 + zz

    sibling = ctx_of(x, y, z, i)
    pair = pair_of(x, y, z, j)
    zo = (z + 2) % 4
    zn = z + 1 - 2 * (z % 2)
    zf = (zn + 2) % 4
    across, next_z, far_z = at(u, v, zo), at(u, v, zn), at(u, v, zf)
    vr, vl, vo = (v + 1) % 4, (v + 3) % 4, (v + 2) % 4
    ur, ul, uo = (u + 1) % 4, (u + 3) % 4, (u + 2) % 4
    right_v, left_v = at(u, vr, z), at(u, vl, z)
    right_u, left_u = at(ur, v, z), at(ul, v, z)

    barrier = pltpu.get_barrier_semaphore()
    pl.semaphore_signal(barrier, inc=1, device_id=(here, other), device_id_type=MESH)
    peers = [sibling, pair, across, next_z, far_z, right_v, left_v, right_u, left_u]
    for peer in peers:
        pl.semaphore_signal(barrier, inc=1, device_id=(peer, f), device_id_type=MESH)

    for r in range(8):
        wide = x_ref[16 * r : 16 * r + 16, :].astype(F32)
        inverse = lax.rsqrt(jnp.mean(wide * wide, axis=-1, keepdims=True) + 1e-05)
        normed_ref[16 * r : 16 * r + 16, :] = (wide * inverse * gain_ref[...]).astype(BF16)
    ids_buf[...] = jnp.broadcast_to(doc_ref[...], (8, 128))
    near = pl.ds(pl.multiple_of(512 * k, 512), 512)
    far = pl.ds(pl.multiple_of(512 * (1 - k), 512), 512)
    dox[0] = do_ref[:, near]

    sent = []

    def push(src, dst, n, send, recv, peer, group=f):
        copy = remote(src, dst, send.at[n], recv.at[n], peer, group)
        copy.start()
        sent.append(copy)

    def got(ref, n, send, recv):
        remote(ref, ref, send.at[n], recv.at[n], sibling, f).wait_recv()

    mine = slot(u, v, z)
    pl.semaphore_wait(barrier, len(peers) + 1)
    push(do_ref.at[:, far], dox.at[1], 3, e_send, e_recv, pair)
    for n, peer in enumerate((next_z, across, far_z)):
        push(ids_buf, idg.at[j, mine], n, zi_send, zi_recv, peer)

    for part in range(8):
        m = lax.broadcasted_iota(I32, (128, 1024), 0)
        column = lax.broadcasted_iota(I32, (128, 1024), 1)
        perm[128 * part : 128 * part + 128, :] = jnp.where(column == 8 * m + part, 1.0, 0.0).astype(BF16)
    pick = lax.broadcasted_iota(I32, (32, 64), 1) == lax.broadcasted_iota(I32, (32, 64), 0) + 32 * f
    second = jnp.sum(jnp.where(pick, bs_ref[...], 0.0), axis=1, keepdims=True) * (1.0 / 256.0)
    quantized = jnp.concatenate([sq_ref[:, 1024 * t : 1024 * t + 1024] for t in range(3)], axis=0)
    packed = lax.dot_general(
        (quantized.astype(F32) + 1.0).astype(BF16),
        perm[...],
        (((1,), (1,)), ((), ())),
        preferred_element_type=F32,
    )
    for t in range(3):
        scale[t] = packed[32 * t : 32 * t + 32] * second

    lower, upper = table_ref[0:8, :], table_ref[8:16, :]

    def tile(t):
        lane = pl.multiple_of(t * 128, 128)
        acc[...] = jnp.zeros_like(acc)

        def chunk(kc, carry):
            for b in range(4):
                row = pl.multiple_of(kc * 256 + b * 64, 64)
                words = codes_ref[pl.ds(row, 64), pl.ds(lane, 128)]
                scale_row = scale[t, pl.ds(kc * 4 + b, 1), :]
                for n in range(8):
                    scales = scale_row[:, 128 * n : 128 * n + 128]
                    scaled_lower, scaled_upper = lower * scales, upper * scales
                    rows = []
                    for r in range(8):
                        word = words[8 * r : 8 * r + 8]
                        index = jnp.bitwise_and(jnp.right_shift(word, 4 * n), 7)
                        high = jnp.left_shift(word, 28 - 4 * n) < 0
                        rows.append(jnp.where(high, lookup(scaled_upper, index), lookup(scaled_lower, index)))
                    w_buf[64 * b : 64 * b + 64, 128 * n : 128 * n + 128] = jnp.concatenate(rows, axis=0).astype(BF16)
            col = pl.multiple_of(f * 2048 + kc * 256, 256)
            acc[...] += jnp.dot(normed_ref[:, pl.ds(col, 256)], w_buf[...], preferred_element_type=F32)
            return carry

        lax.fori_loop(0, 8, chunk, 0)
        full = acc[...]
        high = full.astype(BF16)
        low = (full - high.astype(F32)).astype(BF16)
        natural = jnp.dot(jnp.concatenate([high, low], axis=0), perm[...], preferred_element_type=F32)
        parts[t] = natural[0:128] + natural[128:256]

    def columns(t, offset):
        return parts[t, :, pl.ds(pl.multiple_of(offset, 512), 512)]

    tile(2 - f)
    send_kv[...] = columns(2 - f, 512 * other).astype(BF16)
    push(send_kv, recv_kv, 0, p_send, p_recv, here, other)
    tile(other)
    send_q[:, 0:512] = columns(other, 512 * other).astype(BF16)
    send_q[:, 512:1024] = columns(2 * other, 512 * f).astype(BF16)
    tile(2 * f)

    cosine, sine = cos_ref[0].T, sin_ref[0].T
    cosine = jnp.concatenate([cosine, cosine], axis=1)
    sine = jnp.concatenate([-sine, sine], axis=1)

    def rotate(vector):
        return vector * cosine + pltpu.roll(vector, 64, 1) * sine

    got(recv_kv, 0, p_send, p_recv)
    both = columns(1 + f, 512 * f) + recv_kv[...].astype(F32)
    for h in range(2):
        kv_buf[h, :, 0:128] = rotate(both[:, 128 * h : 128 * h + 128]).astype(BF16)
        kv_buf[h, :, 128:256] = both[:, 256 + 128 * h : 384 + 128 * h].astype(BF16)

    push(kv_buf.at[1 - k], kvg.at[j, mine], 0, e_send, e_recv, across)
    push(kv_buf.at[k], kvg.at[j, mine], 0, z_send, z_recv, next_z)
    local = []

    def keep(src, dst, n):
        copy = pltpu.make_async_copy(src, dst, own_sem.at[n])
        copy.start()
        local.append(copy)

    keep(kv_buf.at[k], kvg.at[j, mine], 0)
    keep(ids_buf, idg.at[j, mine], 1)

    lowt = lax.dot_general(
        downt_ref[...], normed_ref[...], (((1,), (1,)), ((), ())), preferred_element_type=F32
    ).astype(BF16)
    low_buf[...] = lowt
    extra[...] = ADAPTER_SCALE * lax.dot_general(
        lowt, up_ref[...], (((0,), (0,)), ((), ())), preferred_element_type=F32
    )

    block = kvg.at[j, slot(u, v, zo)]
    got(block, 0, e_send, e_recv)
    push(block, block, 1, z_send, z_recv, next_z)
    push(send_q, recv_q, 1, p_send, p_recv, here, other)
    push(low_buf, lowx.at[1], 2, e_send, e_recv, pair)
    keep(low_buf, lowx.at[0], 2)

    got(kvg.at[j, slot(u, v, zn)], 0, z_send, z_recv)
    for n, zz in enumerate((zn, zo, zf)):
        got(idg.at[j, slot(u, v, zz)], n, zi_send, zi_recv)
    local[0].wait()
    local[1].wait()
    got(kvg.at[j, slot(u, v, zf)], 1, z_send, z_recv)

    def half(vv, h):
        return kvg.at[j, pl.ds(slot(u, vv, 0) + 2 * h, 2)]

    def piece(uu, vv):
        return kvg.at[j, pl.ds(slot(uu, vv, 0), 4)]

    def marks(vv):
        return idg.at[j, pl.ds(slot(u, vv, 0), 4)]

    def all_marks(uu):
        return idg.at[j, pl.ds(slot(uu, 0, 0), 16)]

    def same(part, n, send, recv, peer):
        push(part, part, n, send, recv, peer)

    shared = []

    def share(du, dv):
        part = piece((u + du) % 4, (v + dv) % 4)
        same(part, len(shared), s_send, s_recv, sibling)
        shared.append((du, dv))

    same(half(v, 0), 0, a_send, a_recv, right_v)
    same(half(v, 1), 3, a_send, a_recv, left_v)
    same(half(v, 1), 1, a_send, a_recv, right_v)
    same(half(v, 0), 4, a_send, a_recv, left_v)
    same(marks(v), 0, ai_send, ai_recv, right_v)
    same(marks(v), 1, ai_send, ai_recv, left_v)
    same(piece(u, v), 0, b_send, b_recv, right_u)
    same(piece(u, v), 4, b_send, b_recv, left_u)
    share(0, 0)
    got(half(vl, 0), 0, a_send, a_recv)
    same(half(vl, 0), 2, a_send, a_recv, right_v)
    got(half(vr, 1), 3, a_send, a_recv)
    same(half(vr, 1), 5, a_send, a_recv, left_v)
    got(half(vl, 1), 1, a_send, a_recv)
    got(marks(vl), 0, ai_send, ai_recv)
    same(marks(vl), 2, ai_send, ai_recv, right_v)
    same(piece(u, vl), 1, b_send, b_recv, right_u)
    same(piece(u, vl), 5, b_send, b_recv, left_u)
    share(0, 3)
    got(half(vr, 0), 4, a_send, a_recv)
    got(marks(vr), 1, ai_send, ai_recv)
    same(piece(u, vr), 2, b_send, b_recv, right_u)
    same(piece(u, vr), 6, b_send, b_recv, left_u)
    share(0, 1)
    got(half(vo, 0), 2, a_send, a_recv)
    got(half(vo, 1), 5, a_send, a_recv)
    got(marks(vo), 2, ai_send, ai_recv)
    same(piece(u, vo), 3, b_send, b_recv, right_u)
    same(piece(u, vo), 7, b_send, b_recv, left_u)
    share(0, 2)
    same(all_marks(u), 0, bi_send, bi_recv, right_u)
    same(all_marks(u), 1, bi_send, bi_recv, left_u)

    got(piece(ul, v), 0, b_send, b_recv)
    same(piece(ul, v), 8, b_send, b_recv, right_u)
    share(3, 0)
    got(piece(ul, vl), 1, b_send, b_recv)
    same(piece(ul, vl), 9, b_send, b_recv, right_u)
    share(3, 3)

    got(recv_q, 1, p_send, p_recv)
    for h in range(8):
        s = slice(128 * h, 128 * h + 128)
        if h < 4:
            own = parts[f, :, pl.ds(pl.multiple_of(512 * f + 128 * h, 128), 128)]
        else:
            own = parts[2 * f, :, pl.ds(pl.multiple_of(512 * other + 128 * (h - 4), 128), 128)]
        whole = own + recv_q[:, s].astype(F32) + extra[:, s]
        q_buf[:, s] = (rotate(whole) * QUERY_SCALE).astype(BF16)
    push(q_buf.at[:, far], qx.at[1], 1, e_send, e_recv, pair)
    keep(q_buf.at[:, near], qx.at[0], 3)

    got(piece(ur, vr), 6, b_send, b_recv)
    same(piece(ur, vr), 10, b_send, b_recv, left_u)
    share(1, 1)
    got(piece(ur, vo), 7, b_send, b_recv)
    same(piece(ur, vo), 11, b_send, b_recv, left_u)
    share(1, 2)
    got(all_marks(ul), 0, bi_send, bi_recv)
    same(all_marks(ul), 2, bi_send, bi_recv, right_u)
    got(all_marks(ur), 1, bi_send, bi_recv)
    got(piece(ul, vr), 2, b_send, b_recv)
    share(3, 1)
    got(piece(ul, vo), 3, b_send, b_recv)
    share(3, 2)
    got(piece(ur, v), 4, b_send, b_recv)
    share(1, 0)
    got(piece(ur, vl), 5, b_send, b_recv)
    share(1, 3)
    got(all_marks(uo), 2, bi_send, bi_recv)
    same(idg.at[j], 16, s_send, s_recv, sibling)
    got(piece(uo, v), 8, b_send, b_recv)
    share(2, 0)
    got(piece(uo, vr), 10, b_send, b_recv)
    share(2, 1)
    got(piece(uo, vl), 9, b_send, b_recv)
    share(2, 3)
    got(piece(uo, vo), 11, b_send, b_recv)
    share(2, 2)

    got(dox.at[1], 3, e_send, e_recv)
    got(lowx.at[1], 2, e_send, e_recv)
    got(qx.at[1], 1, e_send, e_recv)
    for n, (du, dv) in enumerate(shared):
        got(kvg.at[i, pl.ds(slot((v + du) % 4, (u + dv) % 4, 0), 4)], n, s_send, s_recv)
    got(idg.at[i], 16, s_send, s_recv)
    for copy in local[2:]:
        copy.wait()
    for copy in sent:
        copy.wait_send()


def project(x, gain, codes, sq, bs, downt, up, cosine, sine, table, doc, do):
    vmem = pl.BlockSpec(memory_space=pltpu.VMEM)
    hbm = pl.BlockSpec(memory_space=pl.ANY)
    dma = pltpu.SemaphoreType.DMA
    counts = (2, 2, 4, 4, 4, 2, 2, 3, 3, 6, 6, 3, 3, 12, 12, 3, 3, 17, 17)
    return pl.pallas_call(
        project_kernel,
        name="project",
        out_shape=(
            jax.ShapeDtypeStruct((128, 4096), BF16),
            jax.ShapeDtypeStruct((2, 128, 512), BF16),
            jax.ShapeDtypeStruct((2, 128, 512), BF16),
            jax.ShapeDtypeStruct((2, 64, 128, 256), BF16),
            jax.ShapeDtypeStruct((2, 64, 8, 128), I32),
            jax.ShapeDtypeStruct((2, 16, 128), BF16),
        ),
        in_specs=[vmem] * 12,
        out_specs=(vmem, vmem, hbm, hbm, hbm, hbm),
        scratch_shapes=[
            pltpu.VMEM((1024, 1024), BF16),
            pltpu.VMEM((3, 32, 1024), F32),
            pltpu.VMEM((256, 1024), BF16),
            pltpu.VMEM((128, 1024), F32),
            pltpu.VMEM((3, 128, 1024), F32),
            pltpu.VMEM((128, 512), BF16),
            pltpu.VMEM((128, 512), BF16),
            pltpu.VMEM((128, 1024), BF16),
            pltpu.VMEM((128, 1024), BF16),
            pltpu.VMEM((128, 1024), F32),
            pltpu.VMEM((2, 128, 256), BF16),
            pltpu.VMEM((128, 1024), BF16),
            pltpu.VMEM((16, 128), BF16),
            pltpu.VMEM((8, 128), I32),
        ]
        + [dma((n,)) for n in counts],
        compiler_params=pltpu.CompilerParams(
            collective_id=0, has_side_effects=True, vmem_limit_bytes=VMEM_LIMIT
        ),
    )(x, gain, codes, sq, bs, downt, up, cosine, sine, table, doc, do)


STEP = 512


def attend_kernel(
    qx_ref, dox_ref, kvg_ref, idg_ref, cos_ref, sin_ref, ox_ref, glx_ref,
    qt, dot_, limits, ahead0, ahead1, max0, max1, run_max, run_sum, acc, acc2,
):
    x, y, z, j, _ = places()
    here = ctx_of(x, y, z, j)
    there = pair_of(x, y, z, j)

    def slot(number, core):
        a, b, d = number // 16, (number // 4) % 4, number % 4
        first, second = (a * 4 + b) * 4 + d, (b * 4 + a) * 4 + d
        if isinstance(core, int):
            return second if core else first
        return jnp.where(core == 0, first, second)

    def block(number):
        return jnp.concatenate([kvg_ref[0, slot(number, 0)], kvg_ref[1, slot(number, 1)]], axis=0)

    every = idg_ref[...].reshape(128, 8, 128)
    below = [
        jnp.sum(jnp.sum(jnp.where(every < d, 1, 0), axis=0), axis=1, keepdims=True)[0:1, :] for d in (1, 2, 3)
    ]
    lane = lax.broadcasted_iota(I32, (1, 128), 1)
    for t, place in enumerate((here, there)):
        ids = idg_ref[j, slot(place // 2, j), 0:1, :]
        start = jnp.zeros((1, 128), I32)
        for d in (1, 2, 3):
            start = jnp.where(ids == d, below[d - 1], start)
        limits[t, 0:1, :] = jnp.concatenate([start, start], axis=1)
        position = place * 128 + lane
        limits[t, 1:2, :] = jnp.concatenate([position, position], axis=1)
        for g in range(4):
            lanes = slice(128 * g, 128 * g + 128)
            qt[t, :, lanes] = qx_ref[t, :, lanes].T
            dot_[t, :, lanes] = dox_ref[t, :, lanes].T
    run_max[...] = jnp.full_like(run_max, -1e29)
    run_sum[...] = jnp.zeros_like(run_sum)
    acc[...] = jnp.zeros_like(acc)
    acc2[...] = jnp.zeros_like(acc2)

    def rows(t, carry):
        place = jnp.where(t == 0, here, there)
        first = jnp.min(limits[t, 0:1, :]) // STEP
        latest = jnp.max(limits[t, 0:1, :])
        stop = (place * 128 + 127) // STEP + 1

        def scores_of(number, masked, ahead, ahead_max):
            key = jnp.minimum(number, 31) * 2
            base = number * STEP
            for h in range(2):
                keys = block(key + h)[:, :128]
                for p in range(2):
                    cols = slice(256 * p, 256 * p + 256)
                    scores = jnp.dot(keys, qt[t, :, cols], preferred_element_type=F32)
                    if masked:
                        pos = base + 256 * h + lax.broadcasted_iota(I32, (256, 256), 0)
                        allowed = (pos >= limits[t, 0:1, :]) & (pos <= limits[t, 1:2, :])
                        scores = jnp.where(allowed, scores, -1e30)
                    ahead[256 * h : 256 * h + 256, cols] = scores
                    top = jnp.max(scores, axis=0, keepdims=True)
                    ahead_max[h : h + 1, cols] = top

        def is_edge(number):
            return (number * STEP < latest) | (number * STEP + STEP - 1 > place * 128)

        def step(number, masked, ahead, ahead_max, later, later_max):
            scores_of(number + 1, masked, later, later_max)
            kv = jnp.concatenate([block(2 * number), block(2 * number + 1)], axis=0)
            kvt = kv.T
            values = kv[:, 128:]
            for p in range(2):
                cols = slice(256 * p, 256 * p + 256)
                tops = jnp.maximum(ahead_max[0:1, cols], ahead_max[1:2, cols])
                old = run_max[t, 0:1, cols]
                new = jnp.maximum(old, tops)
                decay = jnp.exp2(old - new)
                run_max[t, 0:1, cols] = new
                grad_dots = jnp.dot(values, dot_[t, :, cols], preferred_element_type=F32)
                expo = jnp.exp2(ahead[:, cols] - new)
                run_sum[t, 0:1, cols] = run_sum[t, 0:1, cols] * decay + jnp.sum(expo, axis=0, keepdims=True)
                weighted = (expo * grad_dots).astype(BF16)
                acc[t, :, cols] = acc[t, :, cols] * decay + jnp.dot(
                    kvt, expo.astype(BF16), preferred_element_type=F32
                )
                acc2[t, :, cols] = acc2[t, :, cols] * decay + jnp.dot(
                    kvt[:128], weighted, preferred_element_type=F32
                )

        scores_of(first, True, ahead0, max0)

        def one(number, *buffers):
            edge = is_edge(number + 1)

            @pl.when(edge)
            def _():
                step(number, True, *buffers)

            @pl.when(jnp.logical_not(edge))
            def _():
                step(number, False, *buffers)

        def body(twice, c):
            number = first + 2 * twice
            one(number, ahead0, max0, ahead1, max1)

            @pl.when(number + 1 < stop)
            def _():
                one(number + 1, ahead1, max1, ahead0, max0)

            return c

        lax.fori_loop(0, (stop - first + 1) // 2, body, 0)
        return carry

    lax.fori_loop(0, 2, rows, 0)

    for t in range(2):
        cosine, sine = cos_ref[t], sin_ref[t]
        for g in range(4):
            lanes = slice(128 * g, 128 * g + 128)
            inverse = 1.0 / run_sum[t, 0:1, lanes]
            out = acc[t, 128:256, lanes] * inverse
            mean_dot = jnp.sum(dot_[t, :, lanes].astype(F32) * out, axis=0, keepdims=True)
            grad = (acc2[t, :, lanes] - mean_dot * acc[t, 0:128, lanes]) * (inverse * SOFT_SCALE)
            ga, gb = grad[:64], grad[64:]
            back = jnp.concatenate([ga * cosine + gb * sine, gb * cosine - ga * sine], axis=0)
            ox_ref[t, :, lanes] = out.T.astype(BF16)
            glx_ref[t, :, lanes] = back.T.astype(BF16)


def attend(qx, dox, kvg, idg, cosine, sine):
    vmem = pl.BlockSpec(memory_space=pltpu.VMEM)
    return pl.pallas_call(
        attend_kernel,
        name="attend",
        out_shape=(jax.ShapeDtypeStruct((2, 128, 512), BF16), jax.ShapeDtypeStruct((2, 128, 512), BF16)),
        in_specs=[vmem] * 6,
        out_specs=(vmem, vmem),
        scratch_shapes=[
            pltpu.VMEM((2, 128, 512), BF16),
            pltpu.VMEM((2, 128, 512), BF16),
            pltpu.VMEM((2, 8, 256), I32),
            pltpu.VMEM((512, 512), F32),
            pltpu.VMEM((512, 512), F32),
            pltpu.VMEM((8, 512), F32),
            pltpu.VMEM((8, 512), F32),
            pltpu.VMEM((2, 8, 512), F32),
            pltpu.VMEM((2, 8, 512), F32),
            pltpu.VMEM((2, 256, 512), F32),
            pltpu.VMEM((2, 128, 512), F32),
        ],
        compiler_params=pltpu.CompilerParams(vmem_limit_bytes=VMEM_LIMIT),
    )(qx, dox, kvg, idg, cosine, sine)


def reduce_kernel(
    ox_ref, glx_ref, lowx_ref, normed_ref, up_ref,
    attn_ref, grad_at_ref, up_out_ref,
    mid_send, mid_recv, buf, rcore, b1, rp, b3, rz, final,
    p_send, p_recv, x_send, x_recv, z_send, z_recv, g_send, g_recv,
):
    x, y, z, j, f = places()
    i = 1 - j
    sibling = ctx_of(x, y, z, i)
    flat = x * 4 + y
    plane = [(flat + d) % 16 for d in range(1, 16)]
    whole_z = f * 4 + z
    zs = [(whole_z + d) % 8 for d in range(1, 8)]

    pair = pair_of(x, y, z, j)
    k = z // 2
    barrier = pltpu.get_barrier_semaphore()
    peers = [(sibling, f), (pair, f)]
    peers += [(ctx_of(p // 4, p % 4, z, j), f) for p in plane]
    peers += [(ctx_of(x, y, p % 4, j), p // 4) for p in zs]
    for peer in peers:
        pl.semaphore_signal(barrier, inc=1, device_id=peer, device_id_type=MESH)

    glx = jnp.concatenate([glx_ref[0], glx_ref[1]], axis=0)
    up = up_ref[:, pl.ds(pl.multiple_of(512 * k, 512), 512)]
    midt = ADAPTER_SCALE * lax.dot_general(
        up, glx, (((1,), (1,)), ((), ())), preferred_element_type=F32
    )
    mid_send[0] = midt[:, 0:128]
    mid_send[1] = midt[:, 128:256]
    pl.semaphore_wait(barrier, len(peers))

    sent = []
    mid_copy = remote(mid_send.at[1], mid_recv, p_send.at[0], p_recv.at[0], pair, f)
    mid_copy.start()
    near = pl.ds(pl.multiple_of(512 * k, 512), 512)
    out_copy = remote(ox_ref.at[1], attn_ref.at[:, near], p_send.at[1], p_recv.at[1], pair, f)
    attn_ref[:, near] = ox_ref[0]

    lowt = jnp.concatenate([lowx_ref[0], lowx_ref[1]], axis=1)
    upg = ADAPTER_SCALE * jnp.dot(lowt, glx, preferred_element_type=F32)
    buf[64:96] = jnp.zeros((32, 8, 128), F32)
    for s in range(2):
        for t in range(4):
            buf[64 + 16 * s + 8 * f + 4 * k + t] = upg[8 * s : 8 * s + 8, 128 * t : 128 * t + 128]
    mid_copy.wait()
    mid = (mid_send[0] + mid_recv[...]).astype(BF16)
    for t in range(4):
        part = jnp.dot(mid, normed_ref[:, 1024 * t : 1024 * t + 1024], preferred_element_type=F32)
        for s in range(2):
            for w in range(8):
                buf[32 * s + 8 * t + w] = part[8 * s : 8 * s + 8, 128 * w : 128 * w + 128]

    core_copy = remote(buf.at[pl.ds(48 * i, 48)], rcore, p_send.at[2], p_recv.at[2], sibling, f)
    core_copy.start()
    core_copy.wait()
    b1[...] = buf[pl.ds(48 * j, 48)] + rcore[...]
    copies = []
    for n, p in enumerate(plane):
        peer = ctx_of(p // 4, p % 4, z, j)
        copy = remote(b1.at[pl.ds(3 * p, 3)], rp.at[n], x_send.at[n], x_recv.at[n], peer, f)
        copy.start()
        copies.append(copy)
    out_copy.start()
    added = b1[pl.ds(3 * flat, 3)]
    for n, copy in enumerate(copies):
        copy.wait()
        added = added + rp[n]
    b3[...] = added
    copies = []
    for n, p in enumerate(zs):
        copy = remote(b3, rz.at[whole_z], z_send.at[n], z_recv.at[n], ctx_of(x, y, p % 4, j), p // 4)
        copy.start()
        copies.append(copy)
    rz[whole_z] = b3[...]
    for n, copy in enumerate(copies):
        source = (whole_z + 7 - n) % 8
        remote(rz.at[source], rz.at[source], z_send.at[n], z_recv.at[n], sibling, f).wait_recv()
    added = rz[0]
    for n in range(1, 8):
        added = added + rz[n]
    row = 48 * j + 3 * flat
    final[pl.ds(row, 3)] = added
    sent += copies

    for n, p in enumerate(plane):
        part = final.at[pl.ds(row, 3)]
        copy = remote(part, part, g_send.at[n], g_recv.at[n], ctx_of(p // 4, p % 4, z, j), f)
        copy.start()
        sent.append(copy)
    for n in range(15):
        part = final.at[pl.ds(48 * j + 3 * ((flat + 15 - n) % 16), 3)]
        remote(part, part, g_send.at[n], g_recv.at[n], sibling, f).wait_recv()
    part = final.at[pl.ds(48 * j, 48)]
    copy = remote(part, part, p_send.at[3], p_recv.at[3], sibling, f)
    copy.start()
    sent.append(copy)
    part = final.at[pl.ds(48 * i, 48)]
    remote(part, part, p_send.at[3], p_recv.at[3], sibling, f).wait_recv()

    for s in range(2):
        for t in range(32):
            grad_at_ref[8 * s : 8 * s + 8, 128 * t : 128 * t + 128] = final[32 * s + t]
        for t in range(8):
            up_out_ref[8 * s : 8 * s + 8, 128 * t : 128 * t + 128] = final[64 + 16 * s + 8 * f + t]

    other_half = attn_ref.at[:, pl.ds(pl.multiple_of(512 * (1 - k), 512), 512)]
    remote(ox_ref.at[1], other_half, p_send.at[1], p_recv.at[1], sibling, f).wait_recv()
    out_copy.wait_send()
    for copy in sent:
        copy.wait_send()


def reduce_all(ox, glx, lowx, normed, up):
    vmem = pl.BlockSpec(memory_space=pltpu.VMEM)
    hbm = pl.BlockSpec(memory_space=pl.ANY)
    dma = pltpu.SemaphoreType.DMA
    tiles = lambda *lead: pltpu.VMEM((*lead, 8, 128), F32)
    return pl.pallas_call(
        reduce_kernel,
        name="reduce_all",
        out_shape=(
            jax.ShapeDtypeStruct((128, 1024), BF16),
            jax.ShapeDtypeStruct((16, 4096), F32),
            jax.ShapeDtypeStruct((16, 1024), F32),
        ),
        in_specs=[vmem] * 5,
        out_specs=(vmem, vmem, vmem),
        scratch_shapes=[
            pltpu.VMEM((2, 16, 128), F32),
            pltpu.VMEM((16, 128), F32),
            tiles(96), tiles(48), tiles(48), tiles(15, 3), tiles(3), tiles(8, 3),
            tiles(96),
        ]
        + [dma((n,)) for n in (4, 4, 15, 15, 7, 7, 15, 15)],
        compiler_params=pltpu.CompilerParams(
            collective_id=1, has_side_effects=True, vmem_limit_bytes=VMEM_LIMIT
        ),
    )(ox, glx, lowx, normed, up)


def hand_over_kernel(a_ref, b_ref, c_ref, a_out, b_out, c_out):
    a_out[...] = a_ref[...]
    b_out[...] = b_ref[...]
    c_out[...] = c_ref[...]


def hand_over(*arrays):
    vmem = pl.BlockSpec(memory_space=pltpu.VMEM)
    return pl.pallas_call(
        hand_over_kernel,
        name="hand_over",
        out_shape=tuple(jax.ShapeDtypeStruct(a.shape, a.dtype) for a in arrays),
        in_specs=[vmem] * 3,
        out_specs=(vmem,) * 3,
        compiler_params=pltpu.CompilerParams(vmem_limit_bytes=VMEM_LIMIT),
    )(*arrays)


def on_device(
    layer_input,
    gain,
    codes,
    column_scale_quantized,
    block_second_scale,
    query_down_map,
    query_up_map,
    token_document,
    output_cotangent,
):
    x, y, z, j, _ = places()
    places_two = jnp.stack([ctx_of(x, y, z, j), pair_of(x, y, z, j)])
    freqs = jnp.exp(jnp.arange(HEAD // 2, dtype=F32) * (-2.0 * math.log(ROPE_BASE) / HEAD))
    positions = (places_two[:, None] * 128 + jnp.arange(128, dtype=I32)[None, :]).astype(F32)
    angle = positions[:, None, :] * freqs[None, :, None]
    cosine, sine = jnp.cos(angle), jnp.sin(angle)
    table = jnp.asarray(np.tile(np.asarray(NF4_LEVELS, np.float32)[:, None], (1, 128)))

    normed, dox, qx, kvg, idg, lowx = project(
        layer_input,
        gain[None, :],
        codes,
        column_scale_quantized,
        block_second_scale[None, :],
        query_down_map.T,
        query_up_map,
        cosine,
        sine,
        table,
        token_document[None, :],
        output_cotangent,
    )
    ox, glx = attend(qx, dox, kvg, idg, cosine, sine)
    attn, grad_at, up_map_gradient = reduce_all(ox, glx, lowx, normed, query_up_map)
    attn, grad_at, up_map_gradient = hand_over(attn, grad_at, up_map_gradient)
    return (attn, grad_at.T, up_map_gradient)


def solution(mesh):
    return jax.shard_map(
        on_device,
        mesh=mesh,
        in_specs=(
            P("ctx", None),
            P(),
            P("fsdp", None),
            P("fsdp", None),
            P(),
            P(),
            P(None, "fsdp"),
            P("ctx"),
            P("ctx", "fsdp"),
        ),
        out_specs=(P("ctx", "fsdp"), P(), P(None, "fsdp")),
        check_vma=False,
    )
```
